64 devices in a mesh: dp: 4 (over x, y), tp: 16 (over z, core).
Axes of the slice: x: 2, y: 2, z: 8, core: 2. Of those that a mesh axis runs over, the one named last changes fastest.
The devices are a block of a 4x4x8 slice.
Arguments:
- q_hidden: bfloat16 [1024, 32, 1024], P(('dp', 'tp')), parts along dimension 0
- d_hidden: bfloat16 [128, 128, 1024], P(('dp', 'tp')), parts along dimension 0
- q_mask: int32 [1024, 32], P(('dp', 'tp')), parts along dimension 0
- d_mask: int32 [128, 128], P(('dp', 'tp')), parts along dimension 0
- positive: int32 [1024], P(('dp', 'tp')), parts along dimension 0
- w_head: bfloat16 [1024, 32768], P(None, 'tp')
- b_head: float32 [32768], P('tp')
Outputs:
- output 1: float32 [4], P('dp'), parts along dimension 0
- output 2: bfloat16 [4096, 32768], P('dp', 'tp'), parts along dimension 0
- output 3: float32 [131072], P(('dp', 'tp')), parts along dimension 0
- output 4: bfloat16 [1024, 32, 1024], P(('dp', 'tp')), parts along dimension 0
- output 5: bfloat16 [128, 128, 1024], P(('dp', 'tp')), parts along dimension 0
There are 4 independent parts. The reference program is written for one: setup_inputs(seed, part) draws one part's arguments, and reference() takes and returns one part's arrays. A program takes and returns all parts, laid end to end along the dimension named above; an argument that names none is the same for every part.
All inputs are finite; a program needn't handle non-finite values.
Results may differ from the reference program's by a relative error of at most 0.0141936.
Values are sent between devices in bfloat16 or wider.
A program may use at most 768 MiB of HBM per device.

```python
import math
import jax
import jax.numpy as jnp
from jax import lax

BQ = 256
BD = 32
LQ = 32
LD = 128
D = 1024
V = 32768

TEMPERATURE = LQ * math.sqrt(V * LD) / 16.0
LAM_Q = 4.0 / (V * LQ * LQ)
LAM_D = 4.0 / (V * LD * LD)


def draw_mask(mask_key, n_rows, length):
    row_lens = jax.random.randint(mask_key, (n_rows,), length // 2, length + 1)
    row_lens = row_lens.at[0].set(length)
    return (jnp.arange(length)[None, :] < row_lens[:, None]).astype(jnp.int32)


def setup_inputs(seed: int = 0, part: int = 0) -> dict:
    base_key = jax.random.key(seed)
    shared_key, part_root = jax.random.split(base_key)
    part_key = jax.random.fold_in(part_root, part)
    part_keys = jax.random.split(part_key, 5)
    shared_keys = jax.random.split(shared_key, 2)
    q_hidden = jax.random.normal(part_keys[0], (BQ, LQ, D), jnp.float32).astype(jnp.bfloat16)
    d_hidden = jax.random.normal(part_keys[1], (BD, LD, D), jnp.float32).astype(jnp.bfloat16)
    q_mask = draw_mask(part_keys[2], BQ, LQ)
    d_mask = draw_mask(part_keys[3], BD, LD)
    positive = jax.random.randint(part_keys[4], (BQ,), 0, BD)
    positive = positive.at[0].set(0).at[BQ - 1].set(BD - 1)
    w_head = (jax.random.normal(shared_keys[0], (D, V), jnp.float32) * D ** -0.5).astype(jnp.bfloat16)
    b_head = 0.5 * jax.random.normal(shared_keys[1], (V,), jnp.float32) - 0.25
    return dict(q_hidden=q_hidden, d_hidden=d_hidden, q_mask=q_mask, d_mask=d_mask,
                positive=positive, w_head=w_head, b_head=b_head)


def head_rows(hidden, mask_arr, w_head, b_head):
    def one_row(row_in):
        hid_row, mask_row = row_in
        logits = jnp.dot(hid_row, w_head, preferred_element_type=jnp.float32) + b_head
        active = jnp.log1p(jnp.maximum(logits, 0.0)) * mask_row[:, None].astype(jnp.float32)
        return jnp.sum(active, axis=0)
    return lax.map(one_row, (hidden, mask_arr))


def head_grads(hidden, mask_arr, grad_rep, w_head, b_head, acc_init):
    def one_row(acc_pair, row_in):
        acc_w, acc_b = acc_pair
        hid_row, mask_row, grad_row = row_in
        logits = jnp.dot(hid_row, w_head, preferred_element_type=jnp.float32) + b_head
        relu_slope = jnp.where(logits > 0.0, 1.0 / (1.0 + jnp.maximum(logits, 0.0)), 0.0)
        grad_logits = grad_row[None, :] * relu_slope * mask_row[:, None].astype(jnp.float32)
        grad_low = grad_logits.astype(jnp.bfloat16)
        acc_w = acc_w + jnp.dot(hid_row.T, grad_low, preferred_element_type=jnp.float32)
        acc_b = acc_b + jnp.sum(grad_logits, axis=0)
        grad_hid = jnp.dot(grad_low, w_head.T, preferred_element_type=jnp.float32).astype(jnp.bfloat16)
        return (acc_w, acc_b), grad_hid
    return lax.scan(one_row, acc_init, (hidden, mask_arr, grad_rep))


def reference(q_hidden, d_hidden, q_mask, d_mask, positive, w_head, b_head):
    q_rep = head_rows(q_hidden, q_mask, w_head, b_head)
    d_rep = head_rows(d_hidden, d_mask, w_head, b_head)
    scores = jnp.dot(q_rep, d_rep.T, preferred_element_type=jnp.float32) / TEMPERATURE
    log_norm = jax.nn.logsumexp(scores, axis=1)
    target = (positive[:, None] == jnp.arange(BD)[None, :]).astype(jnp.float32)
    q_mean = jnp.mean(q_rep, axis=0)
    d_mean = jnp.mean(d_rep, axis=0)
    loss_val = (jnp.mean(log_norm - jnp.sum(scores * target, axis=1))
                + LAM_Q * jnp.sum(q_mean * q_mean) + LAM_D * jnp.sum(d_mean * d_mean))
    grad_scores = (jnp.exp(scores - log_norm[:, None]) - target) / (BQ * TEMPERATURE)
    grad_q = jnp.dot(grad_scores, d_rep, preferred_element_type=jnp.float32) + (2.0 * LAM_Q / BQ) * q_mean
    grad_d = jnp.dot(grad_scores.T, q_rep, preferred_element_type=jnp.float32) + (2.0 * LAM_D / BD) * d_mean
    acc_init = (jnp.zeros((D, V), jnp.float32), jnp.zeros((V,), jnp.float32))
    acc_mid, grad_qh = head_grads(q_hidden, q_mask, grad_q, w_head, b_head, acc_init)
    (acc_w, acc_b), grad_dh = head_grads(d_hidden, d_mask, grad_d, w_head, b_head, acc_mid)
    return jnp.reshape(loss_val, (1,)), acc_w.astype(jnp.bfloat16), acc_b, grad_qh, grad_dh
```

```python
import functools
import math
import jax
import jax.numpy as jnp
from jax import lax
from jax.experimental import pallas as pl
from jax.experimental.pallas import tpu as pltpu
from jax.sharding import PartitionSpec as P

MESH = pl.DeviceIdType.MESH
HIGHEST = lax.Precision.HIGHEST
F32 = jnp.float32
BF16 = jnp.bfloat16

UT = 16
CH = 512
MAXD = 4


def kernel(n_group, q_rows, q_len, d_rows, d_len,
           q_ref, d_ref, w_ref, b_ref, msg_ref,
           loss_ref, gw_out, gb_ref, dq_out, dd_out,
           wbuf, wt, gw, grecv, rep, maskx, own, acc_h, part, xbuf, rbuf, sbuf, gbuf, pbuf, xt,
           rdx, ddx, ddr, bias, gbacc, gbrecv, msgs, smsg, lossx, lossf,
           ag_send, ag_recv, ag_cred, rs_send, rs_recv, rs_cred,
           loc_sem, w_sem, bias_sem, msg_send, msg_recv, sm_send, sm_recv, pair_sem, gx_send, gx_recv,
           loss_send, loss_recv, out_sem):
    nz = n_group // 2
    hid = w_ref.shape[0]
    v_loc = w_ref.shape[1]
    v_chip = 2 * v_loc
    n_q = q_rows * q_len // UT
    n_d = d_rows * d_len // UT
    n_unit = n_q + n_d
    per_row = q_len // UT
    pieces = d_len // q_len
    pad_rows = MAXD // per_row
    rows = nz * UT
    n_chunk = v_chip // CH

    me = lax.axis_index('tp')
    z = me // 2
    c = lax.rem(me, 2)
    right = lax.rem(z + 1, nz)
    left = lax.rem(z + nz - 1, nz)
    sib = {'tp': 2 * z + 1 - c}

    def same(zz):
        return {'tp': 2 * zz + c}

    ahead = (same(right), same(left))
    behind = (same(left), same(right))

    def slot(way, dist):
        return dist if way == 0 else nz - dist

    def dist_of(s):
        return min(s, nz - s)

    def chip_of(s):
        return lax.rem(z - s + nz, nz)

    def rows_of(s):
        return pl.ds(pl.multiple_of(chip_of(s) * UT, UT), UT)

    def far(chip):
        s = lax.rem(z - chip + nz, nz)
        return s - (s // (MAXD + 1)) * (2 * s - nz)

    peers = [same(lax.rem(z + t, nz)) for t in range(1, nz)]

    load_q = pltpu.make_async_copy(q_ref, own.at[pl.ds(0, n_q)], loc_sem.at[0])
    load_d = pltpu.make_async_copy(d_ref, own.at[pl.ds(n_q, n_d)], loc_sem.at[1])
    my_cols = pl.ds(pl.multiple_of(c * v_loc, v_loc), v_loc)
    sib_cols = pl.ds(pl.multiple_of((1 - c) * v_loc, v_loc), v_loc)
    load_w = pltpu.make_async_copy(w_ref, wbuf.at[:, my_cols], loc_sem.at[2])
    load_b = pltpu.make_async_copy(b_ref, bias.at[:, my_cols], loc_sem.at[3])
    load_m = pltpu.make_async_copy(msg_ref, msgs.at[z], loc_sem.at[4])
    for cp in (load_q, load_d, load_w, load_b, load_m):
        cp.start()
    xbuf[...] = jnp.zeros_like(xbuf)

    barrier = pltpu.get_barrier_semaphore()
    for dev in [sib] + peers:
        pl.semaphore_signal(barrier, inc=1, device_id=dev, device_id_type=MESH)
    pl.semaphore_wait(barrier, nz)

    send_m = [pltpu.make_async_remote_copy(msg_ref, msgs.at[z], msg_send.at[t], msg_recv.at[t], device_id=peers[t - 1],
                                           device_id_type=MESH) for t in range(1, nz)]
    for cp in send_m:
        cp.start()
    send_w = pltpu.make_async_remote_copy(w_ref, wbuf.at[:, my_cols], w_sem.at[0], w_sem.at[1], device_id=sib,
                                          device_id_type=MESH)
    send_w.start()
    send_b = pltpu.make_async_remote_copy(b_ref, bias.at[:, my_cols], bias_sem.at[0], bias_sem.at[1], device_id=sib,
                                          device_id_type=MESH)
    send_b.start()
    load_q.wait()
    load_d.wait()
    load_m.wait()

    @pl.loop(0, rep.shape[0])
    def _(i):
        rep[i] = jnp.zeros(rep.shape[1:], F32)

    @pl.loop(0, maskx.shape[0])
    def _(i):
        maskx[i] = jnp.zeros(maskx.shape[1:], F32)
    gbacc[...] = jnp.zeros_like(gbacc)

    @pl.loop(0, hid // 64)
    def _(i):
        gw[pl.ds(pl.multiple_of(i * 64, 64), 64), :] = jnp.zeros((64, v_chip), F32)

    for cp in send_m:
        cp.wait()

    units_in_row = 128 // UT
    for s in range(nz):
        for r in range(n_unit // units_in_row):
            tile = jnp.broadcast_to(msgs[chip_of(s), r:r + 1, :], (128, 128)).T
            for i in range(units_in_row):
                maskx[r * units_in_row + i + dist_of(s), rows_of(s), :] = tile[i * UT:(i + 1) * UT, :]

    load_w.wait()
    load_b.wait()

    def in_range(n):
        return (n >= 0) & (n < n_unit)

    def carries(way, dist, n):
        ok = in_range(n)
        if dist == MAXD:
            ok = ok & (lax.rem(n + 2 * n_unit, 2) == way)
        return ok

    def rows_there(way, dist):
        return rows_of(slot(way, dist - 1) if dist > 1 else 0)

    def ag_copy(j, way, dist):
        n = j - (dist - 1)
        b = lax.rem(j, 2)
        here = xbuf.at[b, rows_of(slot(way, dist - 1))] if dist > 1 else own.at[n]
        s = slot(way, dist)
        return pltpu.make_async_remote_copy(here, xbuf.at[1 - b, rows_there(way, dist)], ag_send.at[way, dist - 1],
                                            ag_recv.at[1 - b, s], device_id=ahead[way], device_id_type=MESH)

    def ag_start(j, way, dist):
        n = j - (dist - 1)

        @pl.when(carries(way, dist, n) & (n >= 2 - dist))
        def _():
            pl.semaphore_wait(ag_cred.at[way, dist - 1], 1)

        @pl.when(carries(way, dist, n))
        def _():
            ag_copy(j, way, dist).start()

    def ag_arrive(j, way, dist):
        @pl.when(carries(way, dist, j - dist))
        def _():
            ag_copy(j - 1, way, dist).wait_recv()

    def ag_service(j):
        ag_start(j, 0, 1)
        ag_start(j, 1, 1)
        for dist in range(1, MAXD + 1):
            for way in (0, 1):
                ag_arrive(j, way, dist)
                if dist < MAXD:
                    ag_start(j, way, dist + 1)

        @pl.when(in_range(j))
        def _():
            xbuf[lax.rem(j, 2), rows_of(0)] = own[j]

    def ag_release(j):
        for dist in range(1, MAXD + 1):
            for way in (0, 1):
                @pl.when(carries(way, dist, j - (dist - 1)))
                def _():
                    ag_copy(j, way, dist).wait_send()
        for dist in range(1, MAXD + 1):
            for way in (0, 1):
                n = j - dist + 2

                @pl.when(carries(way, dist, n))
                def _():
                    pl.semaphore_signal(ag_cred.at[way, dist - 1], inc=1, device_id=behind[way], device_id_type=MESH)

    dists = [far(a) for a in range(nz)]

    def rep_row(j, a):
        return (j - dists[a] + MAXD) // per_row

    def fwd_chunk(j, b, c0):
        cols = pl.ds(c0, CH)
        logits = jnp.dot(xbuf[b], wbuf[:, cols], preferred_element_type=F32)
        for t in range(CH // 128):
            at = pl.ds(c0 + t * 128, 128)
            zt = logits[:, t * 128:(t + 1) * 128] + bias[:, at]
            act = jnp.log(1.0 + jnp.maximum(zt, 0.0)) * maskx[j]
            for s in range(nz):
                row_sum = jnp.sum(act[s * UT:(s + 1) * UT, :], axis=0, keepdims=True)
                idx = rep_row(j, s)
                rep[idx, s:s + 1, at] = rep[idx, s:s + 1, at] + row_sum

    send_w.wait()
    send_b.wait()

    @pl.loop(0, n_unit + MAXD)
    def _(j):
        ag_service(j)
        b = lax.rem(j, 2)
        for k in range(n_chunk):
            fwd_chunk(j, b, k * CH)
        ag_release(j)

        @pl.when(j < v_chip // 128)
        def _():
            at = pl.ds(pl.multiple_of(j * 128, 128), 128)
            wt[at, :] = wbuf[:, at].T

    q_total = q_rows * n_group
    d_total = d_rows * n_group
    v_total = v_loc * n_group
    tau = q_len * math.sqrt(v_total * d_len) / 16.0
    lam_q = 4.0 / (v_total * q_len * q_len)
    lam_d = 4.0 / (v_total * d_len * d_len)
    nd = d_rows * nz
    nq = q_rows * nz
    q0 = pad_rows
    d0 = pad_rows + q_rows

    @pl.loop(0, n_chunk)
    def _(k):
        at = pl.ds(pl.multiple_of(k * CH, CH), CH)
        for r in range(d_rows):
            rdx[c, r * nz:(r + 1) * nz, at] = sum(rep[d0 + r * pieces + i, :, at] for i in range(pieces))
        rdx[c, nd:nd + nz, at] = sum(rep[q0 + i, :, at] for i in range(q_rows))

    def to_sib(src, dst, i):
        return pltpu.make_async_remote_copy(src, dst, pair_sem.at[i, 0], pair_sem.at[i, 1], device_id=sib, device_id_type=MESH)

    send_rd = to_sib(rdx.at[c], rdx.at[c], 0)
    send_rd.start()
    send_rd.wait()

    def d_reps(at):
        return jnp.concatenate([rdx[0, 0:nd, at], rdx[1, 0:nd, at]], axis=0)

    def q_mean_of(at):
        return jnp.sum(rdx[0, nd:nd + nz, at] + rdx[1, nd:nd + nz, at], axis=0, keepdims=True) * (1.0 / q_total)

    def d_mean_of(at):
        return jnp.sum(d_reps(at), axis=0, keepdims=True) * (1.0 / d_total)

    def lanes(v):
        return sum(v[:, t * 128:(t + 1) * 128] for t in range(CH // 128))

    def score_chunk(k, carry):
        s_acc, rq, rd = carry
        at = pl.ds(pl.multiple_of(k * CH, CH), CH)
        q_rep = rep[q0:q0 + q_rows, :, at].reshape(nq, CH)
        s_acc = s_acc + lax.dot_general(d_reps(at), q_rep, (((1,), (1,)), ((), ())), precision=HIGHEST,
                                        preferred_element_type=F32)
        qm, dm = q_mean_of(at), d_mean_of(at)
        return s_acc, rq + lanes(qm * qm), rd + lanes(dm * dm)

    score, reg_q, reg_d = lax.fori_loop(0, n_chunk, score_chunk,
                                        (jnp.zeros((2 * nd, nq), F32), jnp.zeros((1, 128), F32), jnp.zeros((1, 128), F32)))
    smsg[0, 0:2 * nd, 0:nq] = score
    smsg[0, 2 * nd:2 * nd + 1, :] = reg_q
    smsg[0, 2 * nd + 1:2 * nd + 2, :] = reg_d
    send_s = [pltpu.make_async_remote_copy(smsg.at[0], smsg.at[t], sm_send.at[t], sm_recv.at[t], device_id=peers[t - 1],
                                           device_id_type=MESH) for t in range(1, nz)]
    for cp in send_s:
        cp.start()

    pos_rows = jnp.concatenate([msgs[s, 7:8, :] for s in range(nz)], axis=0)
    spread = (lax.broadcasted_iota(jnp.int32, (128, nq), 0)
              == lax.broadcasted_iota(jnp.int32, (128, nq), 1) // nz).astype(F32)
    pos_all = jnp.dot(pos_rows, spread, precision=HIGHEST, preferred_element_type=F32)
    pick = (lax.broadcasted_iota(jnp.int32, (nz, nq), 1) % nz == lax.broadcasted_iota(jnp.int32, (nz, nq), 0))
    pos_row = jnp.sum(jnp.where(pick, pos_all, 0.0), axis=0, keepdims=True)
    ridx = lax.broadcasted_iota(jnp.int32, (2 * nd, nq), 0)
    doc = (2 * (ridx % nz) + ridx // nd) * d_rows + (ridx // nz) % d_rows
    target = (doc.astype(F32) == pos_row).astype(F32)

    for cp in send_s:
        cp.wait()
    total = smsg[0]
    for t in range(1, nz):
        total = total + smsg[t]
    scores = total[0:2 * nd, 0:nq] * (1.0 / tau)
    top = jnp.max(scores, axis=0, keepdims=True)
    log_norm = top + jnp.log(jnp.sum(jnp.exp(scores - top), axis=0, keepdims=True))
    row_loss = log_norm - jnp.sum(scores * target, axis=0, keepdims=True)
    loss_part = jnp.sum(row_loss, axis=1, keepdims=True)
    gt = (jnp.exp(scores - log_norm) - target) * (1.0 / (q_total * tau))
    g = gt.T
    lossx[c] = jnp.broadcast_to(loss_part, (8, 128))
    send_l = to_sib(lossx.at[c], lossx.at[c], 1)
    send_l.start()

    @pl.loop(0, n_chunk)
    def _(k):
        at = pl.ds(pl.multiple_of(k * CH, CH), CH)
        q_rep = rep[q0:q0 + q_rows, :, at].reshape(nq, CH)
        dp = jnp.dot(gt, q_rep, precision=HIGHEST, preferred_element_type=F32)
        ddx[0, :, at] = dp[0:nd]
        ddx[1, :, at] = dp[nd:2 * nd]
        gq = jnp.dot(g, d_reps(at), precision=HIGHEST, preferred_element_type=F32) + q_mean_of(at) * (2.0 * lam_q / q_total)
        rep[q0:q0 + q_rows, :, at] = gq.reshape(q_rows, nz, CH)

    send_dd = to_sib(ddx.at[1 - c], ddr, 2)
    send_dd.start()
    send_l.wait()
    reg = (jnp.sum(total[2 * nd:2 * nd + 1, :], axis=1, keepdims=True) * lam_q
           + jnp.sum(total[2 * nd + 1:2 * nd + 2, :], axis=1, keepdims=True) * lam_d)
    lossf[0] = (lossx[0] + lossx[1]) * (1.0 / q_total) + reg

    send_loss = [pltpu.make_async_remote_copy(lossf.at[0], lossf.at[1], loss_send.at[t], loss_recv, device_id=peers[t - 1],
                                              device_id_type=MESH) for t in range(1, nz)]

    @pl.when(z == 0)
    def _():
        for cp in send_loss:
            cp.start()
    send_dd.wait()

    @pl.loop(0, n_chunk)
    def _(k):
        at = pl.ds(pl.multiple_of(k * CH, CH), CH)
        gd = ddx[c, :, at] + ddr[:, at] + d_mean_of(at) * (2.0 * lam_d / d_total)
        for r in range(d_rows):
            for i in range(pieces):
                rep[d0 + r * pieces + i, :, at] = gd[r * nz:(r + 1) * nz]

    def bwd_chunk(j, b, c0):
        cols = pl.ds(c0, CH)
        logits = jnp.dot(xbuf[b], wbuf[:, cols], preferred_element_type=F32)
        low = []
        for t in range(CH // 128):
            at = pl.ds(c0 + t * 128, 128)
            zt = logits[:, t * 128:(t + 1) * 128] + bias[:, at]
            grad = jnp.concatenate([jnp.broadcast_to(rep[rep_row(j, s), s:s + 1, at], (UT, 128)) for s in range(nz)], axis=0)
            gz = jnp.where(zt > 0.0, grad * maskx[j] / (1.0 + jnp.maximum(zt, 0.0)), 0.0)
            gbacc[:, at] = gbacc[:, at] + jnp.sum(gz.reshape(rows // 8, 8, 128), axis=0)
            low.append(gz.astype(BF16))
        low = jnp.concatenate(low, axis=1)
        gbuf[:, cols] = low
        gw[:, cols] = gw[:, cols] + jnp.dot(xt[...], low, preferred_element_type=F32)

    def bwd_hidden():
        for k in range(hid // 256 if hid >= 256 else 1):
            cols = pl.ds(k * 256, min(256, hid))
            pbuf[:, cols] = jnp.dot(gbuf[...], wt[:, cols], preferred_element_type=F32).astype(BF16)

    def rs_unit(j, dist):
        return j - (2 * MAXD - dist)

    def rs_copy(n, way, dist):
        return pltpu.make_async_remote_copy(sbuf.at[way, dist - 1], rbuf.at[way, dist - 1, lax.rem(n + 2 * n_unit, 2)],
                                            rs_send.at[way, dist - 1],
                                            rs_recv.at[way, dist - 1, lax.rem(n + 2 * n_unit, 2)],
                                            device_id=behind[way], device_id_type=MESH)

    def rs_take(n, way, dist):
        rs_copy(n, way, dist + 1).wait_recv()
        return rbuf[way, dist, lax.rem(n + 2 * n_unit, 2)].astype(F32)

    def rs_credit(n, way, dist):
        @pl.when(n + 2 < n_unit)
        def _():
            pl.semaphore_signal(rs_cred.at[way, dist], inc=1, device_id=ahead[way], device_id_type=MESH)

    def rs_send_on(n, way, dist):
        @pl.when(n >= 2)
        def _():
            pl.semaphore_wait(rs_cred.at[way, dist - 1], 1)
        rs_copy(n, way, dist).start()

    def rs_step(j):
        for dist in range(MAXD, 0, -1):
            for way in (0, 1):
                n_before = rs_unit(j - 1, dist)

                @pl.when(carries(way, dist, n_before))
                def _():
                    rs_copy(n_before, way, dist).wait_send()
        for dist in range(MAXD, 0, -1):
            for way in (0, 1):
                n = rs_unit(j, dist)
                s = slot(way, dist)
                if dist == MAXD:
                    @pl.when(carries(way, dist, n))
                    def _():
                        sbuf[way, dist - 1] = pbuf[rows_of(s), :]
                        rs_send_on(n, way, dist)
                elif dist == MAXD - 1:
                    @pl.when(in_range(n) & carries(way, dist + 1, n))
                    def _():
                        mine = part[s, lax.rem(n, 8)].astype(F32)
                        sbuf[way, dist - 1] = (mine + rs_take(n, way, dist)).astype(BF16)
                        rs_credit(n, way, dist)
                        rs_send_on(n, way, dist)

                    @pl.when(in_range(n) & jnp.logical_not(carries(way, dist + 1, n)))
                    def _():
                        sbuf[way, dist - 1] = part[s, lax.rem(n, 8)]
                        rs_send_on(n, way, dist)
                else:
                    @pl.when(in_range(n))
                    def _():
                        mine = part[s, lax.rem(n, 8)].astype(F32)
                        sbuf[way, dist - 1] = (mine + rs_take(n, way, dist)).astype(BF16)
                        rs_credit(n, way, dist)
                        rs_send_on(n, way, dist)
        home = rs_unit(j, 0)

        @pl.when(in_range(home))
        def _():
            acc_h[home] = (acc_h[home].astype(F32) + rs_take(home, 0, 0) + rs_take(home, 1, 0)).astype(BF16)
            rs_credit(home, 0, 0)
            rs_credit(home, 1, 0)

    @pl.loop(0, n_unit + 2 * MAXD)
    def _(j):
        @pl.when(j < n_unit + MAXD)
        def _():
            ag_service(j)
            b = lax.rem(j, 2)
            xt[...] = xbuf[b].T
            for k in range(n_chunk):
                bwd_chunk(j, b, k * CH)
            ag_release(j)
            bwd_hidden()
            for s in range(1, nz):
                if s != MAXD:
                    n = j - dist_of(s)
                    part[s, lax.rem(n + 8, 8)] = pbuf[rows_of(s), :]

            @pl.when(in_range(j))
            def _():
                acc_h[j] = pbuf[rows_of(0), :]
        rs_step(j)

    out_q = pltpu.make_async_copy(acc_h.at[pl.ds(0, n_q)], dq_out, out_sem.at[0])
    out_d = pltpu.make_async_copy(acc_h.at[pl.ds(n_q, n_d)], dd_out, out_sem.at[1])
    out_q.start()
    out_d.start()
    n_part = gx_send.shape[0] - 1
    step = v_loc // n_part
    send_g = []
    for k in range(n_part):
        theirs = pl.ds(pl.multiple_of((1 - c) * v_loc + k * step, step), step)
        send_g.append(pltpu.make_async_remote_copy(gw.at[:, theirs], grecv.at[:, pl.ds(k * step, step)], gx_send.at[k],
                                                   gx_recv.at[k], device_id=sib, device_id_type=MESH))
    send_gb = pltpu.make_async_remote_copy(gbacc.at[:, sib_cols], gbrecv, gx_send.at[n_part], gx_recv.at[n_part], device_id=sib,
                                           device_id_type=MESH)
    for cp in send_g:
        cp.start()
    send_gb.start()
    outs = []
    for k in range(n_part):
        send_g[k].wait_recv()
        at = pl.ds(pl.multiple_of(c * v_loc + k * step, step), step)

        @pl.loop(0, hid // 64)
        def _(i):
            rr = pl.ds(pl.multiple_of(i * 64, 64), 64)
            wbuf[rr, at] = (gw[rr, at] + grecv[rr, pl.ds(k * step, step)]).astype(BF16)
        outs.append(pltpu.make_async_copy(wbuf.at[:, at], gw_out.at[:, pl.ds(k * step, step)], out_sem.at[2 + k]))
        outs[-1].start()
    send_gb.wait_recv()
    gb_ref[...] = jnp.sum(gbacc[:, my_cols] + gbrecv[...], axis=0, keepdims=True)

    @pl.when(z == 0)
    def _():
        for cp in send_loss:
            cp.wait_send()
        loss_ref[...] = lossf[0]

    @pl.when(z != 0)
    def _():
        send_loss[0].wait_recv()
        loss_ref[...] = lossf[1]
    for cp in send_g:
        cp.wait_send()
    send_gb.wait_send()
    out_q.wait()
    out_d.wait()
    for cp in outs:
        cp.wait()


def solution(mesh):
    n_group = mesh.shape['tp']
    nz = n_group // 2
    row_spec = P(('dp', 'tp'))
    mask_spec = P(('dp', 'tp'), None)
    hid_spec = P(('dp', 'tp'), None, None)

    def local_step(q_hidden, d_hidden, q_mask, d_mask, positive, w_head, b_head):
        q_rows, q_len, hid = q_hidden.shape
        d_rows, d_len, _ = d_hidden.shape
        v_loc = w_head.shape[1]
        v_chip = 2 * v_loc
        n_q = q_rows * q_len // UT
        n_d = d_rows * d_len // UT
        n_unit = n_q + n_d
        per_row = q_len // UT
        rows = nz * UT
        nd, nq = d_rows * nz, q_rows * nz
        n_row = (n_unit + 2 * MAXD) // per_row
        flat = jnp.concatenate([q_mask.reshape(-1), d_mask.reshape(-1)]).astype(F32).reshape(-1, 128)
        pos = jnp.pad(positive.astype(F32), (0, 128 - q_rows)).reshape(1, 128)
        msg = jnp.concatenate([flat, jnp.zeros((7 - flat.shape[0], 128), F32), pos], axis=0)
        s_rows = -(-(2 * nd + 2) // 8) * 8
        n_part = 4
        dma, reg = pltpu.SemaphoreType.DMA, pltpu.SemaphoreType.REGULAR
        anym = pl.BlockSpec(memory_space=pl.ANY)
        vm = pl.BlockSpec(memory_space=pltpu.VMEM)
        out_shape = (
            jax.ShapeDtypeStruct((8, 128), F32),
            jax.ShapeDtypeStruct((hid, v_loc), BF16),
            jax.ShapeDtypeStruct((1, v_loc), F32),
            jax.ShapeDtypeStruct((n_q, UT, hid), BF16),
            jax.ShapeDtypeStruct((n_d, UT, hid), BF16),
        )
        scratch = [
            pltpu.VMEM((hid, v_chip), BF16),
            pltpu.VMEM((v_chip, hid), BF16),
            pltpu.VMEM((hid, v_chip), F32),
            pltpu.VMEM((hid, v_loc), F32),
            pltpu.VMEM((n_row, nz, v_chip), F32),
            pltpu.VMEM((n_unit + MAXD, rows, 128), F32),
            pltpu.VMEM((n_unit, UT, hid), BF16),
            pltpu.VMEM((n_unit, UT, hid), BF16),
            pltpu.VMEM((nz, 8, UT, hid), BF16),
            pltpu.VMEM((2, rows, hid), BF16),
            pltpu.VMEM((2, MAXD, 2, UT, hid), BF16),
            pltpu.VMEM((2, MAXD, UT, hid), BF16),
            pltpu.VMEM((rows, v_chip), BF16),
            pltpu.VMEM((rows, hid), BF16),
            pltpu.VMEM((hid, rows), BF16),
            pltpu.VMEM((2, nd + nz, v_chip), F32),
            pltpu.VMEM((2, nd, v_chip), F32),
            pltpu.VMEM((nd, v_chip), F32),
            pltpu.VMEM((1, v_chip), F32),
            pltpu.VMEM((8, v_chip), F32),
            pltpu.VMEM((8, v_loc), F32),
            pltpu.VMEM((nz, 8, 128), F32),
            pltpu.VMEM((nz, s_rows, 128), F32),
            pltpu.VMEM((2, 8, 128), F32),
            pltpu.VMEM((2, 8, 128), F32),
            dma((2, MAXD)), dma((2, nz)), reg((2, MAXD)),
            dma((2, MAXD)), dma((2, MAXD, 2)), reg((2, MAXD)),
            dma((5,)), dma((2,)), dma((2,)), dma((nz,)), dma((nz,)), dma((nz,)), dma((nz,)), dma((3, 2)),
            dma((n_part + 1,)), dma((n_part + 1,)), dma((nz,)), dma, dma((2 + n_part,)),
        ]
        loss, gw, gb, dq, dd = pl.pallas_call(
            functools.partial(kernel, n_group, q_rows, q_len, d_rows, d_len),
            out_shape=out_shape,
            in_specs=[anym] * 5,
            out_specs=(vm, anym, vm, anym, anym),
            scratch_shapes=scratch,
            compiler_params=pltpu.CompilerParams(collective_id=0, has_side_effects=True, vmem_limit_bytes=67043328),
        )(q_hidden.reshape(n_q, UT, hid), d_hidden.reshape(n_d, UT, hid), w_head, b_head.reshape(1, v_loc), msg)
        return (loss[0, 0:1], gw, gb.reshape(v_loc), dq.reshape(q_hidden.shape), dd.reshape(d_hidden.shape))

    return jax.shard_map(local_step, mesh=mesh,
                         in_specs=(hid_spec, hid_spec, mask_spec, mask_spec, row_spec, P(None, 'tp'), P('tp')),
                         out_specs=(P('dp'), P('dp', 'tp'), row_spec, hid_spec, hid_spec),
                         check_vma=False)
```

```python
import functools
import math
import jax
import jax.numpy as jnp
from jax import lax
from jax.experimental import pallas as pl
from jax.experimental.pallas import tpu as pltpu
from jax.sharding import PartitionSpec as P

MESH = pl.DeviceIdType.MESH
HIGHEST = lax.Precision.HIGHEST
F32 = jnp.float32
BF16 = jnp.bfloat16
BWD = UNROLL = True

UT = 16
CH = 512
MAXD = 4
KF = (1, 1, 2, 2, 3, 2, 1, 1)
KB = (1, 1, 1, 2, 2, 2, 1, 1)
LANE, SUB, PAIR, BIG = 128, 8, 2, 64
DEEP = 4
WAYS = (0, 1)
ORDER = (0, 1, 7, 2, 6, 3, 5, 4)
PAD = 4


def kernel(n_group, q_rows, q_len, d_rows, d_len,
           q_ref, d_ref, w_ref, b_ref, msg_ref,
           loss_ref, gw_out, gb_ref, dq_out, dd_out,
           wbuf, wt, gw, grecv, rep, maskx, own, acc_h, part, xbuf, rbuf, sbuf, hbuf, sibp, sst, gbuf, pbuf, xt,
           rdx, ddx, ddr, bias, gbacc, gbrecv, msgs, smsg, lossx, lossf,
           ag_send, ag_recv, ag_cred, inj_send, inj_cred, sib_send, sib_cred,
           rs_send, rs_recv, rs_cred, h_send, h_recv, h_cred, sp_send, sp_recv, sp_cred,
           loc_sem, w_sem, bias_sem, msg_send, msg_recv, sm_send, sm_recv, pair_sem, gx_send, gx_recv,
           loss_send, loss_recv, out_sem):
    ZERO = jnp.int32(0)
    nz = n_group // PAIR
    hid = w_ref.shape[0]
    v_loc = w_ref.shape[1]
    v_chip = PAIR * v_loc
    per_row = q_len // UT
    pieces = d_len // q_len
    n_qpage = q_rows // PAIR
    n_dpage = d_rows // PAIR * pieces
    n_page = n_qpage + n_dpage
    n_unit = n_page * per_row
    br = PAIR * UT
    rows = nz * br
    half = rows // PAIR
    n_chunk = v_chip // CH
    pos = {s: i for i, s in enumerate(ORDER)}

    me = lax.axis_index('tp')
    z = me // PAIR
    c = lax.rem(me, 2)
    o = 1 - c
    right = lax.rem(z + 1, nz)
    left = lax.rem(z + nz - 1, nz)

    def dev(zz, cc):
        return {'tp': PAIR * zz + cc}

    sib = dev(z, o)
    ahead = (right, left)
    behind = (left, right)

    def slot(way, dist):
        return dist if way == 0 else nz - dist

    def dist_of(s):
        return min(s, nz - s)

    def chip_of(s):
        return lax.rem(z - s + nz, nz)

    def block(s):
        return pl.ds(pos[s] * br, br)

    def part_of_block(s, i):
        return pl.ds(pl.multiple_of(pos[s] * br + i * UT, UT), UT)

    def par(n):
        return lax.rem(n + BIG, 2)

    def unit_rows(n):
        return pl.ds(pl.multiple_of(lax.rem(n, per_row) * UT, UT), UT)

    peers = [dev(lax.rem(z + t, nz), c) for t in range(1, nz)]
    others = [dev(lax.rem(z + t, nz), lax.rem(c + u, 2)) for t in range(nz) for u in WAYS if t or u]

    loads = []
    for cc in WAYS:
        loads.append(pltpu.make_async_copy(q_ref.at[:, cc], own.at[cc, pl.ds(0, n_qpage)], loc_sem.at[len(loads)]))
        for r in range(d_rows // PAIR):
            loads.append(pltpu.make_async_copy(d_ref.at[r, cc], own.at[cc, pl.ds(n_qpage + r * pieces, pieces)],
                                               loc_sem.at[len(loads)]))
    my_cols = pl.ds(pl.multiple_of(c * v_loc, v_loc), v_loc)
    sib_cols = pl.ds(pl.multiple_of(o * v_loc, v_loc), v_loc)
    load_m = pltpu.make_async_copy(msg_ref, msgs.at[me], loc_sem.at[len(loads)])
    load_w = pltpu.make_async_copy(w_ref, wbuf.at[:, my_cols], loc_sem.at[len(loads) + 1])
    load_b = pltpu.make_async_copy(b_ref, bias.at[:, my_cols], loc_sem.at[len(loads) + 2])
    for cp in loads + [load_m, load_w, load_b]:
        cp.start()
    xbuf[...] = jnp.zeros_like(xbuf)

    barrier = pltpu.get_barrier_semaphore()
    for d in others:
        pl.semaphore_signal(barrier, device_id=d, device_id_type=MESH)
    pl.semaphore_wait(barrier, n_group - 1)

    def remote(src, dst, ss, rs, to):
        return pltpu.make_async_remote_copy(src, dst, ss, rs, device_id=to, device_id_type=MESH)

    send_m = [remote(msg_ref, msgs.at[me], msg_send.at[k], msg_recv.at[k], d) for k, d in enumerate(others)]
    for cp in send_m:
        cp.start()
    for cp in loads:
        cp.wait()

    def carries(way, dist, n, stop=n_unit):
        ok = (n >= 0) & (n < stop)
        if dist == MAXD:
            ok = ok & (par(n) == way)
        return ok

    def credits_before(k, way, dist, n, bwd):
        later = n >= 3 - k[slot(way, dist) % nz]
        if not bwd:
            return [(later, 1)]
        if dist < MAXD:
            return [(n == 0, 2), (later, 1)]
        return [(n < 2, 1), (later, 1)]

    def wait_credit(sem, k, way, dist, n, bwd):
        for cond, amount in credits_before(k, way, dist, n, bwd):
            @pl.when(cond)
            def _():
                pl.semaphore_wait(sem, amount)

    def hop_copy(k, n, way, dist):
        s, s0 = slot(way, dist), slot(way, dist - 1)
        return remote(xbuf.at[par(n + k[s0]), block(s0)], xbuf.at[par(n + k[s]), block(s)],
                      ag_send.at[way, dist - 1, par(n)], ag_recv.at[par(n + k[s]), s, 0], dev(ahead[way], c))

    def inj_copy(k, n, way, cc, i):
        s = slot(way, 1)
        return remote(own.at[cc, n // per_row, unit_rows(n)], xbuf.at[par(n + k[s]), part_of_block(s, i)],
                      inj_send.at[way, cc], ag_recv.at[par(n + k[s]), s, i], dev(ahead[way], cc))

    def sib_copy(k, n):
        return remote(own.at[o, n // per_row, unit_rows(n)], xbuf.at[par(n + k[0]), part_of_block(0, c)],
                      sib_send, ag_recv.at[par(n + k[0]), 0, 0], sib)

    def inject(k, n, bwd=False):
        @pl.when((n >= 0) & (n < n_unit))
        def _():
            for cc in WAYS:
                for way in WAYS:
                    wait_credit(inj_cred.at[way, cc], k, way, 1, n, bwd)
                    inj_copy(k, n, way, cc, c).start()
            wait_credit(sib_cred, k, 0, 0, n, bwd)
            sib_copy(k, n).start()

    def injected(k, n):
        @pl.when((n >= 0) & (n < n_unit))
        def _():
            for cc in WAYS:
                for way in WAYS:
                    inj_copy(k, n, way, cc, c).wait_send()
            sib_copy(k, n).wait_send()

    def arrive(k, n, way, dist):
        @pl.when(carries(way, dist, n))
        def _():
            if dist == 0:
                sib_copy(k, n).wait_recv()
            elif dist == 1:
                for i in WAYS:
                    inj_copy(k, n, way, 0, i).wait_recv()
            else:
                hop_copy(k, n, way, dist).wait_recv()

    def forward(k, n, way, dist, bwd=False):
        @pl.when(carries(way, dist + 1, n))
        def _():
            wait_credit(ag_cred.at[way, dist], k, way, dist + 1, n, bwd)
            hop_copy(k, n, way, dist + 1).start()

    def relay(k, n, dist, bwd=False):
        for way in WAYS:
            arrive(k, n, way, dist)
            if dist < MAXD:
                forward(k, n, way, dist, bwd)

    def take_own(k, n):
        @pl.when((n >= 0) & (n < n_unit))
        def _():
            xbuf[par(n + k[0]), part_of_block(0, c)] = own[c, n // per_row, unit_rows(n)]

    def give_credit(way, dist, amount=1):
        if dist == 0:
            pl.semaphore_signal(sib_cred, inc=amount, device_id=sib, device_id_type=MESH)
        elif dist == 1:
            for i in WAYS:
                pl.semaphore_signal(inj_cred.at[way, c], inc=amount, device_id=dev(behind[way], i), device_id_type=MESH)
        else:
            pl.semaphore_signal(ag_cred.at[way, dist - 1], inc=amount, device_id=dev(behind[way], c), device_id_type=MESH)

    def lanes_of(s):
        if s == 0:
            return ((0, 0),)
        if s == MAXD:
            return ((0, MAXD), (1, MAXD))
        return ((0, s),) if s < MAXD else ((1, nz - s),)

    def release(k, j, slots):
        for s in slots:
            for way, dist in lanes_of(s):
                n = j - k[s]
                if 1 <= dist < MAXD:
                    @pl.when(carries(way, dist + 1, n))
                    def _():
                        hop_copy(k, n, way, dist + 1).wait_send()
        for s in slots:
            for way, dist in lanes_of(s):
                @pl.when(carries(way, dist, j - k[s] + 2))
                def _():
                    give_credit(way, dist)

    near, far = ORDER[:nz // PAIR], ORDER[nz // PAIR:]

    inject(KF, ZERO)

    @pl.loop(0, rep.shape[0])
    def _(i):
        rep[i] = jnp.zeros(rep.shape[1:], F32)

    @pl.loop(0, PAD)
    def _(i):
        maskx[i] = jnp.zeros(maskx.shape[1:], F32)
        maskx[PAD + n_unit + i] = jnp.zeros(maskx.shape[1:], F32)
    gbacc[...] = jnp.zeros_like(gbacc)

    @pl.loop(0, hid // BIG)
    def _(i):
        gw[pl.ds(pl.multiple_of(i * BIG, BIG), BIG), :] = jnp.zeros((BIG, v_chip), F32)

    load_m.wait()
    for cp in send_m:
        cp.wait()
    send_w = remote(w_ref, wbuf.at[:, my_cols], w_sem.at[0], w_sem.at[1], sib)
    send_w.start()
    send_b = remote(b_ref, bias.at[:, my_cols], bias_sem.at[0], bias_sem.at[1], sib)
    send_b.start()

    in_row = LANE // UT
    for s in range(nz):
        for i in WAYS:
            for r in range(n_unit // in_row):
                tile = jnp.broadcast_to(msgs[PAIR * chip_of(s) + i, c, r:r + 1, :], (LANE, LANE)).T
                for t in range(in_row):
                    at = pos[s] * br + i * UT
                    maskx[PAD + r * in_row + t, at:at + UT, :] = tile[t * UT:(t + 1) * UT, :]

    relay(KF, ZERO, 1)
    injected(KF, ZERO)
    load_w.wait()
    load_b.wait()
    send_w.wait()
    send_b.wait()

    def pages(j, k):
        after = {d: (j - d + PAD) // per_row for d in set(k)}
        return [after[k[s]] for s in range(nz)]

    def mask_rows(j, k, slots):
        return jnp.concatenate([maskx[j - k[s] + PAD, block(s), :] for s in slots], axis=0)

    def fwd_group(j, b, g, k0, k1):
        slots = (near, far)[g]
        page = pages(j, KF)

        @functools.partial(lax.fori_loop, k0, k1, init_val=None, unroll=UNROLL)
        def _(k, _):
            at = pl.ds(pl.multiple_of(k * CH, CH), CH)
            logits = jnp.dot(xbuf[b, g * half:(g + 1) * half], wbuf[:, at], preferred_element_type=F32)
            for t in range(CH // LANE):
                at = pl.ds(pl.multiple_of(k * CH + t * LANE, LANE), LANE)
                zt = logits[:, t * LANE:(t + 1) * LANE] + bias[:, at]
                act = jnp.log(1.0 + jnp.maximum(zt, 0.0)) * mask_rows(j, KF, slots)
                for i, s in enumerate(slots):
                    for u in WAYS:
                        r0 = i * br + u * UT
                        row_sum = jnp.sum(act[r0:r0 + UT, :], axis=0, keepdims=True)
                        rep[page[s], PAIR * s + u:PAIR * s + u + 1, at] = rep[page[s], PAIR * s + u:PAIR * s + u + 1, at] + row_sum

    def cut(eighths):
        return n_chunk * eighths // SUB

    fwd_end = n_unit + KF[MAXD]

    def release_far(j):
        @pl.when(j >= 1)
        def _():
            release(KF, j, far)

    @pl.loop(1, fwd_end)
    def _(j):
        b = par(j)
        release_far(j - 1)
        inject(KF, j)
        take_own(KF, j - KF[0])
        arrive(KF, j - KF[0], 0, 0)
        fwd_group(j, b, 0, 0, cut(6))
        relay(KF, j - 2, 3)
        fwd_group(j, b, 0, cut(6), n_chunk)
        release(KF, j, near)
        relay(KF, j - 1, 2)
        relay(KF, j - 3, 4)
        fwd_group(j, b, 1, 0, cut(4))
        relay(KF, j, 1)
        fwd_group(j, b, 1, cut(4), n_chunk)
        injected(KF, j)

        @pl.when(j <= v_chip // 256)
        def _():
            for u in WAYS:
                at = pl.ds(pl.multiple_of((j - 1) * 256 + u * LANE, LANE), LANE)
                wt[at, :] = wbuf[:, at].T

    release_far(jnp.int32(fwd_end - 1))

    for s in range(nz):
        for way, dist in lanes_of(s):
            give_credit(way, dist, 2 if dist < MAXD else 1)

    q_total = q_rows * n_group
    d_total = d_rows * n_group
    v_total = v_loc * n_group
    tau = q_len * math.sqrt(v_total * d_len) / 16.0
    lam_q = 4.0 / (v_total * q_len * q_len)
    lam_d = 4.0 / (v_total * d_len * d_len)
    nd = d_rows // PAIR * n_group
    nq = q_rows // PAIR * n_group
    q0 = PAD // per_row
    d0 = q0 + n_qpage

    @pl.loop(0, n_chunk)
    def _(k):
        at = pl.ds(pl.multiple_of(k * CH, CH), CH)
        for r in range(d_rows // PAIR):
            rdx[c, r * n_group:(r + 1) * n_group, at] = sum(rep[d0 + r * pieces + i, :, at] for i in range(pieces))
        q_sum = sum(rep[q0 + i, :, at] for i in range(n_qpage))
        rdx[c, nd:nd + SUB, at] = sum(q_sum[i * SUB:(i + 1) * SUB] for i in range(n_group // SUB))

    def to_sib(src, dst, i):
        return remote(src, dst, pair_sem.at[i, 0], pair_sem.at[i, 1], sib)

    send_rd = to_sib(rdx.at[c], rdx.at[c], 0)
    send_rd.start()
    inject(KB, ZERO, BWD)
    send_rd.wait()

    def d_reps(at):
        return jnp.concatenate([rdx[0, 0:nd, at], rdx[1, 0:nd, at]], axis=0)

    def q_mean_of(at):
        return jnp.sum(rdx[0, nd:nd + SUB, at] + rdx[1, nd:nd + SUB, at], axis=0, keepdims=True) * (1.0 / q_total)

    def d_mean_of(at):
        return jnp.sum(d_reps(at), axis=0, keepdims=True) * (1.0 / d_total)

    def lanes(v):
        return sum(v[:, t * LANE:(t + 1) * LANE] for t in range(CH // LANE))

    def score_chunk(k, carry):
        s_acc, rq, rd = carry
        at = pl.ds(pl.multiple_of(k * CH, CH), CH)
        q_rep = rep[q0:q0 + n_qpage, :, at].reshape(nq, CH)
        s_acc = s_acc + lax.dot_general(d_reps(at), q_rep, (((1,), (1,)), ((), ())), precision=HIGHEST,
                                        preferred_element_type=F32)
        qm, dm = q_mean_of(at), d_mean_of(at)
        return s_acc, rq + lanes(qm * qm), rd + lanes(dm * dm)

    score, reg_q, reg_d = lax.fori_loop(0, n_chunk, score_chunk,
                                        (jnp.zeros((PAIR * nd, nq), F32), jnp.zeros((1, LANE), F32), jnp.zeros((1, LANE), F32)))

    def turn(n):
        i = lax.broadcasted_iota(jnp.int32, (n, n), 0)
        k = lax.broadcasted_iota(jnp.int32, (n, n), 1)
        same = (i // n_group == k // n_group) & (i % 2 == k % 2)
        return (same & (((i // PAIR) % nz + (k // PAIR) % nz) % nz == z)).astype(F32)

    def exact(a, b):
        return jnp.dot(a, b, precision=HIGHEST, preferred_element_type=F32)

    turn_d, turn_q = turn(PAIR * nd), turn(nq)
    smsg[0, 0:PAIR * nd, 0:nq] = exact(exact(turn_d, score), turn_q)
    smsg[0, PAIR * nd:PAIR * nd + 1, :] = reg_q
    smsg[0, PAIR * nd + 1:PAIR * nd + 2, :] = reg_d
    send_s = [remote(smsg.at[0], smsg.at[t], sm_send.at[t], sm_recv.at[t], peers[t - 1]) for t in range(1, nz)]
    for cp in send_s:
        cp.start()

    pos_rows = jnp.concatenate([msgs[i, 0, 3:4, :] for i in range(n_group)], axis=0)
    spread = (lax.broadcasted_iota(jnp.int32, (LANE, nq), 0)
              == PAIR * (lax.broadcasted_iota(jnp.int32, (LANE, nq), 1) // n_group) + c).astype(F32)
    pos_all = exact(pos_rows, spread)
    pick = (lax.broadcasted_iota(jnp.int32, (n_group, nq), 1) % n_group
            == lax.broadcasted_iota(jnp.int32, (n_group, nq), 0))
    pos_row = jnp.sum(jnp.where(pick, pos_all, 0.0), axis=0, keepdims=True)
    ridx = lax.broadcasted_iota(jnp.int32, (PAIR * nd, nq), 0)
    doc = (ridx % n_group) * d_rows + PAIR * ((ridx % nd) // n_group) + ridx // nd
    target = (doc.astype(F32) == pos_row).astype(F32)

    relay(KB, ZERO, 1, BWD)
    injected(KB, ZERO)
    for cp in send_s:
        cp.wait()
    total = smsg[0]
    for t in range(1, nz):
        total = total + smsg[t]
    scores = total[0:PAIR * nd, 0:nq] * (1.0 / tau)
    top = jnp.max(scores, axis=0, keepdims=True)
    log_norm = top + jnp.log(jnp.sum(jnp.exp(scores - top), axis=0, keepdims=True))
    row_loss = log_norm - jnp.sum(scores * target, axis=0, keepdims=True)
    loss_part = jnp.sum(row_loss, axis=1, keepdims=True)
    gt = (jnp.exp(scores - log_norm) - target) * (1.0 / (q_total * tau))
    gt = exact(exact(turn_d, gt), turn_q)
    g = gt.T
    lossx[c] = jnp.broadcast_to(loss_part, (SUB, LANE))
    send_l = to_sib(lossx.at[c], lossx.at[c], 1)
    send_l.start()
    inject(KB, ZERO + 1, BWD)
    relay(KB, ZERO, 2, BWD)

    @pl.loop(0, n_chunk)
    def _(k):
        at = pl.ds(pl.multiple_of(k * CH, CH), CH)
        q_rep = rep[q0:q0 + n_qpage, :, at].reshape(nq, CH)
        dp = exact(gt, q_rep)
        ddx[0, :, at] = dp[0:nd]
        ddx[1, :, at] = dp[nd:PAIR * nd]
        gq = exact(g, d_reps(at)) + q_mean_of(at) * (2.0 * lam_q / q_total)
        rep[q0:q0 + n_qpage, :, at] = gq.reshape(n_qpage, n_group, CH)

    send_dd = to_sib(ddx.at[o], ddr, 2)
    send_dd.start()
    send_l.wait()
    reg = (jnp.sum(total[PAIR * nd:PAIR * nd + 1, :], axis=1, keepdims=True) * lam_q
           + jnp.sum(total[PAIR * nd + 1:PAIR * nd + 2, :], axis=1, keepdims=True) * lam_d)
    lossf[0] = (lossx[0] + lossx[1]) * (1.0 / q_total) + reg

    send_loss = [remote(lossf.at[0], lossf.at[1], loss_send.at[t], loss_recv, peers[t - 1]) for t in range(1, nz)]

    @pl.when(z == 0)
    def _():
        for cp in send_loss:
            cp.start()
    relay(KB, ZERO + 1, 1, BWD)
    injected(KB, ZERO + 1)
    relay(KB, ZERO, 3, BWD)
    send_dd.wait()

    @pl.loop(0, n_chunk)
    def _(k):
        at = pl.ds(pl.multiple_of(k * CH, CH), CH)
        gd = ddx[c, :, at] + ddr[:, at] + d_mean_of(at) * (2.0 * lam_d / d_total)
        for r in range(d_rows // PAIR):
            for i in range(pieces):
                rep[d0 + r * pieces + i, :, at] = gd[r * n_group:(r + 1) * n_group]

    def bwd_chunk(j, b, page, k):
        cols = pl.ds(pl.multiple_of(k * CH, CH), CH)
        logits = jnp.dot(xbuf[b], wbuf[:, cols], preferred_element_type=F32)
        low = []
        for t in range(CH // LANE):
            at = pl.ds(pl.multiple_of(k * CH + t * LANE, LANE), LANE)
            zt = logits[:, t * LANE:(t + 1) * LANE] + bias[:, at]
            grad = jnp.concatenate([jnp.broadcast_to(rep[page[s], PAIR * s + u:PAIR * s + u + 1, at], (UT, LANE))
                                    for s in ORDER for u in WAYS], axis=0)
            gz = jnp.where(zt > 0.0, grad * mask_rows(j, KB, ORDER) / (1.0 + jnp.maximum(zt, 0.0)), 0.0)
            gbacc[:, at] = gbacc[:, at] + jnp.sum(gz.reshape(rows // SUB, SUB, LANE), axis=0)
            low.append(gz.astype(BF16))
        low = jnp.concatenate(low, axis=1)
        gbuf[:, cols] = low
        gw[:, cols] = gw[:, cols] + jnp.dot(xt[...], low, preferred_element_type=F32)

    def bwd_hidden(k0, k1):
        wide = hid // 4

        @functools.partial(lax.fori_loop, k0, k1, init_val=None, unroll=UNROLL)
        def _(k, _):
            cols = pl.ds(pl.multiple_of(k * wide, wide), wide)
            pbuf[:, cols] = jnp.dot(gbuf[...], wt[:, cols], preferred_element_type=F32).astype(BF16)

    def deep(n):
        return lax.rem(n + BIG, DEEP)

    def rs_copy(n, way, dist):
        return remote(sbuf.at[way, dist - 1], rbuf.at[way, dist - 2, deep(n)], rs_send.at[way, dist - 1],
                      rs_recv.at[way, dist - 2, deep(n)], dev(behind[way], c))

    def home_copy(n, way, cc, i):
        return remote(sbuf.at[way, 0, pl.ds(i * UT, UT)], hbuf.at[way, cc, deep(n)], h_send.at[way, i],
                      h_recv.at[way, cc, deep(n)], dev(behind[way], i))

    def pair_copy(n):
        return remote(sst.at[par(n)], sibp.at[par(n)], sp_send.at[par(n)], sp_recv.at[par(n)], sib)

    def rs_sent(n, way, dist):
        @pl.when(carries(way, dist, n))
        def _():
            if dist == 1:
                for i in WAYS:
                    home_copy(n, way, c, i).wait_send()
            else:
                rs_copy(n, way, dist).wait_send()

    def rs_go(n, way, dist):
        @pl.when(n >= DEEP)
        def _():
            if dist == 1:
                for i in WAYS:
                    pl.semaphore_wait(h_cred.at[way, i])
            else:
                pl.semaphore_wait(rs_cred.at[way, dist - 1])
        if dist == 1:
            for i in WAYS:
                home_copy(n, way, c, i).start()
        else:
            rs_copy(n, way, dist).start()

    def rs_event(n, way, dist):
        s = slot(way, dist)
        rs_sent(n - (2 if dist == MAXD else 1), way, dist)
        mine = (lambda: pbuf[block(s), :]) if dist == MAXD else (lambda: part[s, deep(n)])
        incoming = carries(way, dist + 1, n) if dist + 1 <= MAXD else None
        if dist == MAXD:
            alone, joined = carries(way, dist, n), None
        elif dist + 1 == MAXD:
            alone, joined = carries(way, dist, n) & (par(n) != way), incoming
        else:
            alone, joined = None, incoming
        if alone is not None:
            @pl.when(alone)
            def _():
                sbuf[way, dist - 1] = mine()
                rs_go(n, way, dist)
        if joined is not None:
            @pl.when(joined)
            def _():
                rs_copy(n, way, dist + 1).wait_recv()
                got = rbuf[way, dist - 1, deep(n)]
                sbuf[way, dist - 1] = (mine().astype(F32) + got.astype(F32)).astype(BF16)

                @pl.when(n + DEEP < n_unit)
                def _():
                    pl.semaphore_signal(rs_cred.at[way, dist], device_id=dev(ahead[way], c), device_id_type=MESH)
                rs_go(n, way, dist)

    def rs_home(n):
        @pl.when((n >= 0) & (n < n_unit))
        def _():
            for cc in WAYS:
                for way in WAYS:
                    home_copy(n, way, cc, 0).wait_recv()
                at = unit_rows(n)
                acc_h[cc, n // per_row, at] = (acc_h[cc, n // per_row, at].astype(F32) + hbuf[0, cc, deep(n)].astype(F32)
                                               + hbuf[1, cc, deep(n)].astype(F32)).astype(BF16)

                @pl.when(n + DEEP < n_unit)
                def _():
                    for way in WAYS:
                        pl.semaphore_signal(h_cred.at[way, c], device_id=dev(ahead[way], cc), device_id_type=MESH)

    def pair_send(n):
        @pl.when((n >= 2) & (n < n_unit + 2))
        def _():
            pair_copy(n - 2).wait_send()

        @pl.when((n >= 0) & (n < n_unit))
        def _():
            sst[par(n)] = pbuf[part_of_block(0, o), :]

            @pl.when(n >= 2)
            def _():
                pl.semaphore_wait(sp_cred)
            pair_copy(n).start()
            acc_h[c, n // per_row, unit_rows(n)] = pbuf[part_of_block(0, c), :]

    def pair_take(n):
        @pl.when((n >= 0) & (n < n_unit))
        def _():
            pair_copy(n).wait_recv()
            acc_h[o, n // per_row, unit_rows(n)] = sibp[par(n)]

            @pl.when(n + 2 < n_unit)
            def _():
                pl.semaphore_signal(sp_cred, device_id=sib, device_id_type=MESH)

    last = n_unit + KB[MAXD]

    def rs_both(n, dist):
        for way in WAYS:
            rs_event(n, way, dist)

    @pl.loop(1, last)
    def _(j):
        b = par(j)
        page = pages(j, KB)

        def weights(k0, k1):
            @functools.partial(lax.fori_loop, k0, k1, init_val=None, unroll=UNROLL)
            def _(k, _):
                bwd_chunk(j, b, page, k)

        relay(KB, j - 2, 4)
        take_own(KB, j - 1)
        arrive(KB, j - 1, 0, 0)
        rs_both(j - 3, 4)
        rs_both(j - 5, 1)
        xt[...] = xbuf[b].T
        weights(0, cut(4))

        @pl.when(j >= 2)
        def _():
            relay(KB, j, 1, BWD)
        rs_both(j - 4, 2)
        weights(cut(4), cut(6))

        @pl.when(j >= 2)
        def _():
            relay(KB, j - 1, 3, BWD)
        weights(cut(6), n_chunk)
        release(KB, j, ORDER)
        rs_both(j - 3, 3)
        bwd_hidden(0, 3)

        @pl.when(j >= 2)
        def _():
            injected(KB, j)
        inject(KB, j + 1, BWD)
        relay(KB, j, 2, BWD)
        rs_home(j - 5)
        bwd_hidden(3, 4)
        for s in range(1, nz):
            if s != MAXD:
                part[s, deep(j - KB[s])] = pbuf[block(s), :]
        pair_send(j - 1)
        pair_take(j - 2)

    n_part = gx_send.shape[0] - 1
    step = v_loc // n_part
    send_g = []
    for k in range(n_part):
        theirs = pl.ds(pl.multiple_of(o * v_loc + k * step, step), step)
        send_g.append(remote(gw.at[:, theirs], grecv.at[:, pl.ds(k * step, step)], gx_send.at[k], gx_recv.at[k], sib))
    send_gb = remote(gbacc.at[:, sib_cols], gbrecv, gx_send.at[n_part], gx_recv.at[n_part], sib)
    for cp in send_g:
        cp.start()
    send_gb.start()

    @pl.loop(last, n_unit + 5)
    def _(j):
        rs_both(j - 3, 4)
        rs_both(j - 5, 1)
        rs_both(j - 4, 2)
        rs_both(j - 3, 3)
        pair_send(j - 1)
        rs_home(j - 5)
    for way in WAYS:
        rs_sent(jnp.int32(n_unit - 1), way, 1)

    outs = []
    for cc in WAYS:
        outs.append(pltpu.make_async_copy(acc_h.at[cc, pl.ds(0, n_qpage)], dq_out.at[:, cc], out_sem.at[len(outs)]))
        for r in range(d_rows // PAIR):
            outs.append(pltpu.make_async_copy(acc_h.at[cc, pl.ds(n_qpage + r * pieces, pieces)], dd_out.at[r, cc],
                                              out_sem.at[len(outs)]))
    for cp in outs:
        cp.start()
    for k in range(n_part):
        send_g[k].wait_recv()
        at = pl.ds(pl.multiple_of(c * v_loc + k * step, step), step)

        @pl.loop(0, hid // BIG)
        def _(i):
            rr = pl.ds(pl.multiple_of(i * BIG, BIG), BIG)
            wbuf[rr, at] = (gw[rr, at] + grecv[rr, pl.ds(k * step, step)]).astype(BF16)
        outs.append(pltpu.make_async_copy(wbuf.at[:, at], gw_out.at[:, pl.ds(k * step, step)], out_sem.at[len(outs)]))
        outs[-1].start()
    send_gb.wait_recv()
    gb_ref[...] = jnp.sum(gbacc[:, my_cols] + gbrecv[...], axis=0, keepdims=True)

    @pl.when(z == 0)
    def _():
        for cp in send_loss:
            cp.wait_send()
        loss_ref[...] = lossf[0]

    @pl.when(z != 0)
    def _():
        send_loss[0].wait_recv()
        loss_ref[...] = lossf[1]
    for cp in send_g:
        cp.wait_send()
    send_gb.wait_send()
    for cp in outs:
        cp.wait()


def solution(mesh):
    n_group = mesh.shape['tp']
    nz = n_group // PAIR
    row_spec = P(('dp', 'tp'))
    mask_spec = P(('dp', 'tp'), None)
    hid_spec = P(('dp', 'tp'), None, None)

    def local_step(q_hidden, d_hidden, q_mask, d_mask, positive, w_head, b_head):
        q_rows, q_len, hid = q_hidden.shape
        d_rows, d_len, _ = d_hidden.shape
        v_loc = w_head.shape[1]
        v_chip = PAIR * v_loc
        per_row = q_len // UT
        pieces = d_len // q_len
        n_page = q_rows // PAIR + d_rows // PAIR * pieces
        n_unit = n_page * per_row
        rows = nz * PAIR * UT
        nd, nq = d_rows // PAIR * n_group, q_rows // PAIR * n_group
        by_core = jnp.concatenate([jnp.swapaxes(q_mask.reshape(q_rows // PAIR, 2, q_len), 0, 1).reshape(2, -1),
                                   jnp.swapaxes(d_mask.reshape(d_rows // PAIR, 2, d_len), 0, 1).reshape(2, -1)], axis=1)
        by_core = by_core.astype(F32).reshape(2, -1, LANE)
        by_core = jnp.pad(by_core, ((0, 0), (0, 3 - by_core.shape[1]), (0, 0)))
        where = jnp.pad(positive.astype(F32), (0, LANE - q_rows)).reshape(1, 1, LANE)
        msg = jnp.concatenate([by_core, jnp.broadcast_to(where, (2, 1, LANE))], axis=1)
        s_rows = -(-(PAIR * nd + 2) // SUB) * SUB
        n_part = 4 if v_loc >= 512 else 2
        n_load = PAIR * (1 + d_rows // PAIR)
        dma, reg = pltpu.SemaphoreType.DMA, pltpu.SemaphoreType.REGULAR
        anym = pl.BlockSpec(memory_space=pl.ANY)
        vm = pl.BlockSpec(memory_space=pltpu.VMEM)
        q_shape = (q_rows // PAIR, 2, q_len, hid)
        d_shape = (d_rows // PAIR, 2, pieces, q_len, hid)
        out_shape = (
            jax.ShapeDtypeStruct((SUB, LANE), F32),
            jax.ShapeDtypeStruct((hid, v_loc), BF16),
            jax.ShapeDtypeStruct((1, v_loc), F32),
            jax.ShapeDtypeStruct(q_shape, BF16),
            jax.ShapeDtypeStruct(d_shape, BF16),
        )
        scratch = [
            pltpu.VMEM((hid, v_chip), BF16),
            pltpu.VMEM((v_chip, hid), BF16),
            pltpu.VMEM((hid, v_chip), F32),
            pltpu.VMEM((hid, v_loc), F32),
            pltpu.VMEM(((n_unit + PAIR * PAD) // per_row, n_group, v_chip), F32),
            pltpu.VMEM((n_unit + PAIR * PAD, rows, LANE), F32),
            pltpu.VMEM((PAIR, n_page, q_len, hid), BF16),
            pltpu.VMEM((PAIR, n_page, q_len, hid), BF16),
            pltpu.VMEM((nz, DEEP, PAIR * UT, hid), BF16),
            pltpu.VMEM((PAIR, rows, hid), BF16),
            pltpu.VMEM((PAIR, MAXD - 1, DEEP, PAIR * UT, hid), BF16),
            pltpu.VMEM((PAIR, MAXD, PAIR * UT, hid), BF16),
            pltpu.VMEM((PAIR, 2, DEEP, UT, hid), BF16),
            pltpu.VMEM((PAIR, UT, hid), BF16),
            pltpu.VMEM((PAIR, UT, hid), BF16),
            pltpu.VMEM((rows, v_chip), BF16),
            pltpu.VMEM((rows, hid), BF16),
            pltpu.VMEM((hid, rows), BF16),
            pltpu.VMEM((PAIR, nd + SUB, v_chip), F32),
            pltpu.VMEM((PAIR, nd, v_chip), F32),
            pltpu.VMEM((nd, v_chip), F32),
            pltpu.VMEM((1, v_chip), F32),
            pltpu.VMEM((SUB, v_chip), F32),
            pltpu.VMEM((SUB, v_loc), F32),
            pltpu.VMEM((n_group, 2, 4, LANE), F32),
            pltpu.VMEM((nz, s_rows, LANE), F32),
            pltpu.VMEM((PAIR, SUB, LANE), F32),
            pltpu.VMEM((PAIR, SUB, LANE), F32),
            dma((PAIR, MAXD, 2)), dma((PAIR, nz, 2)), reg((PAIR, MAXD)), dma((PAIR, 2)), reg((PAIR, 2)), dma, reg,
            dma((PAIR, MAXD)), dma((PAIR, MAXD - 1, DEEP)), reg((PAIR, MAXD)), dma((PAIR, 2)), dma((PAIR, 2, DEEP)), reg((PAIR, 2)),
            dma((PAIR,)), dma((PAIR,)), reg,
            dma((n_load + 3,)), dma((PAIR,)), dma((PAIR,)), dma((n_group - 1,)), dma((n_group - 1,)), dma((nz,)), dma((nz,)),
            dma((3, 2)), dma((n_part + 1,)), dma((n_part + 1,)), dma((nz,)), dma, dma((n_load + n_part,)),
        ]
        loss, gw, gb, dq, dd = pl.pallas_call(
            functools.partial(kernel, n_group, q_rows, q_len, d_rows, d_len),
            out_shape=out_shape,
            in_specs=[anym] * 5,
            out_specs=(vm, anym, vm, anym, anym),
            scratch_shapes=scratch,
            compiler_params=pltpu.CompilerParams(collective_id=0, has_side_effects=True, vmem_limit_bytes=67043328),
        )(q_hidden.reshape(q_shape), d_hidden.reshape(d_shape), w_head, b_head.reshape(1, v_loc), msg)
        return (loss[0, 0:1], gw, gb.reshape(v_loc), dq.reshape(q_hidden.shape), dd.reshape(d_hidden.shape))

    return jax.shard_map(local_step, mesh=mesh,
                         in_specs=(hid_spec, hid_spec, mask_spec, mask_spec, row_spec, P(None, 'tp'), P('tp')),
                         out_specs=(P('dp'), P('dp', 'tp'), row_spec, hid_spec, hid_spec),
                         check_vma=False)
```

```python
import functools
import math
import jax
import jax.numpy as jnp
from jax import lax
from jax.experimental import pallas as pl
from jax.experimental.pallas import tpu as pltpu
from jax.sharding import PartitionSpec as P

MESH = pl.DeviceIdType.MESH
HIGHEST = lax.Precision.HIGHEST
F32 = jnp.float32
BF16 = jnp.bfloat16
BWD = UNROLL = True

UT = 16
CH = 512
CB = 1024
MAXD = 4
KF = (1, 1, 2, 2, 3, 2, 1, 1)
KB = (1, 1, 1, 2, 2, 2, 1, 1)
LANE, SUB, PAIR, BIG = 128, 8, 2, 64
DEEP = 4
WAYS = (0, 1)
ORDER = (0, 1, 7, 2, 6, 3, 5, 4)
PAD = 4


def kernel(n_group, q_rows, q_len, d_rows, d_len,
           q_ref, d_ref, w_ref, b_ref, msg_ref,
           loss_ref, gw_out, gb_ref, dq_out, dd_out,
           wbuf, wt, gw, grecv, rep, maskx, own, acc_h, part, xbuf, rbuf, sbuf, hbuf, sibp, sst, gbuf, pbuf, xt,
           rdx, ddx, ddr, bias, gbacc, gbrecv, msgs, smsg, lossx, lossf,
           ag_send, ag_recv, ag_cred, inj_send, inj_cred, sib_send, sib_cred,
           rs_send, rs_recv, rs_cred, h_send, h_recv, h_cred, sp_send, sp_recv, sp_cred,
           loc_sem, w_sem, bias_sem, msg_send, msg_recv, sm_send, sm_recv, pair_sem, gx_send, gx_recv, gx_cred,
           loss_send, loss_recv, out_sem):
    ZERO = jnp.int32(0)
    nz = n_group // PAIR
    hid = w_ref.shape[0]
    v_loc = w_ref.shape[1]
    v_chip = PAIR * v_loc
    per_row = q_len // UT
    pieces = d_len // q_len
    n_qpage = q_rows // PAIR
    n_dpage = d_rows // PAIR * pieces
    n_page = n_qpage + n_dpage
    n_unit = n_page * per_row
    br = PAIR * UT
    rows = nz * br
    half = rows // PAIR
    n_chunk = v_chip // CH
    pos = {s: i for i, s in enumerate(ORDER)}

    me = lax.axis_index('tp')
    z = me // PAIR
    c = lax.rem(me, 2)
    o = 1 - c
    right = lax.rem(z + 1, nz)
    left = lax.rem(z + nz - 1, nz)

    def dev(zz, cc):
        return {'tp': PAIR * zz + cc}

    sib = dev(z, o)
    ahead = (right, left)
    behind = (left, right)

    def slot(way, dist):
        return dist if way == 0 else nz - dist

    def dist_of(s):
        return min(s, nz - s)

    def chip_of(s):
        return lax.rem(z - s + nz, nz)

    def block(s):
        return pl.ds(pos[s] * br, br)

    def part_of_block(s, i):
        return pl.ds(pl.multiple_of(pos[s] * br + i * UT, UT), UT)

    def par(n):
        return lax.rem(n + BIG, 2)

    def unit_rows(n):
        return pl.ds(pl.multiple_of(lax.rem(n, per_row) * UT, UT), UT)

    peers = [dev(lax.rem(z + t, nz), c) for t in range(1, nz)]
    others = [dev(lax.rem(z + t, nz), lax.rem(c + u, 2)) for t in range(nz) for u in WAYS if t or u]

    loads = []
    for cc in WAYS:
        loads.append(pltpu.make_async_copy(q_ref.at[:, cc], own.at[cc, pl.ds(0, n_qpage)], loc_sem.at[len(loads)]))
        for r in range(d_rows // PAIR):
            loads.append(pltpu.make_async_copy(d_ref.at[r, cc], own.at[cc, pl.ds(n_qpage + r * pieces, pieces)],
                                               loc_sem.at[len(loads)]))
    my_cols = pl.ds(pl.multiple_of(c * v_loc, v_loc), v_loc)
    sib_cols = pl.ds(pl.multiple_of(o * v_loc, v_loc), v_loc)
    load_m = pltpu.make_async_copy(msg_ref, msgs.at[me], loc_sem.at[len(loads)])
    load_w = pltpu.make_async_copy(w_ref, wbuf.at[:, my_cols], loc_sem.at[len(loads) + 1])
    load_b = pltpu.make_async_copy(b_ref, bias.at[:, my_cols], loc_sem.at[len(loads) + 2])
    for cp in loads + [load_m, load_w, load_b]:
        cp.start()
    xbuf[...] = jnp.zeros_like(xbuf)

    barrier = pltpu.get_barrier_semaphore()
    for d in others:
        pl.semaphore_signal(barrier, device_id=d, device_id_type=MESH)
    pl.semaphore_wait(barrier, n_group - 1)

    def remote(src, dst, ss, rs, to):
        return pltpu.make_async_remote_copy(src, dst, ss, rs, device_id=to, device_id_type=MESH)

    send_m = [remote(msg_ref, msgs.at[me], msg_send.at[k], msg_recv.at[k], d) for k, d in enumerate(others)]
    for cp in send_m:
        cp.start()
    send_w = remote(w_ref, wbuf.at[:, my_cols], w_sem.at[0], w_sem.at[1], sib)
    send_w.start()
    send_b = remote(b_ref, bias.at[:, my_cols], bias_sem.at[0], bias_sem.at[1], sib)
    send_b.start()
    for cp in loads:
        cp.wait()

    def carries(way, dist, n, stop=n_unit):
        ok = (n >= 0) & (n < stop)
        if dist == MAXD:
            ok = ok & (par(n) == way)
        return ok

    def credits_before(k, way, dist, n, bwd):
        later = n >= 3 - k[slot(way, dist) % nz]
        if not bwd:
            return [(later, 1)]
        if dist < MAXD:
            return [(n == 0, 2), (later, 1)]
        return [(n < 2, 1), (later, 1)]

    def wait_credit(sem, k, way, dist, n, bwd):
        for cond, amount in credits_before(k, way, dist, n, bwd):
            @pl.when(cond)
            def _():
                pl.semaphore_wait(sem, amount)

    def hop_copy(k, n, way, dist):
        s, s0 = slot(way, dist), slot(way, dist - 1)
        return remote(xbuf.at[par(n + k[s0]), block(s0)], xbuf.at[par(n + k[s]), block(s)],
                      ag_send.at[way, dist - 1, par(n)], ag_recv.at[par(n + k[s]), s, 0], dev(ahead[way], c))

    def inj_copy(k, n, way, cc, i):
        s = slot(way, 1)
        return remote(own.at[cc, n // per_row, unit_rows(n)], xbuf.at[par(n + k[s]), part_of_block(s, i)],
                      inj_send.at[way, cc], ag_recv.at[par(n + k[s]), s, i], dev(ahead[way], cc))

    def sib_copy(k, n):
        return remote(own.at[o, n // per_row, unit_rows(n)], xbuf.at[par(n + k[0]), part_of_block(0, c)],
                      sib_send, ag_recv.at[par(n + k[0]), 0, 0], sib)

    def inject(k, n, bwd=False):
        @pl.when((n >= 0) & (n < n_unit))
        def _():
            for cc in WAYS:
                for way in WAYS:
                    wait_credit(inj_cred.at[way, cc], k, way, 1, n, bwd)
                    inj_copy(k, n, way, cc, c).start()
            wait_credit(sib_cred, k, 0, 0, n, bwd)
            sib_copy(k, n).start()

    def injected(k, n):
        @pl.when((n >= 0) & (n < n_unit))
        def _():
            for cc in WAYS:
                for way in WAYS:
                    inj_copy(k, n, way, cc, c).wait_send()
            sib_copy(k, n).wait_send()

    def arrive(k, n, way, dist):
        @pl.when(carries(way, dist, n))
        def _():
            if dist == 0:
                sib_copy(k, n).wait_recv()
            elif dist == 1:
                for i in WAYS:
                    inj_copy(k, n, way, 0, i).wait_recv()
            else:
                hop_copy(k, n, way, dist).wait_recv()

    def forward(k, n, way, dist, bwd=False):
        @pl.when(carries(way, dist + 1, n))
        def _():
            wait_credit(ag_cred.at[way, dist], k, way, dist + 1, n, bwd)
            hop_copy(k, n, way, dist + 1).start()

    def relay(k, n, dist, bwd=False):
        for way in WAYS:
            arrive(k, n, way, dist)
            if dist < MAXD:
                forward(k, n, way, dist, bwd)

    def take_own(k, n):
        @pl.when((n >= 0) & (n < n_unit))
        def _():
            xbuf[par(n + k[0]), part_of_block(0, c)] = own[c, n // per_row, unit_rows(n)]

    def give_credit(way, dist, amount=1):
        if dist == 0:
            pl.semaphore_signal(sib_cred, inc=amount, device_id=sib, device_id_type=MESH)
        elif dist == 1:
            for i in WAYS:
                pl.semaphore_signal(inj_cred.at[way, c], inc=amount, device_id=dev(behind[way], i), device_id_type=MESH)
        else:
            pl.semaphore_signal(ag_cred.at[way, dist - 1], inc=amount, device_id=dev(behind[way], c), device_id_type=MESH)

    def lanes_of(s):
        if s == 0:
            return ((0, 0),)
        if s == MAXD:
            return ((0, MAXD), (1, MAXD))
        return ((0, s),) if s < MAXD else ((1, nz - s),)

    def release(k, j, slots):
        for s in slots:
            for way, dist in lanes_of(s):
                n = j - k[s]
                if 1 <= dist < MAXD:
                    @pl.when(carries(way, dist + 1, n))
                    def _():
                        hop_copy(k, n, way, dist + 1).wait_send()
        for s in slots:
            for way, dist in lanes_of(s):
                @pl.when(carries(way, dist, j - k[s] + 2))
                def _():
                    give_credit(way, dist)

    near, far = ORDER[:nz // PAIR], ORDER[nz // PAIR:]

    inject(KF, ZERO)

    @pl.loop(0, rep.shape[0])
    def _(i):
        rep[i] = jnp.zeros(rep.shape[1:], F32)

    @pl.loop(0, PAD)
    def _(i):
        maskx[i] = jnp.zeros(maskx.shape[1:], F32)
        maskx[PAD + n_unit + i] = jnp.zeros(maskx.shape[1:], F32)
    gbacc[...] = jnp.zeros_like(gbacc)

    @pl.loop(0, hid // BIG)
    def _(i):
        gw[pl.ds(pl.multiple_of(i * BIG, BIG), BIG), :] = jnp.zeros((BIG, v_chip), F32)

    load_m.wait()
    for cp in send_m:
        cp.wait()

    in_row = LANE // UT
    for s in range(nz):
        for i in WAYS:
            for r in range(n_unit // in_row):
                tile = jnp.broadcast_to(msgs[PAIR * chip_of(s) + i, c, r:r + 1, :], (LANE, LANE)).T
                for t in range(in_row):
                    at = pos[s] * br + i * UT
                    maskx[PAD + r * in_row + t, at:at + UT, :] = tile[t * UT:(t + 1) * UT, :]

    relay(KF, ZERO, 1)
    injected(KF, ZERO)
    load_w.wait()
    load_b.wait()
    send_w.wait()
    send_b.wait()

    def pages(j, k):
        after = {d: (j - d + PAD) // per_row for d in set(k)}
        return [after[k[s]] for s in range(nz)]

    def mask_rows(j, k, slots):
        return jnp.concatenate([maskx[j - k[s] + PAD, block(s), :] for s in slots], axis=0)

    def fwd_group(j, b, g, k0, k1):
        slots = (near, far)[g]
        page = pages(j, KF)

        @functools.partial(lax.fori_loop, k0, k1, init_val=None, unroll=UNROLL)
        def _(k, _):
            at = pl.ds(pl.multiple_of(k * CH, CH), CH)
            logits = jnp.dot(xbuf[b, g * half:(g + 1) * half], wbuf[:, at], preferred_element_type=F32)
            for t in range(CH // LANE):
                at = pl.ds(pl.multiple_of(k * CH + t * LANE, LANE), LANE)
                zt = logits[:, t * LANE:(t + 1) * LANE] + bias[:, at]
                act = jnp.log(1.0 + jnp.maximum(zt, 0.0)) * mask_rows(j, KF, slots)
                for i, s in enumerate(slots):
                    for u in WAYS:
                        r0 = i * br + u * UT
                        row_sum = jnp.sum(act[r0:r0 + UT, :], axis=0, keepdims=True)
                        rep[page[s], PAIR * s + u:PAIR * s + u + 1, at] = rep[page[s], PAIR * s + u:PAIR * s + u + 1, at] + row_sum

    def cut(eighths):
        return n_chunk * eighths // SUB

    fwd_end = n_unit + KF[MAXD]

    def release_far(j):
        @pl.when(j >= 1)
        def _():
            release(KF, j, far)

    @pl.loop(1, fwd_end)
    def _(j):
        b = par(j)
        release_far(j - 1)
        inject(KF, j)
        take_own(KF, j - KF[0])
        arrive(KF, j - KF[0], 0, 0)
        fwd_group(j, b, 0, 0, cut(6))
        relay(KF, j - 2, 3)
        fwd_group(j, b, 0, cut(6), n_chunk)
        release(KF, j, near)
        relay(KF, j - 1, 2)
        relay(KF, j - 3, 4)
        fwd_group(j, b, 1, 0, cut(4))
        relay(KF, j, 1)
        fwd_group(j, b, 1, cut(4), n_chunk)
        injected(KF, j)

        @pl.when(j <= v_chip // 256)
        def _():
            for u in WAYS:
                at = pl.ds(pl.multiple_of((j - 1) * 256 + u * LANE, LANE), LANE)
                wt[at, :] = wbuf[:, at].T

    release_far(jnp.int32(fwd_end - 1))

    for s in range(nz):
        for way, dist in lanes_of(s):
            give_credit(way, dist, 2 if dist < MAXD else 1)

    q_total = q_rows * n_group
    d_total = d_rows * n_group
    v_total = v_loc * n_group
    tau = q_len * math.sqrt(v_total * d_len) / 16.0
    lam_q = 4.0 / (v_total * q_len * q_len)
    lam_d = 4.0 / (v_total * d_len * d_len)
    nd = d_rows // PAIR * n_group
    nq = q_rows // PAIR * n_group
    q0 = PAD // per_row
    d0 = q0 + n_qpage

    @pl.loop(0, n_chunk)
    def _(k):
        at = pl.ds(pl.multiple_of(k * CH, CH), CH)
        for r in range(d_rows // PAIR):
            rdx[c, r * n_group:(r + 1) * n_group, at] = sum(rep[d0 + r * pieces + i, :, at] for i in range(pieces))
        q_sum = sum(rep[q0 + i, :, at] for i in range(n_qpage))
        rdx[c, nd:nd + SUB, at] = sum(q_sum[i * SUB:(i + 1) * SUB] for i in range(n_group // SUB))

    def to_sib(src, dst, i):
        return remote(src, dst, pair_sem.at[i, 0], pair_sem.at[i, 1], sib)

    send_rd = to_sib(rdx.at[c], rdx.at[c], 0)
    send_rd.start()
    inject(KB, ZERO, BWD)
    send_rd.wait()

    def d_reps(at):
        return jnp.concatenate([rdx[0, 0:nd, at], rdx[1, 0:nd, at]], axis=0)

    def q_mean_of(at):
        return jnp.sum(rdx[0, nd:nd + SUB, at] + rdx[1, nd:nd + SUB, at], axis=0, keepdims=True) * (1.0 / q_total)

    def d_mean_of(at):
        return jnp.sum(d_reps(at), axis=0, keepdims=True) * (1.0 / d_total)

    def lanes(v):
        return sum(v[:, t * LANE:(t + 1) * LANE] for t in range(CH // LANE))

    def score_chunk(k, carry):
        s_acc, rq, rd = carry
        at = pl.ds(pl.multiple_of(k * CH, CH), CH)
        q_rep = rep[q0:q0 + n_qpage, :, at].reshape(nq, CH)
        s_acc = s_acc + lax.dot_general(d_reps(at), q_rep, (((1,), (1,)), ((), ())), precision=HIGHEST,
                                        preferred_element_type=F32)
        qm, dm = q_mean_of(at), d_mean_of(at)
        return s_acc, rq + lanes(qm * qm), rd + lanes(dm * dm)

    score, reg_q, reg_d = lax.fori_loop(0, n_chunk, score_chunk,
                                        (jnp.zeros((PAIR * nd, nq), F32), jnp.zeros((1, LANE), F32), jnp.zeros((1, LANE), F32)))

    def turn(n):
        i = lax.broadcasted_iota(jnp.int32, (n, n), 0)
        k = lax.broadcasted_iota(jnp.int32, (n, n), 1)
        same = (i // n_group == k // n_group) & (i % 2 == k % 2)
        return (same & (((i // PAIR) % nz + (k // PAIR) % nz) % nz == z)).astype(F32)

    def exact(a, b):
        return jnp.dot(a, b, precision=HIGHEST, preferred_element_type=F32)

    turn_d, turn_q = turn(PAIR * nd), turn(nq)
    smsg[0, 0:PAIR * nd, 0:nq] = exact(exact(turn_d, score), turn_q)
    smsg[0, PAIR * nd:PAIR * nd + 1, :] = reg_q
    smsg[0, PAIR * nd + 1:PAIR * nd + 2, :] = reg_d
    send_s = [remote(smsg.at[0], smsg.at[t], sm_send.at[t], sm_recv.at[t], peers[t - 1]) for t in range(1, nz)]
    for cp in send_s:
        cp.start()

    pos_rows = jnp.concatenate([msgs[i, 0, 3:4, :] for i in range(n_group)], axis=0)
    spread = (lax.broadcasted_iota(jnp.int32, (LANE, nq), 0)
              == PAIR * (lax.broadcasted_iota(jnp.int32, (LANE, nq), 1) // n_group) + c).astype(F32)
    pos_all = exact(pos_rows, spread)
    pick = (lax.broadcasted_iota(jnp.int32, (n_group, nq), 1) % n_group
            == lax.broadcasted_iota(jnp.int32, (n_group, nq), 0))
    pos_row = jnp.sum(jnp.where(pick, pos_all, 0.0), axis=0, keepdims=True)
    ridx = lax.broadcasted_iota(jnp.int32, (PAIR * nd, nq), 0)
    doc = (ridx % n_group) * d_rows + PAIR * ((ridx % nd) // n_group) + ridx // nd
    target = (doc.astype(F32) == pos_row).astype(F32)

    relay(KB, ZERO, 1, BWD)
    injected(KB, ZERO)
    for cp in send_s:
        cp.wait()
    total = smsg[0]
    for t in range(1, nz):
        total = total + smsg[t]
    scores = total[0:PAIR * nd, 0:nq] * (1.0 / tau)
    top = jnp.max(scores, axis=0, keepdims=True)
    log_norm = top + jnp.log(jnp.sum(jnp.exp(scores - top), axis=0, keepdims=True))
    row_loss = log_norm - jnp.sum(scores * target, axis=0, keepdims=True)
    loss_part = jnp.sum(row_loss, axis=1, keepdims=True)
    gt = (jnp.exp(scores - log_norm) - target) * (1.0 / (q_total * tau))
    gt = exact(exact(turn_d, gt), turn_q)
    g = gt.T
    lossx[c] = jnp.broadcast_to(loss_part, (SUB, LANE))
    send_l = to_sib(lossx.at[c], lossx.at[c], 1)
    send_l.start()
    inject(KB, ZERO + 1, BWD)
    relay(KB, ZERO, 2, BWD)

    @pl.loop(0, n_chunk)
    def _(k):
        at = pl.ds(pl.multiple_of(k * CH, CH), CH)
        q_rep = rep[q0:q0 + n_qpage, :, at].reshape(nq, CH)
        dp = exact(gt, q_rep)
        ddx[0, :, at] = dp[0:nd]
        ddx[1, :, at] = dp[nd:PAIR * nd]

    send_dd = to_sib(ddx.at[o], ddr, 2)
    send_dd.start()

    @pl.loop(0, n_chunk)
    def _(k):
        at = pl.ds(pl.multiple_of(k * CH, CH), CH)
        gq = exact(g, d_reps(at)) + q_mean_of(at) * (2.0 * lam_q / q_total)
        rep[q0:q0 + n_qpage, :, at] = gq.reshape(n_qpage, n_group, CH)

    send_l.wait()
    reg = (jnp.sum(total[PAIR * nd:PAIR * nd + 1, :], axis=1, keepdims=True) * lam_q
           + jnp.sum(total[PAIR * nd + 1:PAIR * nd + 2, :], axis=1, keepdims=True) * lam_d)
    lossf[0] = (lossx[0] + lossx[1]) * (1.0 / q_total) + reg

    send_loss = [remote(lossf.at[0], lossf.at[1], loss_send.at[t], loss_recv, peers[t - 1]) for t in range(1, nz)]

    @pl.when(z == 0)
    def _():
        for cp in send_loss:
            cp.start()
    relay(KB, ZERO + 1, 1, BWD)
    injected(KB, ZERO + 1)
    relay(KB, ZERO, 3, BWD)
    send_dd.wait()

    @pl.loop(0, n_chunk)
    def _(k):
        at = pl.ds(pl.multiple_of(k * CH, CH), CH)
        gd = ddx[c, :, at] + ddr[:, at] + d_mean_of(at) * (2.0 * lam_d / d_total)
        for r in range(d_rows // PAIR):
            for i in range(pieces):
                rep[d0 + r * pieces + i, :, at] = gd[r * n_group:(r + 1) * n_group]

    def bwd_chunk(j, b, page, k):
        cols = pl.ds(pl.multiple_of(k * CB, CB), CB)
        logits = jnp.dot(xbuf[b], wbuf[:, cols], preferred_element_type=F32)
        low = []
        for t in range(CB // LANE):
            at = pl.ds(pl.multiple_of(k * CB + t * LANE, LANE), LANE)
            zt = logits[:, t * LANE:(t + 1) * LANE] + bias[:, at]
            grad = jnp.concatenate([jnp.broadcast_to(rep[page[s], PAIR * s + u:PAIR * s + u + 1, at], (UT, LANE))
                                    for s in ORDER for u in WAYS], axis=0)
            gz = jnp.where(zt > 0.0, grad * mask_rows(j, KB, ORDER) / (1.0 + jnp.maximum(zt, 0.0)), 0.0)
            gbacc[:, at] = gbacc[:, at] + jnp.sum(gz.reshape(rows // SUB, SUB, LANE), axis=0)
            low.append(gz.astype(BF16))
        low = jnp.concatenate(low, axis=1)
        gbuf[:, cols] = low
        gw[:, cols] = gw[:, cols] + jnp.dot(xt[...], low, preferred_element_type=F32)

    def bwd_hidden(k0, k1):
        wide = hid // 4

        @functools.partial(lax.fori_loop, k0, k1, init_val=None, unroll=UNROLL)
        def _(k, _):
            cols = pl.ds(pl.multiple_of(k * wide, wide), wide)
            pbuf[:, cols] = jnp.dot(gbuf[...], wt[:, cols], preferred_element_type=F32).astype(BF16)

    def deep(n):
        return lax.rem(n + BIG, DEEP)

    def rs_copy(n, way, dist):
        return remote(sbuf.at[way, dist - 1], rbuf.at[way, dist - 2, deep(n)], rs_send.at[way, dist - 1],
                      rs_recv.at[way, dist - 2, deep(n)], dev(behind[way], c))

    def home_copy(n, way, cc, i):
        return remote(sbuf.at[way, 0, pl.ds(i * UT, UT)], hbuf.at[way, cc, deep(n)], h_send.at[way, i],
                      h_recv.at[way, cc, deep(n)], dev(behind[way], i))

    def pair_copy(n):
        return remote(sst.at[par(n)], sibp.at[par(n)], sp_send.at[par(n)], sp_recv.at[par(n)], sib)

    def rs_sent(n, way, dist):
        @pl.when(carries(way, dist, n))
        def _():
            if dist == 1:
                for i in WAYS:
                    home_copy(n, way, c, i).wait_send()
            else:
                rs_copy(n, way, dist).wait_send()

    def rs_go(n, way, dist):
        @pl.when(n >= DEEP)
        def _():
            if dist == 1:
                for i in WAYS:
                    pl.semaphore_wait(h_cred.at[way, i])
            else:
                pl.semaphore_wait(rs_cred.at[way, dist - 1])
        if dist == 1:
            for i in WAYS:
                home_copy(n, way, c, i).start()
        else:
            rs_copy(n, way, dist).start()

    def rs_event(n, way, dist):
        s = slot(way, dist)
        rs_sent(n - (2 if dist == MAXD else 1), way, dist)
        mine = (lambda: pbuf[block(s), :]) if dist == MAXD else (lambda: part[s, deep(n)])
        incoming = carries(way, dist + 1, n) if dist + 1 <= MAXD else None
        if dist == MAXD:
            alone, joined = carries(way, dist, n), None
        elif dist + 1 == MAXD:
            alone, joined = carries(way, dist, n) & (par(n) != way), incoming
        else:
            alone, joined = None, incoming
        if alone is not None:
            @pl.when(alone)
            def _():
                sbuf[way, dist - 1] = mine()
                rs_go(n, way, dist)
        if joined is not None:
            @pl.when(joined)
            def _():
                rs_copy(n, way, dist + 1).wait_recv()
                got = rbuf[way, dist - 1, deep(n)]
                sbuf[way, dist - 1] = (mine().astype(F32) + got.astype(F32)).astype(BF16)

                @pl.when(n + DEEP < n_unit)
                def _():
                    pl.semaphore_signal(rs_cred.at[way, dist], device_id=dev(ahead[way], c), device_id_type=MESH)
                rs_go(n, way, dist)

    def rs_home(n):
        @pl.when((n >= 0) & (n < n_unit))
        def _():
            for cc in WAYS:
                for way in WAYS:
                    home_copy(n, way, cc, 0).wait_recv()
                at = unit_rows(n)
                acc_h[cc, n // per_row, at] = (acc_h[cc, n // per_row, at].astype(F32) + hbuf[0, cc, deep(n)].astype(F32)
                                               + hbuf[1, cc, deep(n)].astype(F32)).astype(BF16)

                @pl.when(n + DEEP < n_unit)
                def _():
                    for way in WAYS:
                        pl.semaphore_signal(h_cred.at[way, c], device_id=dev(ahead[way], cc), device_id_type=MESH)

    def pair_send(n):
        @pl.when((n >= 2) & (n < n_unit + 2))
        def _():
            pair_copy(n - 2).wait_send()

        @pl.when((n >= 0) & (n < n_unit))
        def _():
            sst[par(n)] = pbuf[part_of_block(0, o), :]

            @pl.when(n >= 2)
            def _():
                pl.semaphore_wait(sp_cred)
            pair_copy(n).start()
            acc_h[c, n // per_row, unit_rows(n)] = pbuf[part_of_block(0, c), :]

    def pair_take(n):
        @pl.when((n >= 0) & (n < n_unit))
        def _():
            pair_copy(n).wait_recv()
            acc_h[o, n // per_row, unit_rows(n)] = sibp[par(n)]

            @pl.when(n + 2 < n_unit)
            def _():
                pl.semaphore_signal(sp_cred, device_id=sib, device_id_type=MESH)

    last = n_unit + KB[MAXD]

    def part_b(eighths):
        return v_chip // CB * eighths // SUB

    def rs_both(n, dist):
        for way in WAYS:
            rs_event(n, way, dist)

    @pl.loop(1, last)
    def _(j):
        b = par(j)
        page = pages(j, KB)

        def weights(k0, k1):
            @functools.partial(lax.fori_loop, k0, k1, init_val=None, unroll=UNROLL)
            def _(k, _):
                bwd_chunk(j, b, page, k)

        relay(KB, j - 2, 4)
        take_own(KB, j - 1)
        arrive(KB, j - 1, 0, 0)
        rs_both(j - 3, 4)
        rs_both(j - 5, 1)
        xt[...] = xbuf[b].T
        weights(0, part_b(4))

        @pl.when(j >= 2)
        def _():
            relay(KB, j, 1, BWD)
        rs_both(j - 4, 2)
        weights(part_b(4), part_b(6))

        @pl.when(j >= 2)
        def _():
            relay(KB, j - 1, 3, BWD)
        weights(part_b(6), v_chip // CB)
        release(KB, j, ORDER)
        rs_both(j - 3, 3)
        bwd_hidden(0, 3)

        @pl.when(j >= 2)
        def _():
            injected(KB, j)
        inject(KB, j + 1, BWD)
        relay(KB, j, 2, BWD)
        rs_home(j - 5)
        bwd_hidden(3, 4)
        for s in range(1, nz):
            if s != MAXD:
                part[s, deep(j - KB[s])] = pbuf[block(s), :]
        pair_send(j - 1)
        pair_take(j - 2)

    n_part = gx_send.shape[0] - 1
    step = v_loc // n_part
    send_g = []
    for k in range(n_part):
        theirs = pl.ds(pl.multiple_of(o * v_loc + k * step, step), step)
        send_g.append(remote(gw.at[:, theirs], grecv.at[k % PAIR], gx_send.at[k], gx_recv.at[k], sib))
    send_gb = remote(gbacc.at[:, sib_cols], gbrecv, gx_send.at[n_part], gx_recv.at[n_part], sib)
    for cp in send_g[:PAIR]:
        cp.start()
    send_gb.start()

    w_outs = []

    def add_part():
        k = len(w_outs)
        send_g[k].wait_recv()
        at = pl.ds(pl.multiple_of(c * v_loc + k * step, step), step)

        @pl.loop(0, hid // BIG)
        def _(i):
            rr = pl.ds(pl.multiple_of(i * BIG, BIG), BIG)
            wbuf[rr, at] = (gw[rr, at] + grecv[k % PAIR, rr]).astype(BF16)
        w_outs.append(pltpu.make_async_copy(wbuf.at[:, at], gw_out.at[:, pl.ds(k * step, step)], out_sem.at[n_load + k]))
        w_outs[-1].start()
        if k + PAIR < n_part:
            pl.semaphore_signal(gx_cred, device_id=sib, device_id_type=MESH)
            pl.semaphore_wait(gx_cred)
            send_g[k + PAIR].start()

    n_load = len(loads)
    for j in range(last, n_unit + 5):
        n = ZERO + j
        rs_both(n - 3, 4)
        rs_both(n - 5, 1)
        if j > last:
            add_part()
        rs_both(n - 4, 2)
        rs_both(n - 3, 3)
        pair_send(n - 1)
        if j == last:
            add_part()
        rs_home(n - 5)
    for way in WAYS:
        rs_sent(jnp.int32(n_unit - 1), way, 1)

    outs = []
    for cc in WAYS:
        outs.append(pltpu.make_async_copy(acc_h.at[cc, pl.ds(0, n_qpage)], dq_out.at[:, cc], out_sem.at[len(outs)]))
        for r in range(d_rows // PAIR):
            outs.append(pltpu.make_async_copy(acc_h.at[cc, pl.ds(n_qpage + r * pieces, pieces)], dd_out.at[r, cc],
                                              out_sem.at[len(outs)]))
    for cp in outs:
        cp.start()
    while len(w_outs) < n_part:
        add_part()
    send_gb.wait_recv()
    gb_ref[...] = jnp.sum(gbacc[:, my_cols] + gbrecv[...], axis=0, keepdims=True)

    @pl.when(z == 0)
    def _():
        for cp in send_loss:
            cp.wait_send()
        loss_ref[...] = lossf[0, 0:1, 0:1]

    @pl.when(z != 0)
    def _():
        send_loss[0].wait_recv()
        loss_ref[...] = lossf[1, 0:1, 0:1]
    for cp in send_g:
        cp.wait_send()
    send_gb.wait_send()
    for cp in outs + w_outs:
        cp.wait()


def solution(mesh):
    n_group = mesh.shape['tp']
    nz = n_group // PAIR
    row_spec = P(('dp', 'tp'))
    mask_spec = P(('dp', 'tp'), None)
    hid_spec = P(('dp', 'tp'), None, None)

    def local_step(q_hidden, d_hidden, q_mask, d_mask, positive, w_head, b_head):
        q_rows, q_len, hid = q_hidden.shape
        d_rows, d_len, _ = d_hidden.shape
        v_loc = w_head.shape[1]
        v_chip = PAIR * v_loc
        per_row = q_len // UT
        pieces = d_len // q_len
        n_page = q_rows // PAIR + d_rows // PAIR * pieces
        n_unit = n_page * per_row
        rows = nz * PAIR * UT
        nd, nq = d_rows // PAIR * n_group, q_rows // PAIR * n_group
        by_core = jnp.concatenate([jnp.swapaxes(q_mask.reshape(q_rows // PAIR, 2, q_len), 0, 1).reshape(2, -1),
                                   jnp.swapaxes(d_mask.reshape(d_rows // PAIR, 2, d_len), 0, 1).reshape(2, -1)], axis=1)
        by_core = by_core.astype(F32).reshape(2, -1, LANE)
        by_core = jnp.pad(by_core, ((0, 0), (0, 3 - by_core.shape[1]), (0, 0)))
        where = jnp.pad(positive.astype(F32), (0, LANE - q_rows)).reshape(1, 1, LANE)
        msg = jnp.concatenate([by_core, jnp.broadcast_to(where, (2, 1, LANE))], axis=1)
        s_rows = -(-(PAIR * nd + 2) // SUB) * SUB
        n_part = 4 if v_loc >= 512 else 2
        n_load = PAIR * (1 + d_rows // PAIR)
        dma, reg = pltpu.SemaphoreType.DMA, pltpu.SemaphoreType.REGULAR
        anym = pl.BlockSpec(memory_space=pl.ANY)
        vm = pl.BlockSpec(memory_space=pltpu.VMEM)
        q_shape = (q_rows // PAIR, 2, q_len, hid)
        d_shape = (d_rows // PAIR, 2, pieces, q_len, hid)
        out_shape = (
            jax.ShapeDtypeStruct((1, 1), F32),
            jax.ShapeDtypeStruct((hid, v_loc), BF16),
            jax.ShapeDtypeStruct((1, v_loc), F32),
            jax.ShapeDtypeStruct(q_shape, BF16),
            jax.ShapeDtypeStruct(d_shape, BF16),
        )
        scratch = [
            pltpu.VMEM((hid, v_chip), BF16),
            pltpu.VMEM((v_chip, hid), BF16),
            pltpu.VMEM((hid, v_chip), F32),
            pltpu.VMEM((PAIR, hid, v_loc // n_part), F32),
            pltpu.VMEM(((n_unit + PAIR * PAD) // per_row, n_group, v_chip), F32),
            pltpu.VMEM((n_unit + PAIR * PAD, rows, LANE), F32),
            pltpu.VMEM((PAIR, n_page, q_len, hid), BF16),
            pltpu.VMEM((PAIR, n_page, q_len, hid), BF16),
            pltpu.VMEM((nz, DEEP, PAIR * UT, hid), BF16),
            pltpu.VMEM((PAIR, rows, hid), BF16),
            pltpu.VMEM((PAIR, MAXD - 1, DEEP, PAIR * UT, hid), BF16),
            pltpu.VMEM((PAIR, MAXD, PAIR * UT, hid), BF16),
            pltpu.VMEM((PAIR, 2, DEEP, UT, hid), BF16),
            pltpu.VMEM((PAIR, UT, hid), BF16),
            pltpu.VMEM((PAIR, UT, hid), BF16),
            pltpu.VMEM((rows, v_chip), BF16),
            pltpu.VMEM((rows, hid), BF16),
            pltpu.VMEM((hid, rows), BF16),
            pltpu.VMEM((PAIR, nd + SUB, v_chip), F32),
            pltpu.VMEM((PAIR, nd, v_chip), F32),
            pltpu.VMEM((nd, v_chip), F32),
            pltpu.VMEM((1, v_chip), F32),
            pltpu.VMEM((SUB, v_chip), F32),
            pltpu.VMEM((SUB, v_loc), F32),
            pltpu.VMEM((n_group, 2, 4, LANE), F32),
            pltpu.VMEM((nz, s_rows, LANE), F32),
            pltpu.VMEM((PAIR, SUB, LANE), F32),
            pltpu.VMEM((PAIR, SUB, LANE), F32),
            dma((PAIR, MAXD, 2)), dma((PAIR, nz, 2)), reg((PAIR, MAXD)), dma((PAIR, 2)), reg((PAIR, 2)), dma, reg,
            dma((PAIR, MAXD)), dma((PAIR, MAXD - 1, DEEP)), reg((PAIR, MAXD)), dma((PAIR, 2)), dma((PAIR, 2, DEEP)), reg((PAIR, 2)),
            dma((PAIR,)), dma((PAIR,)), reg,
            dma((n_load + 3,)), dma((PAIR,)), dma((PAIR,)), dma((n_group - 1,)), dma((n_group - 1,)), dma((nz,)), dma((nz,)),
            dma((3, 2)), dma((n_part + 1,)), dma((n_part + 1,)), reg, dma((nz,)), dma, dma((n_load + n_part,)),
        ]
        loss, gw, gb, dq, dd = pl.pallas_call(
            functools.partial(kernel, n_group, q_rows, q_len, d_rows, d_len),
            out_shape=out_shape,
            in_specs=[anym] * 5,
            out_specs=(vm, anym, vm, anym, anym),
            scratch_shapes=scratch,
            compiler_params=pltpu.CompilerParams(collective_id=0, has_side_effects=True, vmem_limit_bytes=67043328),
        )(q_hidden.reshape(q_shape), d_hidden.reshape(d_shape), w_head, b_head.reshape(1, v_loc), msg)
        return (loss.reshape(1), gw, gb.reshape(v_loc), dq.reshape(q_hidden.shape), dd.reshape(d_hidden.shape))

    return jax.shard_map(local_step, mesh=mesh,
                         in_specs=(hid_spec, hid_spec, mask_spec, mask_spec, row_spec, P(None, 'tp'), P('tp')),
                         out_specs=(P('dp'), P('dp', 'tp'), row_spec, hid_spec, hid_spec),
                         check_vma=False)
```

```python
import functools
import math
import jax
import jax.numpy as jnp
from jax import lax
from jax.experimental import pallas as pl
from jax.experimental.pallas import tpu as pltpu
from jax.sharding import PartitionSpec as P

MESH = pl.DeviceIdType.MESH
HIGHEST = lax.Precision.HIGHEST
F32 = jnp.float32
BF16 = jnp.bfloat16
BWD = UNROLL = True

UT = 16
CH = 512
CB = 1024
MAXD = 4
KF = (1, 1, 2, 2, 3, 2, 1, 1)
KB = (1, 1, 1, 2, 2, 2, 1, 1)
LANE, SUB, PAIR, BIG = 128, 8, 2, 64
DEEP = 4
WAYS = (0, 1)
ORDER = (0, 1, 7, 2, 6, 3, 5, 4)
PAD = 4


def kernel(n_group, q_rows, q_len, d_rows, d_len,
           q_ref, d_ref, w_ref, b_ref, qm_ref, dm_ref, pos_ref,
           loss_ref, gw_out, gb_ref, dq_out, dd_out,
           wbuf, wt, gw, grecv, rep, maskx, own, acc_h, part, xbuf, rbuf, sbuf, hbuf, sibp, sst, gbuf, pbuf, xt,
           rdx, ddx, ddr, bias, gbacc, gbrecv, msgs, smsg, lossx, lossf,
           ag_send, ag_recv, ag_cred, inj_send, inj_cred, sib_send, sib_cred,
           rs_send, rs_recv, rs_cred, h_send, h_recv, h_cred, sp_send, sp_recv, sp_cred,
           loc_sem, w_sem, bias_sem, msg_send, msg_recv, sm_send, sm_recv, pair_sem, gx_send, gx_recv, gx_cred,
           loss_send, loss_recv, out_sem):
    ZERO = jnp.int32(0)
    nz = n_group // PAIR
    hid = w_ref.shape[0]
    v_loc = w_ref.shape[1]
    v_chip = PAIR * v_loc
    per_row = q_len // UT
    pieces = d_len // q_len
    n_qpage = q_rows // PAIR
    n_dpage = d_rows // PAIR * pieces
    n_page = n_qpage + n_dpage
    n_unit = n_page * per_row
    br = PAIR * UT
    rows = nz * br
    half = rows // PAIR
    n_chunk = v_chip // CH
    pos = {s: i for i, s in enumerate(ORDER)}

    me = lax.axis_index('tp')
    z = me // PAIR
    c = lax.rem(me, 2)
    o = 1 - c
    right = lax.rem(z + 1, nz)
    left = lax.rem(z + nz - 1, nz)

    def dev(zz, cc):
        return {'tp': PAIR * zz + cc}

    sib = dev(z, o)
    ahead = (right, left)
    behind = (left, right)

    def slot(way, dist):
        return dist if way == 0 else nz - dist

    def dist_of(s):
        return min(s, nz - s)

    def chip_of(s):
        return lax.rem(z - s + nz, nz)

    def block(s):
        return pl.ds(pos[s] * br, br)

    def part_of_block(s, i):
        return pl.ds(pl.multiple_of(pos[s] * br + i * UT, UT), UT)

    def par(n):
        return lax.rem(n + BIG, 2)

    def unit_rows(n):
        return pl.ds(pl.multiple_of(lax.rem(n, per_row) * UT, UT), UT)

    peers = [dev(lax.rem(z + t, nz), c) for t in range(1, nz)]
    others = [dev(lax.rem(z + t, nz), lax.rem(c + u, 2)) for t in range(nz) for u in WAYS if t or u]

    loads = []
    for cc in WAYS:
        loads.append(pltpu.make_async_copy(q_ref.at[:, cc], own.at[cc, pl.ds(0, n_qpage)], loc_sem.at[len(loads)]))
        for r in range(d_rows // PAIR):
            loads.append(pltpu.make_async_copy(d_ref.at[r, cc], own.at[cc, pl.ds(n_qpage + r * pieces, pieces)],
                                               loc_sem.at[len(loads)]))
    my_cols = pl.ds(pl.multiple_of(c * v_loc, v_loc), v_loc)
    sib_cols = pl.ds(pl.multiple_of(o * v_loc, v_loc), v_loc)
    load_w = pltpu.make_async_copy(w_ref, wbuf.at[:, my_cols], loc_sem.at[len(loads)])
    load_b = pltpu.make_async_copy(b_ref, bias.at[:, my_cols], loc_sem.at[len(loads) + 1])
    for cp in loads + [load_w, load_b]:
        cp.start()
    xbuf[...] = jnp.zeros_like(xbuf)

    where = jnp.concatenate([pos_ref[...], jnp.zeros((1, LANE - q_rows), jnp.int32)], axis=1)
    for cc in WAYS:
        tokens = jnp.concatenate([qm_ref[r:r + 1, :] for r in range(cc, q_rows, PAIR)]
                                 + [dm_ref[r:r + 1, :] for r in range(cc, d_rows, PAIR)], axis=1)
        for r in range(tokens.shape[1] // LANE):
            msgs[me, cc, r:r + 1, :] = tokens[:, r * LANE:(r + 1) * LANE].astype(F32)
        msgs[me, cc, 3:4, :] = where.astype(F32)

    barrier = pltpu.get_barrier_semaphore()
    for d in others:
        pl.semaphore_signal(barrier, device_id=d, device_id_type=MESH)
    pl.semaphore_wait(barrier, n_group - 1)

    def remote(src, dst, ss, rs, to):
        return pltpu.make_async_remote_copy(src, dst, ss, rs, device_id=to, device_id_type=MESH)

    send_m = [remote(msgs.at[me], msgs.at[me], msg_send.at[k], msg_recv.at[k], d) for k, d in enumerate(others)]
    for cp in send_m:
        cp.start()
    send_w = remote(w_ref, wbuf.at[:, my_cols], w_sem.at[0], w_sem.at[1], sib)
    send_w.start()
    send_b = remote(b_ref, bias.at[:, my_cols], bias_sem.at[0], bias_sem.at[1], sib)
    send_b.start()
    for cp in loads:
        cp.wait()

    def carries(way, dist, n, stop=n_unit):
        ok = (n >= 0) & (n < stop)
        if dist == MAXD:
            ok = ok & (par(n) == way)
        return ok

    def credits_before(k, way, dist, n, bwd):
        later = n >= 3 - k[slot(way, dist) % nz]
        if not bwd:
            return [(later, 1)]
        if dist < MAXD:
            return [(n == 0, 2), (later, 1)]
        return [(n < 2, 1), (later, 1)]

    def wait_credit(sem, k, way, dist, n, bwd):
        for cond, amount in credits_before(k, way, dist, n, bwd):
            @pl.when(cond)
            def _():
                pl.semaphore_wait(sem, amount)

    def hop_copy(k, n, way, dist):
        s, s0 = slot(way, dist), slot(way, dist - 1)
        return remote(xbuf.at[par(n + k[s0]), block(s0)], xbuf.at[par(n + k[s]), block(s)],
                      ag_send.at[way, dist - 1, par(n)], ag_recv.at[par(n + k[s]), s, 0], dev(ahead[way], c))

    def inj_copy(k, n, way, cc, i):
        s = slot(way, 1)
        return remote(own.at[cc, n // per_row, unit_rows(n)], xbuf.at[par(n + k[s]), part_of_block(s, i)],
                      inj_send.at[way, cc], ag_recv.at[par(n + k[s]), s, i], dev(ahead[way], cc))

    def sib_copy(k, n):
        return remote(own.at[o, n // per_row, unit_rows(n)], xbuf.at[par(n + k[0]), part_of_block(0, c)],
                      sib_send, ag_recv.at[par(n + k[0]), 0, 0], sib)

    def inject(k, n, bwd=False):
        @pl.when((n >= 0) & (n < n_unit))
        def _():
            for cc in WAYS:
                for way in WAYS:
                    wait_credit(inj_cred.at[way, cc], k, way, 1, n, bwd)
                    inj_copy(k, n, way, cc, c).start()
            wait_credit(sib_cred, k, 0, 0, n, bwd)
            sib_copy(k, n).start()

    def injected(k, n):
        @pl.when((n >= 0) & (n < n_unit))
        def _():
            for cc in WAYS:
                for way in WAYS:
                    inj_copy(k, n, way, cc, c).wait_send()
            sib_copy(k, n).wait_send()

    def arrive(k, n, way, dist):
        @pl.when(carries(way, dist, n))
        def _():
            if dist == 0:
                sib_copy(k, n).wait_recv()
            elif dist == 1:
                for i in WAYS:
                    inj_copy(k, n, way, 0, i).wait_recv()
            else:
                hop_copy(k, n, way, dist).wait_recv()

    def forward(k, n, way, dist, bwd=False):
        @pl.when(carries(way, dist + 1, n))
        def _():
            wait_credit(ag_cred.at[way, dist], k, way, dist + 1, n, bwd)
            hop_copy(k, n, way, dist + 1).start()

    def relay(k, n, dist, bwd=False):
        for way in WAYS:
            arrive(k, n, way, dist)
            if dist < MAXD:
                forward(k, n, way, dist, bwd)

    def take_own(k, n):
        @pl.when((n >= 0) & (n < n_unit))
        def _():
            xbuf[par(n + k[0]), part_of_block(0, c)] = own[c, n // per_row, unit_rows(n)]

    def give_credit(way, dist, amount=1):
        if dist == 0:
            pl.semaphore_signal(sib_cred, inc=amount, device_id=sib, device_id_type=MESH)
        elif dist == 1:
            for i in WAYS:
                pl.semaphore_signal(inj_cred.at[way, c], inc=amount, device_id=dev(behind[way], i), device_id_type=MESH)
        else:
            pl.semaphore_signal(ag_cred.at[way, dist - 1], inc=amount, device_id=dev(behind[way], c), device_id_type=MESH)

    def lanes_of(s):
        if s == 0:
            return ((0, 0),)
        if s == MAXD:
            return ((0, MAXD), (1, MAXD))
        return ((0, s),) if s < MAXD else ((1, nz - s),)

    def release(k, j, slots):
        for s in slots:
            for way, dist in lanes_of(s):
                n = j - k[s]
                if 1 <= dist < MAXD:
                    @pl.when(carries(way, dist + 1, n))
                    def _():
                        hop_copy(k, n, way, dist + 1).wait_send()
        for s in slots:
            for way, dist in lanes_of(s):
                @pl.when(carries(way, dist, j - k[s] + 2))
                def _():
                    give_credit(way, dist)

    near, far = ORDER[:nz // PAIR], ORDER[nz // PAIR:]

    inject(KF, ZERO)

    @pl.loop(0, rep.shape[0])
    def _(i):
        rep[i] = jnp.zeros(rep.shape[1:], F32)

    @pl.loop(0, PAD)
    def _(i):
        maskx[i] = jnp.zeros(maskx.shape[1:], F32)
        maskx[PAD + n_unit + i] = jnp.zeros(maskx.shape[1:], F32)
    gbacc[...] = jnp.zeros_like(gbacc)

    @pl.loop(0, hid // BIG)
    def _(i):
        gw[pl.ds(pl.multiple_of(i * BIG, BIG), BIG), :] = jnp.zeros((BIG, v_chip), F32)

    for cp in send_m:
        cp.wait()

    in_row = LANE // UT
    for s in range(nz):
        for i in WAYS:
            for r in range(n_unit // in_row):
                tile = jnp.broadcast_to(msgs[PAIR * chip_of(s) + i, c, r:r + 1, :], (LANE, LANE)).T
                for t in range(in_row):
                    at = pos[s] * br + i * UT
                    maskx[PAD + r * in_row + t, at:at + UT, :] = tile[t * UT:(t + 1) * UT, :]

    relay(KF, ZERO, 1)
    injected(KF, ZERO)
    load_w.wait()
    load_b.wait()
    send_w.wait()
    send_b.wait()

    def pages(j, k):
        after = {d: (j - d + PAD) // per_row for d in set(k)}
        return [after[k[s]] for s in range(nz)]

    def mask_rows(j, k, slots):
        return jnp.concatenate([maskx[j - k[s] + PAD, block(s), :] for s in slots], axis=0)

    def fwd_group(j, b, g, k0, k1):
        slots = (near, far)[g]
        page = pages(j, KF)

        @functools.partial(lax.fori_loop, k0, k1, init_val=None, unroll=UNROLL)
        def _(k, _):
            at = pl.ds(pl.multiple_of(k * CH, CH), CH)
            logits = jnp.dot(xbuf[b, g * half:(g + 1) * half], wbuf[:, at], preferred_element_type=F32)
            for t in range(CH // LANE):
                at = pl.ds(pl.multiple_of(k * CH + t * LANE, LANE), LANE)
                zt = logits[:, t * LANE:(t + 1) * LANE] + bias[:, at]
                act = jnp.log(1.0 + jnp.maximum(zt, 0.0)) * mask_rows(j, KF, slots)
                for i, s in enumerate(slots):
                    for u in WAYS:
                        r0 = i * br + u * UT
                        row_sum = jnp.sum(act[r0:r0 + UT, :], axis=0, keepdims=True)
                        rep[page[s], PAIR * s + u:PAIR * s + u + 1, at] = rep[page[s], PAIR * s + u:PAIR * s + u + 1, at] + row_sum

    def cut(eighths):
        return n_chunk * eighths // SUB

    fwd_end = n_unit + KF[MAXD]

    def release_far(j):
        @pl.when(j >= 1)
        def _():
            release(KF, j, far)

    @pl.loop(1, fwd_end)
    def _(j):
        b = par(j)
        release_far(j - 1)
        inject(KF, j)
        take_own(KF, j - KF[0])
        arrive(KF, j - KF[0], 0, 0)
        near_left = j < n_unit + max(KF[s] for s in near)

        @pl.when(near_left)
        def _():
            fwd_group(j, b, 0, 0, cut(6))
        relay(KF, j - 2, 3)

        @pl.when(near_left)
        def _():
            fwd_group(j, b, 0, cut(6), n_chunk)
        release(KF, j, near)
        relay(KF, j - 1, 2)
        relay(KF, j - 3, 4)
        fwd_group(j, b, 1, 0, cut(4))
        relay(KF, j, 1)
        fwd_group(j, b, 1, cut(4), n_chunk)
        injected(KF, j)

        @pl.when(j <= v_chip // 256)
        def _():
            for u in WAYS:
                at = pl.ds(pl.multiple_of((j - 1) * 256 + u * LANE, LANE), LANE)
                wt[at, :] = wbuf[:, at].T

    release_far(jnp.int32(fwd_end - 1))

    for s in range(nz):
        for way, dist in lanes_of(s):
            give_credit(way, dist, 2 if dist < MAXD else 1)

    q_total = q_rows * n_group
    d_total = d_rows * n_group
    v_total = v_loc * n_group
    tau = q_len * math.sqrt(v_total * d_len) / 16.0
    lam_q = 4.0 / (v_total * q_len * q_len)
    lam_d = 4.0 / (v_total * d_len * d_len)
    nd = d_rows // PAIR * n_group
    nq = q_rows // PAIR * n_group
    q0 = PAD // per_row
    d0 = q0 + n_qpage

    @pl.loop(0, v_chip // CB)
    def _(k):
        at = pl.ds(pl.multiple_of(k * CB, CB), CB)
        for r in range(d_rows // PAIR):
            rdx[c, r * n_group:(r + 1) * n_group, at] = sum(rep[d0 + r * pieces + i, :, at] for i in range(pieces))
        q_sum = sum(rep[q0 + i, :, at] for i in range(n_qpage))
        rdx[c, nd:nd + SUB, at] = sum(q_sum[i * SUB:(i + 1) * SUB] for i in range(n_group // SUB))

    def to_sib(src, dst, i):
        return remote(src, dst, pair_sem.at[i, 0], pair_sem.at[i, 1], sib)

    send_rd = to_sib(rdx.at[c], rdx.at[c], 0)
    send_rd.start()
    inject(KB, ZERO, BWD)
    send_rd.wait()

    def d_reps(at):
        return jnp.concatenate([rdx[0, 0:nd, at], rdx[1, 0:nd, at]], axis=0)

    def q_mean_of(at):
        return jnp.sum(rdx[0, nd:nd + SUB, at] + rdx[1, nd:nd + SUB, at], axis=0, keepdims=True) * (1.0 / q_total)

    def d_mean_of(at):
        return jnp.sum(d_reps(at), axis=0, keepdims=True) * (1.0 / d_total)

    def lanes(v):
        return sum(v[:, t * LANE:(t + 1) * LANE] for t in range(CB // LANE))

    def score_chunk(k, carry):
        s_acc, rq, rd = carry
        at = pl.ds(pl.multiple_of(k * CB, CB), CB)
        q_rep = rep[q0:q0 + n_qpage, :, at].reshape(nq, CB)
        s_acc = s_acc + lax.dot_general(d_reps(at), q_rep, (((1,), (1,)), ((), ())), precision=HIGHEST,
                                        preferred_element_type=F32)
        qm, dm = q_mean_of(at), d_mean_of(at)
        return s_acc, rq + lanes(qm * qm), rd + lanes(dm * dm)

    score, reg_q, reg_d = lax.fori_loop(0, v_chip // CB, score_chunk,
                                        (jnp.zeros((PAIR * nd, nq), F32), jnp.zeros((1, LANE), F32), jnp.zeros((1, LANE), F32)))

    def turn(n):
        i = lax.broadcasted_iota(jnp.int32, (n, n), 0)
        k = lax.broadcasted_iota(jnp.int32, (n, n), 1)
        same = (i // n_group == k // n_group) & (i % 2 == k % 2)
        return (same & (((i // PAIR) % nz + (k // PAIR) % nz) % nz == z)).astype(F32)

    def exact(a, b):
        return jnp.dot(a, b, precision=HIGHEST, preferred_element_type=F32)

    turn_d, turn_q = turn(PAIR * nd), turn(nq)
    smsg[0, 0:PAIR * nd, 0:nq] = exact(exact(turn_d, score), turn_q)
    smsg[0, PAIR * nd:PAIR * nd + 1, :] = reg_q
    smsg[0, PAIR * nd + 1:PAIR * nd + 2, :] = reg_d
    send_s = [remote(smsg.at[0], smsg.at[t], sm_send.at[t], sm_recv.at[t], peers[t - 1]) for t in range(1, nz)]
    for cp in send_s:
        cp.start()

    pos_rows = jnp.concatenate([msgs[i, 0, 3:4, :] for i in range(n_group)], axis=0)
    spread = (lax.broadcasted_iota(jnp.int32, (LANE, nq), 0)
              == PAIR * (lax.broadcasted_iota(jnp.int32, (LANE, nq), 1) // n_group) + c).astype(F32)
    pos_all = exact(pos_rows, spread)
    pick = (lax.broadcasted_iota(jnp.int32, (n_group, nq), 1) % n_group
            == lax.broadcasted_iota(jnp.int32, (n_group, nq), 0))
    pos_row = jnp.sum(jnp.where(pick, pos_all, 0.0), axis=0, keepdims=True)
    ridx = lax.broadcasted_iota(jnp.int32, (PAIR * nd, nq), 0)
    doc = (ridx % n_group) * d_rows + PAIR * ((ridx % nd) // n_group) + ridx // nd
    target = (doc.astype(F32) == pos_row).astype(F32)

    relay(KB, ZERO, 1, BWD)
    injected(KB, ZERO)
    for cp in send_s:
        cp.wait()
    total = smsg[0]
    for t in range(1, nz):
        total = total + smsg[t]
    scores = total[0:PAIR * nd, 0:nq] * (1.0 / tau)
    top = jnp.max(scores, axis=0, keepdims=True)
    log_norm = top + jnp.log(jnp.sum(jnp.exp(scores - top), axis=0, keepdims=True))
    row_loss = log_norm - jnp.sum(scores * target, axis=0, keepdims=True)
    loss_part = jnp.sum(row_loss, axis=1, keepdims=True)
    gt = (jnp.exp(scores - log_norm) - target) * (1.0 / (q_total * tau))
    gt = exact(exact(turn_d, gt), turn_q)
    g = gt.T
    lossx[c] = jnp.broadcast_to(loss_part, (SUB, LANE))
    send_l = to_sib(lossx.at[c], lossx.at[c], 1)
    send_l.start()
    inject(KB, ZERO + 1, BWD)
    relay(KB, ZERO, 2, BWD)

    @pl.loop(0, v_chip // CB)
    def _(k):
        at = pl.ds(pl.multiple_of(k * CB, CB), CB)
        q_rep = rep[q0:q0 + n_qpage, :, at].reshape(nq, CB)
        dp = exact(gt, q_rep)
        ddx[0, :, at] = dp[0:nd]
        ddx[1, :, at] = dp[nd:PAIR * nd]

    send_dd = to_sib(ddx.at[o], ddr, 2)
    send_dd.start()

    @pl.loop(0, v_chip // CB)
    def _(k):
        at = pl.ds(pl.multiple_of(k * CB, CB), CB)
        gq = exact(g, d_reps(at)) + q_mean_of(at) * (2.0 * lam_q / q_total)
        rep[q0:q0 + n_qpage, :, at] = gq.reshape(n_qpage, n_group, CB)

    send_l.wait()
    reg = (jnp.sum(total[PAIR * nd:PAIR * nd + 1, :], axis=1, keepdims=True) * lam_q
           + jnp.sum(total[PAIR * nd + 1:PAIR * nd + 2, :], axis=1, keepdims=True) * lam_d)
    lossf[0] = (lossx[0] + lossx[1]) * (1.0 / q_total) + reg

    send_loss = [remote(lossf.at[0], lossf.at[1], loss_send.at[t], loss_recv, peers[t - 1]) for t in range(1, nz)]

    @pl.when(z == 0)
    def _():
        for cp in send_loss:
            cp.start()
    relay(KB, ZERO + 1, 1, BWD)
    injected(KB, ZERO + 1)
    relay(KB, ZERO, 3, BWD)
    send_dd.wait()

    @pl.loop(0, v_chip // CB)
    def _(k):
        at = pl.ds(pl.multiple_of(k * CB, CB), CB)
        gd = ddx[c, :, at] + ddr[:, at] + d_mean_of(at) * (2.0 * lam_d / d_total)
        for r in range(d_rows // PAIR):
            for i in range(pieces):
                rep[d0 + r * pieces + i, :, at] = gd[r * n_group:(r + 1) * n_group]

    def bwd_chunk(j, b, page, k, slots=ORDER, weights=BWD):
        at0 = pos[slots[0]] * br
        some = slice(at0, at0 + len(slots) * br)
        cols = pl.ds(pl.multiple_of(k * CB, CB), CB)
        logits = jnp.dot(xbuf[b, some], wbuf[:, cols], preferred_element_type=F32)
        low = []
        for t in range(CB // LANE):
            at = pl.ds(pl.multiple_of(k * CB + t * LANE, LANE), LANE)
            zt = logits[:, t * LANE:(t + 1) * LANE] + bias[:, at]
            grad = jnp.concatenate([jnp.broadcast_to(rep[page[s], PAIR * s + u:PAIR * s + u + 1, at], (UT, LANE))
                                    for s in slots for u in WAYS], axis=0)
            gz = jnp.where(zt > 0.0, grad * mask_rows(j, KB, slots) / (1.0 + jnp.maximum(zt, 0.0)), 0.0)
            gbacc[:, at] = gbacc[:, at] + jnp.sum(gz.reshape(-1, SUB, LANE), axis=0)
            low.append(gz.astype(BF16))
        low = jnp.concatenate(low, axis=1)
        gbuf[some, cols] = low
        if weights:
            gw[:, cols] = gw[:, cols] + jnp.dot(xt[...], low, preferred_element_type=F32)

    def bwd_hidden(k0, k1, some=slice(None)):
        wide = hid // 4

        @functools.partial(lax.fori_loop, k0, k1, init_val=None, unroll=UNROLL)
        def _(k, _):
            cols = pl.ds(pl.multiple_of(k * wide, wide), wide)
            pbuf[some, cols] = jnp.dot(gbuf[some, :], wt[:, cols], preferred_element_type=F32).astype(BF16)

    def deep(n):
        return lax.rem(n + BIG, DEEP)

    def rs_copy(n, way, dist):
        return remote(sbuf.at[way, dist - 1], rbuf.at[way, dist - 2, deep(n)], rs_send.at[way, dist - 1],
                      rs_recv.at[way, dist - 2, deep(n)], dev(behind[way], c))

    def home_copy(n, way, cc, i):
        return remote(sbuf.at[way, 0, pl.ds(i * UT, UT)], hbuf.at[way, cc, deep(n)], h_send.at[way, i],
                      h_recv.at[way, cc, deep(n)], dev(behind[way], i))

    def pair_copy(n):
        return remote(sst.at[par(n)], sibp.at[par(n)], sp_send.at[par(n)], sp_recv.at[par(n)], sib)

    def rs_sent(n, way, dist):
        @pl.when(carries(way, dist, n))
        def _():
            if dist == 1:
                for i in WAYS:
                    home_copy(n, way, c, i).wait_send()
            else:
                rs_copy(n, way, dist).wait_send()

    def rs_go(n, way, dist):
        @pl.when(n >= DEEP)
        def _():
            if dist == 1:
                for i in WAYS:
                    pl.semaphore_wait(h_cred.at[way, i])
            else:
                pl.semaphore_wait(rs_cred.at[way, dist - 1])
        if dist == 1:
            for i in WAYS:
                home_copy(n, way, c, i).start()
        else:
            rs_copy(n, way, dist).start()

    def rs_event(n, way, dist):
        s = slot(way, dist)
        rs_sent(n - (2 if dist == MAXD else 1), way, dist)
        mine = (lambda: pbuf[block(s), :]) if dist == MAXD else (lambda: part[s, deep(n)])
        incoming = carries(way, dist + 1, n) if dist + 1 <= MAXD else None
        if dist == MAXD:
            alone, joined = carries(way, dist, n), None
        elif dist + 1 == MAXD:
            alone, joined = carries(way, dist, n) & (par(n) != way), incoming
        else:
            alone, joined = None, incoming
        if alone is not None:
            @pl.when(alone)
            def _():
                sbuf[way, dist - 1] = mine()
                rs_go(n, way, dist)
        if joined is not None:
            @pl.when(joined)
            def _():
                rs_copy(n, way, dist + 1).wait_recv()
                got = rbuf[way, dist - 1, deep(n)]
                sbuf[way, dist - 1] = (mine().astype(F32) + got.astype(F32)).astype(BF16)

                @pl.when(n + DEEP < n_unit)
                def _():
                    pl.semaphore_signal(rs_cred.at[way, dist], device_id=dev(ahead[way], c), device_id_type=MESH)
                rs_go(n, way, dist)

    def rs_home(n):
        @pl.when((n >= 0) & (n < n_unit))
        def _():
            for cc in WAYS:
                for way in WAYS:
                    home_copy(n, way, cc, 0).wait_recv()
                at = unit_rows(n)
                acc_h[cc, n // per_row, at] = (acc_h[cc, n // per_row, at].astype(F32) + hbuf[0, cc, deep(n)].astype(F32)
                                               + hbuf[1, cc, deep(n)].astype(F32)).astype(BF16)

                @pl.when(n + DEEP < n_unit)
                def _():
                    for way in WAYS:
                        pl.semaphore_signal(h_cred.at[way, c], device_id=dev(ahead[way], cc), device_id_type=MESH)

    def pair_send(n):
        @pl.when((n >= 2) & (n < n_unit + 2))
        def _():
            pair_copy(n - 2).wait_send()

        @pl.when((n >= 0) & (n < n_unit))
        def _():
            sst[par(n)] = pbuf[part_of_block(0, o), :]

            @pl.when(n >= 2)
            def _():
                pl.semaphore_wait(sp_cred)
            pair_copy(n).start()
            acc_h[c, n // per_row, unit_rows(n)] = pbuf[part_of_block(0, c), :]

    def pair_take(n):
        @pl.when((n >= 0) & (n < n_unit))
        def _():
            pair_copy(n).wait_recv()
            acc_h[o, n // per_row, unit_rows(n)] = sibp[par(n)]

            @pl.when(n + 2 < n_unit)
            def _():
                pl.semaphore_signal(sp_cred, device_id=sib, device_id_type=MESH)

    last = n_unit + KB[MAXD]
    assert all(n_unit + KB[s] < last for s in near)

    def part_b(eighths):
        return v_chip // CB * eighths // SUB

    def rs_both(n, dist):
        for way in WAYS:
            rs_event(n, way, dist)

    @pl.loop(1, last - 1)
    def _(j):
        b = par(j)
        page = pages(j, KB)

        def weights(k0, k1):
            @functools.partial(lax.fori_loop, k0, k1, init_val=None, unroll=UNROLL)
            def _(k, _):
                bwd_chunk(j, b, page, k)

        relay(KB, j - 2, 4)
        take_own(KB, j - 1)
        arrive(KB, j - 1, 0, 0)
        rs_both(j - 3, 4)
        rs_both(j - 5, 1)
        xt[...] = xbuf[b].T
        weights(0, part_b(4))

        @pl.when(j >= 2)
        def _():
            relay(KB, j, 1, BWD)
        rs_both(j - 4, 2)
        weights(part_b(4), part_b(6))

        @pl.when(j >= 2)
        def _():
            relay(KB, j - 1, 3, BWD)
        weights(part_b(6), v_chip // CB)
        release(KB, j, ORDER)
        rs_both(j - 3, 3)
        bwd_hidden(0, 3)

        @pl.when(j >= 2)
        def _():
            injected(KB, j)
        inject(KB, j + 1, BWD)
        relay(KB, j, 2, BWD)
        rs_home(j - 5)
        bwd_hidden(3, 4)
        for s in range(1, nz):
            if s != MAXD:
                part[s, deep(j - KB[s])] = pbuf[block(s), :]
        pair_send(j - 1)
        pair_take(j - 2)

    j = ZERO + last - 1
    b = par(j)
    page = pages(j, KB)
    some = slice(half, rows)
    relay(KB, j - 2, 4)
    rs_both(j - 3, 4)
    rs_both(j - 5, 1)

    @functools.partial(lax.fori_loop, 0, v_chip // CB, init_val=None, unroll=UNROLL)
    def _(k, _):
        bwd_chunk(j, b, page, k, far, False)
    rs_both(j - 4, 2)
    bwd_hidden(0, 4, some)
    for s in far:
        if s != MAXD:
            part[s, deep(j - KB[s])] = pbuf[block(s), :]
    rs_both(j + 1 - 3, 4)
    rs_both(j - 3, 3)
    release(KB, j, ORDER)
    pair_send(j - 1)
    pair_take(j - 2)
    rs_home(j - 5)
    xt[:, some] = xbuf[b, some].T

    @functools.partial(lax.fori_loop, 0, v_chip // CB, init_val=None, unroll=UNROLL)
    def _(k, _):
        cols = pl.ds(pl.multiple_of(k * CB, CB), CB)
        gw[:, cols] = gw[:, cols] + jnp.dot(xt[:, some], gbuf[some, cols], preferred_element_type=F32)

    n_part = gx_send.shape[0] - 1
    step = v_loc // n_part
    send_g = []
    for k in range(n_part):
        theirs = pl.ds(pl.multiple_of(o * v_loc + k * step, step), step)
        send_g.append(remote(gw.at[:, theirs], grecv.at[k % PAIR], gx_send.at[k], gx_recv.at[k], sib))
    send_gb = remote(gbacc.at[:, sib_cols], gbrecv, gx_send.at[n_part], gx_recv.at[n_part], sib)
    for cp in send_g[:PAIR]:
        cp.start()
    send_gb.start()

    w_outs = []

    def add_part():
        k = len(w_outs)
        send_g[k].wait_recv()
        at = pl.ds(pl.multiple_of(c * v_loc + k * step, step), step)

        @pl.loop(0, hid // BIG)
        def _(i):
            rr = pl.ds(pl.multiple_of(i * BIG, BIG), BIG)
            wbuf[rr, at] = (gw[rr, at] + grecv[k % PAIR, rr]).astype(BF16)
        w_outs.append(pltpu.make_async_copy(wbuf.at[:, at], gw_out.at[:, pl.ds(k * step, step)], out_sem.at[n_load + k]))
        w_outs[-1].start()
        if k + PAIR < n_part:
            pl.semaphore_signal(gx_cred, device_id=sib, device_id_type=MESH)
            pl.semaphore_wait(gx_cred)
            send_g[k + PAIR].start()

    n_load = len(loads)
    for j in range(last, n_unit + 5):
        n = ZERO + j
        if j > last:
            rs_both(n - 3, 4)
        rs_both(n - 5, 1)
        if j > last:
            add_part()
        rs_both(n - 4, 2)
        rs_both(n - 3, 3)
        pair_send(n - 1)
        if j == last:
            add_part()
        rs_home(n - 5)
    for way in WAYS:
        rs_sent(jnp.int32(n_unit - 1), way, 1)

    outs = []
    for cc in WAYS:
        outs.append(pltpu.make_async_copy(acc_h.at[cc, pl.ds(0, n_qpage)], dq_out.at[:, cc], out_sem.at[len(outs)]))
        for r in range(d_rows // PAIR):
            outs.append(pltpu.make_async_copy(acc_h.at[cc, pl.ds(n_qpage + r * pieces, pieces)], dd_out.at[r, cc],
                                              out_sem.at[len(outs)]))
    for cp in outs:
        cp.start()
    while len(w_outs) < n_part:
        add_part()
    send_gb.wait_recv()
    gb_ref[...] = jnp.sum(gbacc[:, my_cols] + gbrecv[...], axis=0, keepdims=True)

    @pl.when(z == 0)
    def _():
        for cp in send_loss:
            cp.wait_send()
        loss_ref[...] = lossf[0, 0:1, 0:1]

    @pl.when(z != 0)
    def _():
        send_loss[0].wait_recv()
        loss_ref[...] = lossf[1, 0:1, 0:1]
    for cp in send_g:
        cp.wait_send()
    send_gb.wait_send()
    for cp in outs + w_outs:
        cp.wait()


def solution(mesh):
    n_group = mesh.shape['tp']
    nz = n_group // PAIR
    row_spec = P(('dp', 'tp'))
    mask_spec = P(('dp', 'tp'), None)
    hid_spec = P(('dp', 'tp'), None, None)

    def local_step(q_hidden, d_hidden, q_mask, d_mask, positive, w_head, b_head):
        q_rows, q_len, hid = q_hidden.shape
        d_rows, d_len, _ = d_hidden.shape
        v_loc = w_head.shape[1]
        v_chip = PAIR * v_loc
        per_row = q_len // UT
        pieces = d_len // q_len
        n_page = q_rows // PAIR + d_rows // PAIR * pieces
        n_unit = n_page * per_row
        rows = nz * PAIR * UT
        nd, nq = d_rows // PAIR * n_group, q_rows // PAIR * n_group
        s_rows = -(-(PAIR * nd + 2) // SUB) * SUB
        n_part = 4 if v_loc >= 512 else 2
        n_load = PAIR * (1 + d_rows // PAIR)
        dma, reg = pltpu.SemaphoreType.DMA, pltpu.SemaphoreType.REGULAR
        anym = pl.BlockSpec(memory_space=pl.ANY)
        vm = pl.BlockSpec(memory_space=pltpu.VMEM)
        q_shape = (q_rows // PAIR, 2, q_len, hid)
        d_shape = (d_rows // PAIR, 2, pieces, q_len, hid)
        out_shape = (
            jax.ShapeDtypeStruct((1, 1), F32),
            jax.ShapeDtypeStruct((hid, v_loc), BF16),
            jax.ShapeDtypeStruct((1, v_loc), F32),
            jax.ShapeDtypeStruct(q_shape, BF16),
            jax.ShapeDtypeStruct(d_shape, BF16),
        )
        scratch = [
            pltpu.VMEM((hid, v_chip), BF16),
            pltpu.VMEM((v_chip, hid), BF16),
            pltpu.VMEM((hid, v_chip), F32),
            pltpu.VMEM((PAIR, hid, v_loc // n_part), F32),
            pltpu.VMEM(((n_unit + PAIR * PAD) // per_row, n_group, v_chip), F32),
            pltpu.VMEM((n_unit + PAIR * PAD, rows, LANE), F32),
            pltpu.VMEM((PAIR, n_page, q_len, hid), BF16),
            pltpu.VMEM((PAIR, n_page, q_len, hid), BF16),
            pltpu.VMEM((nz, DEEP, PAIR * UT, hid), BF16),
            pltpu.VMEM((PAIR, rows, hid), BF16),
            pltpu.VMEM((PAIR, MAXD - 1, DEEP, PAIR * UT, hid), BF16),
            pltpu.VMEM((PAIR, MAXD, PAIR * UT, hid), BF16),
            pltpu.VMEM((PAIR, 2, DEEP, UT, hid), BF16),
            pltpu.VMEM((PAIR, UT, hid), BF16),
            pltpu.VMEM((PAIR, UT, hid), BF16),
            pltpu.VMEM((rows, v_chip), BF16),
            pltpu.VMEM((rows, hid), BF16),
            pltpu.VMEM((hid, rows), BF16),
            pltpu.VMEM((PAIR, nd + SUB, v_chip), F32),
            pltpu.VMEM((PAIR, nd, v_chip), F32),
            pltpu.VMEM((nd, v_chip), F32),
            pltpu.VMEM((1, v_chip), F32),
            pltpu.VMEM((SUB, v_chip), F32),
            pltpu.VMEM((SUB, v_loc), F32),
            pltpu.VMEM((n_group, 2, 4, LANE), F32),
            pltpu.VMEM((nz, s_rows, LANE), F32),
            pltpu.VMEM((PAIR, SUB, LANE), F32),
            pltpu.VMEM((PAIR, SUB, LANE), F32),
            dma((PAIR, MAXD, 2)), dma((PAIR, nz, 2)), reg((PAIR, MAXD)), dma((PAIR, 2)), reg((PAIR, 2)), dma, reg,
            dma((PAIR, MAXD)), dma((PAIR, MAXD - 1, DEEP)), reg((PAIR, MAXD)), dma((PAIR, 2)), dma((PAIR, 2, DEEP)), reg((PAIR, 2)),
            dma((PAIR,)), dma((PAIR,)), reg,
            dma((n_load + PAIR,)), dma((PAIR,)), dma((PAIR,)), dma((n_group - 1,)), dma((n_group - 1,)), dma((nz,)), dma((nz,)),
            dma((3, 2)), dma((n_part + 1,)), dma((n_part + 1,)), reg, dma((nz,)), dma, dma((n_load + n_part,)),
        ]
        loss, gw, gb, dq, dd = pl.pallas_call(
            functools.partial(kernel, n_group, q_rows, q_len, d_rows, d_len),
            out_shape=out_shape,
            in_specs=[anym] * 4 + [vm] * 3,
            out_specs=(vm, anym, vm, anym, anym),
            scratch_shapes=scratch,
            compiler_params=pltpu.CompilerParams(collective_id=0, has_side_effects=True, vmem_limit_bytes=67043328),
        )(q_hidden.reshape(q_shape), d_hidden.reshape(d_shape), w_head, b_head.reshape(1, v_loc),
          q_mask, d_mask, positive.reshape(1, q_rows))
        return (loss.reshape(1), gw, gb.reshape(v_loc), dq.reshape(q_hidden.shape), dd.reshape(d_hidden.shape))

    return jax.shard_map(local_step, mesh=mesh,
                         in_specs=(hid_spec, hid_spec, mask_spec, mask_spec, row_spec, P(None, 'tp'), P('tp')),
                         out_specs=(P('dp'), P('dp', 'tp'), row_spec, hid_spec, hid_spec),
                         check_vma=False)
```

```python
import functools
import math
import jax
import jax.numpy as jnp
from jax import lax
from jax.experimental import pallas as pl
from jax.experimental.pallas import tpu as pltpu
from jax.sharding import PartitionSpec as P

MESH = pl.DeviceIdType.MESH
HIGHEST = lax.Precision.HIGHEST
F32 = jnp.float32
BF16 = jnp.bfloat16
BWD = UNROLL = True

UT = 16
CH = 512
CB = 1024
MAXD = 4
KF = (1, 1, 2, 2, 3, 2, 1, 1)
KB = (1, 1, 1, 2, 2, 2, 1, 1)
LANE, SUB, PAIR, BIG = 128, 8, 2, 64
DEEP = 4
ROOM = 8
WAYS = (0, 1)
ORDER = (0, 1, 7, 2, 6, 3, 5, 4)
PAD = 4


def kernel(n_group, q_rows, q_len, d_rows, d_len,
           q_ref, d_ref, w_ref, b_ref, qm_ref, dm_ref, pos_ref,
           loss_ref, gw_out, gb_ref, dq_out, dd_out,
           wbuf, wt, gw, grecv, rep, maskx, own, acc_h, part, xbuf, rbuf, sbuf, hbuf, sibp, sst, gbuf, pbuf, xt,
           rdx, ddx, ddr, bias, gbacc, gbrecv, msgs, smsg, lossx, lossf,
           ag_send, ag_recv, ag_cred, inj_send, inj_cred, sib_send, sib_cred,
           rs_send, rs_recv, h_send, h_recv, sp_send, sp_recv,
           loc_sem, w_sem, bias_sem, msg_send, msg_recv, sm_send, sm_recv, pair_sem, gx_send, gx_recv, gx_cred,
           loss_send, loss_recv, out_sem):
    ZERO = jnp.int32(0)
    nz = n_group // PAIR
    hid = w_ref.shape[0]
    v_loc = w_ref.shape[1]
    v_chip = PAIR * v_loc
    per_row = q_len // UT
    pieces = d_len // q_len
    n_qpage = q_rows // PAIR
    n_dpage = d_rows // PAIR * pieces
    n_page = n_qpage + n_dpage
    n_unit = n_page * per_row
    br = PAIR * UT
    rows = nz * br
    half = rows // PAIR
    n_chunk = v_chip // CH
    pos = {s: i for i, s in enumerate(ORDER)}

    me = lax.axis_index('tp')
    z = me // PAIR
    c = lax.rem(me, 2)
    o = 1 - c
    right = lax.rem(z + 1, nz)
    left = lax.rem(z + nz - 1, nz)

    def dev(zz, cc):
        return {'tp': PAIR * zz + cc}

    sib = dev(z, o)
    ahead = (right, left)
    behind = (left, right)

    def slot(way, dist):
        return dist if way == 0 else nz - dist

    def dist_of(s):
        return min(s, nz - s)

    def chip_of(s):
        return lax.rem(z - s + nz, nz)

    def block(s):
        return pl.ds(pos[s] * br, br)

    def part_of_block(s, i):
        return pl.ds(pl.multiple_of(pos[s] * br + i * UT, UT), UT)

    def par(n):
        return lax.rem(n + BIG, 2)

    def unit_rows(n):
        return pl.ds(pl.multiple_of(lax.rem(n, per_row) * UT, UT), UT)

    peers = [dev(lax.rem(z + t, nz), c) for t in range(1, nz)]
    others = [dev(lax.rem(z + t, nz), lax.rem(c + u, 2)) for t in range(nz) for u in WAYS if t or u]

    loads = []
    for cc in WAYS:
        loads.append(pltpu.make_async_copy(q_ref.at[:, cc], own.at[cc, pl.ds(0, n_qpage)], loc_sem.at[len(loads)]))
        for r in range(d_rows // PAIR):
            loads.append(pltpu.make_async_copy(d_ref.at[r, cc], own.at[cc, pl.ds(n_qpage + r * pieces, pieces)],
                                               loc_sem.at[len(loads)]))
    my_cols = pl.ds(pl.multiple_of(c * v_loc, v_loc), v_loc)
    sib_cols = pl.ds(pl.multiple_of(o * v_loc, v_loc), v_loc)
    load_w = pltpu.make_async_copy(w_ref, wbuf.at[:, my_cols], loc_sem.at[len(loads)])
    load_b = pltpu.make_async_copy(b_ref, bias.at[:, my_cols], loc_sem.at[len(loads) + 1])
    for cp in loads + [load_w, load_b]:
        cp.start()
    xbuf[...] = jnp.zeros_like(xbuf)

    where = jnp.concatenate([pos_ref[...], jnp.zeros((1, LANE - q_rows), jnp.int32)], axis=1)
    for cc in WAYS:
        tokens = jnp.concatenate([qm_ref[r:r + 1, :] for r in range(cc, q_rows, PAIR)]
                                 + [dm_ref[r:r + 1, :] for r in range(cc, d_rows, PAIR)], axis=1)
        for r in range(tokens.shape[1] // LANE):
            msgs[me, cc, r:r + 1, :] = tokens[:, r * LANE:(r + 1) * LANE].astype(F32)
        msgs[me, cc, 3:4, :] = where.astype(F32)

    barrier = pltpu.get_barrier_semaphore()
    for d in others:
        pl.semaphore_signal(barrier, device_id=d, device_id_type=MESH)
    pl.semaphore_wait(barrier, n_group - 1)

    def remote(src, dst, ss, rs, to):
        return pltpu.make_async_remote_copy(src, dst, ss, rs, device_id=to, device_id_type=MESH)

    send_m = [remote(msgs.at[me], msgs.at[me], msg_send.at[k], msg_recv.at[k], d) for k, d in enumerate(others)]
    for cp in send_m:
        cp.start()
    send_w = remote(w_ref, wbuf.at[:, my_cols], w_sem.at[0], w_sem.at[1], sib)
    send_w.start()
    send_b = remote(b_ref, bias.at[:, my_cols], bias_sem.at[0], bias_sem.at[1], sib)
    send_b.start()
    for cp in loads:
        cp.wait()

    steady = []

    def guard(cond):
        return (lambda f: f()) if cond is None else pl.when(cond)

    def exists(n):
        return None if steady else (n >= 0) & (n < n_unit)

    def choose(way, a, b):
        return jnp.where(way == 0, a, b)

    def wait_credits(sems, k, s, n, bwd):
        if steady:
            for sem in sems:
                pl.semaphore_wait(sem)
            return
        counts = [(n >= 3 - k[s], 1)]
        if bwd:
            counts.append((n < 2, 1) if s == MAXD else (n == 0, 2))
        for cond, amount in counts:
            @pl.when(cond)
            def _():
                for sem in sems:
                    pl.semaphore_wait(sem, amount)

    def hop_copy(k, n, way, dist):
        s, s0 = slot(way, dist), slot(way, dist - 1)
        return remote(xbuf.at[par(n + k[s0]), block(s0)], xbuf.at[par(n + k[s]), block(s)],
                      ag_send.at[way, dist - 1, par(n)], ag_recv.at[par(n + k[s]), s, 0], dev(ahead[way], c))

    def last_hop(k, n):
        way, s0 = par(n), MAXD - 1
        here = pl.ds(pl.multiple_of(choose(way, pos[s0] * br, pos[nz - s0] * br), br), br)
        return remote(xbuf.at[par(n + k[s0]), here], xbuf.at[par(n + k[MAXD]), block(MAXD)],
                      ag_send.at[way, s0, par(n)], ag_recv.at[par(n + k[MAXD]), MAXD, 0], dev(choose(way, right, left), c))

    def inj_copy(k, n, way, cc, i):
        s = slot(way, 1)
        return remote(own.at[cc, n // per_row, unit_rows(n)], xbuf.at[par(n + k[s]), part_of_block(s, i)],
                      inj_send.at[way, cc], ag_recv.at[par(n + k[s]), s, i], dev(ahead[way], cc))

    def sib_copy(k, n):
        return remote(own.at[o, n // per_row, unit_rows(n)], xbuf.at[par(n + k[0]), part_of_block(0, c)],
                      sib_send, ag_recv.at[par(n + k[0]), 0, 0], sib)

    def inject(k, n, bwd=False):
        @guard(exists(n))
        def _():
            both = [(way, cc) for cc in WAYS for way in WAYS]
            wait_credits([inj_cred.at[way, cc] for way, cc in both] + [sib_cred], k, 0, n, bwd)
            for way, cc in both:
                inj_copy(k, n, way, cc, c).start()
            sib_copy(k, n).start()

    def injected(k, n):
        @guard(exists(n))
        def _():
            for cc in WAYS:
                for way in WAYS:
                    inj_copy(k, n, way, cc, c).wait_send()
            sib_copy(k, n).wait_send()

    def relay(k, n, dist, bwd=False):
        @guard(exists(n))
        def _():
            if dist == MAXD:
                last_hop(k, n).wait_recv()
                return
            for way in WAYS:
                if dist == 1:
                    for i in WAYS:
                        inj_copy(k, n, way, 0, i).wait_recv()
                else:
                    hop_copy(k, n, way, dist).wait_recv()
                if dist < MAXD - 1:
                    wait_credits([ag_cred.at[way, dist]], k, slot(way, dist + 1), n, bwd)
                    hop_copy(k, n, way, dist + 1).start()
            if dist == MAXD - 1:
                wait_credits([ag_cred.at[par(n), dist]], k, MAXD, n, bwd)
                last_hop(k, n).start()

    def own_chip(k, n):
        @guard(exists(n))
        def _():
            xbuf[par(n + k[0]), part_of_block(0, c)] = own[c, n // per_row, unit_rows(n)]
            sib_copy(k, n).wait_recv()

    def give_credit(s, way, amount=1):
        dist = dist_of(s)
        if dist == 0:
            pl.semaphore_signal(sib_cred, inc=amount, device_id=sib, device_id_type=MESH)
        elif dist == 1:
            for i in WAYS:
                pl.semaphore_signal(inj_cred.at[way, c], inc=amount, device_id=dev(behind[way], i), device_id_type=MESH)
        elif dist < MAXD:
            pl.semaphore_signal(ag_cred.at[way, dist - 1], inc=amount, device_id=dev(behind[way], c), device_id_type=MESH)
        else:
            pl.semaphore_signal(ag_cred.at[way, dist - 1], inc=amount, device_id=dev(choose(way, left, right), c),
                                device_id_type=MESH)

    def way_of(s):
        return 0 if s < MAXD else 1

    def release(k, j, slots):
        for s in slots:
            n, dist = j - k[s], dist_of(s)
            if 1 <= dist < MAXD - 1 or s == MAXD - 1:
                @guard(exists(n))
                def _():
                    (last_hop(k, n) if s == MAXD - 1 else hop_copy(k, n, way_of(s), dist + 1)).wait_send()
        for s in slots:
            n = j - k[s] + 2

            @guard(exists(n))
            def _():
                give_credit(s, par(n) if s == MAXD else way_of(s))

    near, far = ORDER[:nz // PAIR], ORDER[nz // PAIR:]
    for k in (KF, KB):
        assert k[0] == k[1] == k[nz - 1] and k[MAXD - 1] == k[MAXD + 1] and {MAXD - 1, MAXD, MAXD + 1} <= set(far)

    inject(KF, ZERO)

    @pl.loop(0, rep.shape[0])
    def _(i):
        rep[i] = jnp.zeros(rep.shape[1:], F32)

    @pl.loop(0, PAD)
    def _(i):
        maskx[i] = jnp.zeros(maskx.shape[1:], F32)
        maskx[PAD + n_unit + i] = jnp.zeros(maskx.shape[1:], F32)
    gbacc[...] = jnp.zeros_like(gbacc)

    @pl.loop(0, hid // BIG)
    def _(i):
        gw[pl.ds(pl.multiple_of(i * BIG, BIG), BIG), :] = jnp.zeros((BIG, v_chip), F32)

    for cp in send_m:
        cp.wait()

    in_row = LANE // UT
    for s in range(nz):
        for i in WAYS:
            for r in range(n_unit // in_row):
                tile = jnp.broadcast_to(msgs[PAIR * chip_of(s) + i, c, r:r + 1, :], (LANE, LANE)).T
                for t in range(in_row):
                    at = pos[s] * br + i * UT
                    maskx[PAD + r * in_row + t, at:at + UT, :] = tile[t * UT:(t + 1) * UT, :]

    relay(KF, ZERO, 1)
    injected(KF, ZERO)
    load_w.wait()
    load_b.wait()
    send_w.wait()
    send_b.wait()

    def pages(j, k):
        after = {d: (j - d + PAD) // per_row for d in set(k)}
        return [after[k[s]] for s in range(nz)]

    def mask_rows(j, k, slots):
        return jnp.concatenate([maskx[j - k[s] + PAD, block(s), :] for s in slots], axis=0)

    def fwd_group(j, b, g, k0, k1):
        slots = (near, far)[g]
        page = pages(j, KF)

        @functools.partial(lax.fori_loop, k0, k1, init_val=None, unroll=UNROLL)
        def _(k, _):
            at = pl.ds(pl.multiple_of(k * CH, CH), CH)
            logits = jnp.dot(xbuf[b, g * half:(g + 1) * half], wbuf[:, at], preferred_element_type=F32)
            for t in range(CH // LANE):
                at = pl.ds(pl.multiple_of(k * CH + t * LANE, LANE), LANE)
                zt = logits[:, t * LANE:(t + 1) * LANE] + bias[:, at]
                act = jnp.log(1.0 + jnp.maximum(zt, 0.0)) * mask_rows(j, KF, slots)
                for i, s in enumerate(slots):
                    for u in WAYS:
                        r0 = i * br + u * UT
                        row_sum = jnp.sum(act[r0:r0 + UT, :], axis=0, keepdims=True)
                        rep[page[s], PAIR * s + u:PAIR * s + u + 1, at] = rep[page[s], PAIR * s + u:PAIR * s + u + 1, at] + row_sum

    def cut(eighths):
        return n_chunk * eighths // SUB

    fwd_end = n_unit + KF[MAXD]

    def release_far(j):
        @pl.when(j >= 1)
        def _():
            release(KF, j, far)

    @pl.loop(1, fwd_end)
    def _(j):
        b = par(j)
        release_far(j - 1)
        inject(KF, j)
        own_chip(KF, j - KF[0])
        near_left = j < n_unit + max(KF[s] for s in near)

        @pl.when(near_left)
        def _():
            fwd_group(j, b, 0, 0, cut(6))
        relay(KF, j - 2, 3)

        @pl.when(near_left)
        def _():
            fwd_group(j, b, 0, cut(6), n_chunk)
        release(KF, j, near)
        relay(KF, j - 1, 2)
        relay(KF, j - 3, 4)
        fwd_group(j, b, 1, 0, cut(4))
        relay(KF, j, 1)
        fwd_group(j, b, 1, cut(4), n_chunk)
        injected(KF, j)

        @pl.when(j <= v_chip // 256)
        def _():
            for u in WAYS:
                at = pl.ds(pl.multiple_of((j - 1) * 256 + u * LANE, LANE), LANE)
                wt[at, :] = wbuf[:, at].T

    release_far(jnp.int32(fwd_end - 1))

    for s in range(nz):
        if s == MAXD:
            for way in WAYS:
                give_credit(s, way)
        else:
            give_credit(s, way_of(s), 2)

    q_total = q_rows * n_group
    d_total = d_rows * n_group
    v_total = v_loc * n_group
    tau = q_len * math.sqrt(v_total * d_len) / 16.0
    lam_q = 4.0 / (v_total * q_len * q_len)
    lam_d = 4.0 / (v_total * d_len * d_len)
    nd = d_rows // PAIR * n_group
    nq = q_rows // PAIR * n_group
    q0 = PAD // per_row
    d0 = q0 + n_qpage

    @pl.loop(0, v_chip // CB)
    def _(k):
        at = pl.ds(pl.multiple_of(k * CB, CB), CB)
        for r in range(d_rows // PAIR):
            rdx[c, r * n_group:(r + 1) * n_group, at] = sum(rep[d0 + r * pieces + i, :, at] for i in range(pieces))
        q_sum = sum(rep[q0 + i, :, at] for i in range(n_qpage))
        rdx[c, nd:nd + SUB, at] = sum(q_sum[i * SUB:(i + 1) * SUB] for i in range(n_group // SUB))

    def to_sib(src, dst, i):
        return remote(src, dst, pair_sem.at[i, 0], pair_sem.at[i, 1], sib)

    send_rd = to_sib(rdx.at[c], rdx.at[c], 0)
    send_rd.start()
    inject(KB, ZERO, BWD)
    send_rd.wait()

    def d_reps(at):
        return jnp.concatenate([rdx[0, 0:nd, at], rdx[1, 0:nd, at]], axis=0)

    def q_mean_of(at):
        return jnp.sum(rdx[0, nd:nd + SUB, at] + rdx[1, nd:nd + SUB, at], axis=0, keepdims=True) * (1.0 / q_total)

    def d_mean_of(at):
        return jnp.sum(d_reps(at), axis=0, keepdims=True) * (1.0 / d_total)

    def lanes(v):
        return sum(v[:, t * LANE:(t + 1) * LANE] for t in range(CB // LANE))

    def score_chunk(k, carry):
        s_acc, rq, rd = carry
        at = pl.ds(pl.multiple_of(k * CB, CB), CB)
        q_rep = rep[q0:q0 + n_qpage, :, at].reshape(nq, CB)
        s_acc = s_acc + lax.dot_general(d_reps(at), q_rep, (((1,), (1,)), ((), ())), precision=HIGHEST,
                                        preferred_element_type=F32)
        qm, dm = q_mean_of(at), d_mean_of(at)
        return s_acc, rq + lanes(qm * qm), rd + lanes(dm * dm)

    score, reg_q, reg_d = lax.fori_loop(0, v_chip // CB, score_chunk,
                                        (jnp.zeros((PAIR * nd, nq), F32), jnp.zeros((1, LANE), F32), jnp.zeros((1, LANE), F32)))

    def turn(n):
        i = lax.broadcasted_iota(jnp.int32, (n, n), 0)
        k = lax.broadcasted_iota(jnp.int32, (n, n), 1)
        same = (i // n_group == k // n_group) & (i % 2 == k % 2)
        return (same & (((i // PAIR) % nz + (k // PAIR) % nz) % nz == z)).astype(F32)

    def exact(a, b):
        return jnp.dot(a, b, precision=HIGHEST, preferred_element_type=F32)

    turn_d, turn_q = turn(PAIR * nd), turn(nq)
    smsg[0, 0:PAIR * nd, 0:nq] = exact(exact(turn_d, score), turn_q)
    smsg[0, PAIR * nd:PAIR * nd + 1, :] = reg_q
    smsg[0, PAIR * nd + 1:PAIR * nd + 2, :] = reg_d
    send_s = [remote(smsg.at[0], smsg.at[t], sm_send.at[t], sm_recv.at[t], peers[t - 1]) for t in range(1, nz)]
    for cp in send_s:
        cp.start()

    pos_rows = jnp.concatenate([msgs[i, 0, 3:4, :] for i in range(n_group)], axis=0)
    spread = (lax.broadcasted_iota(jnp.int32, (LANE, nq), 0)
              == PAIR * (lax.broadcasted_iota(jnp.int32, (LANE, nq), 1) // n_group) + c).astype(F32)
    pos_all = exact(pos_rows, spread)
    pick = (lax.broadcasted_iota(jnp.int32, (n_group, nq), 1) % n_group
            == lax.broadcasted_iota(jnp.int32, (n_group, nq), 0))
    pos_row = jnp.sum(jnp.where(pick, pos_all, 0.0), axis=0, keepdims=True)
    ridx = lax.broadcasted_iota(jnp.int32, (PAIR * nd, nq), 0)
    doc = (ridx % n_group) * d_rows + PAIR * ((ridx % nd) // n_group) + ridx // nd
    target = (doc.astype(F32) == pos_row).astype(F32)

    relay(KB, ZERO, 1, BWD)
    injected(KB, ZERO)
    for cp in send_s:
        cp.wait()
    total = smsg[0]
    for t in range(1, nz):
        total = total + smsg[t]
    scores = total[0:PAIR * nd, 0:nq] * (1.0 / tau)
    top = jnp.max(scores, axis=0, keepdims=True)
    log_norm = top + jnp.log(jnp.sum(jnp.exp(scores - top), axis=0, keepdims=True))
    row_loss = log_norm - jnp.sum(scores * target, axis=0, keepdims=True)
    loss_part = jnp.sum(row_loss, axis=1, keepdims=True)
    gt = (jnp.exp(scores - log_norm) - target) * (1.0 / (q_total * tau))
    gt = exact(exact(turn_d, gt), turn_q)
    g = gt.T
    lossx[c] = jnp.broadcast_to(loss_part, (SUB, LANE))
    send_l = to_sib(lossx.at[c], lossx.at[c], 1)
    send_l.start()
    inject(KB, ZERO + 1, BWD)
    relay(KB, ZERO, 2, BWD)

    @pl.loop(0, v_chip // CB)
    def _(k):
        at = pl.ds(pl.multiple_of(k * CB, CB), CB)
        q_rep = rep[q0:q0 + n_qpage, :, at].reshape(nq, CB)
        dp = exact(gt, q_rep)
        ddx[0, :, at] = dp[0:nd]
        ddx[1, :, at] = dp[nd:PAIR * nd]

    send_dd = to_sib(ddx.at[o], ddr, 2)
    send_dd.start()

    @pl.loop(0, v_chip // CB)
    def _(k):
        at = pl.ds(pl.multiple_of(k * CB, CB), CB)
        gq = exact(g, d_reps(at)) + q_mean_of(at) * (2.0 * lam_q / q_total)
        rep[q0:q0 + n_qpage, :, at] = gq.reshape(n_qpage, n_group, CB)

    send_l.wait()
    reg = (jnp.sum(total[PAIR * nd:PAIR * nd + 1, :], axis=1, keepdims=True) * lam_q
           + jnp.sum(total[PAIR * nd + 1:PAIR * nd + 2, :], axis=1, keepdims=True) * lam_d)
    lossf[0] = (lossx[0] + lossx[1]) * (1.0 / q_total) + reg

    send_loss = [remote(lossf.at[0], lossf.at[1], loss_send.at[t], loss_recv, peers[t - 1]) for t in range(1, nz)]

    @pl.when(z == 0)
    def _():
        for cp in send_loss:
            cp.start()
    relay(KB, ZERO + 1, 1, BWD)
    injected(KB, ZERO + 1)
    relay(KB, ZERO, 3, BWD)
    send_dd.wait()

    @pl.loop(0, v_chip // CB)
    def _(k):
        at = pl.ds(pl.multiple_of(k * CB, CB), CB)
        gd = ddx[c, :, at] + ddr[:, at] + d_mean_of(at) * (2.0 * lam_d / d_total)
        for r in range(d_rows // PAIR):
            for i in range(pieces):
                rep[d0 + r * pieces + i, :, at] = gd[r * n_group:(r + 1) * n_group]

    def bwd_chunk(j, b, page, k, slots=ORDER, weights=BWD):
        at0 = pos[slots[0]] * br
        some = slice(at0, at0 + len(slots) * br)
        cols = pl.ds(pl.multiple_of(k * CB, CB), CB)
        logits = jnp.dot(xbuf[b, some], wbuf[:, cols], preferred_element_type=F32)
        low = []
        for t in range(CB // LANE):
            at = pl.ds(pl.multiple_of(k * CB + t * LANE, LANE), LANE)
            zt = logits[:, t * LANE:(t + 1) * LANE] + bias[:, at]
            grad = jnp.concatenate([jnp.broadcast_to(rep[page[s], PAIR * s + u:PAIR * s + u + 1, at], (UT, LANE))
                                    for s in slots for u in WAYS], axis=0)
            gz = jnp.where(zt > 0.0, grad * mask_rows(j, KB, slots) / (1.0 + jnp.maximum(zt, 0.0)), 0.0)
            gbacc[:, at] = gbacc[:, at] + jnp.sum(gz.reshape(-1, SUB, LANE), axis=0)
            low.append(gz.astype(BF16))
        low = jnp.concatenate(low, axis=1)
        gbuf[some, cols] = low
        if weights:
            gw[:, cols] = gw[:, cols] + jnp.dot(xt[...], low, preferred_element_type=F32)

    def bwd_hidden(k0, k1, some=slice(None)):
        wide = hid // 4

        @functools.partial(lax.fori_loop, k0, k1, init_val=None, unroll=UNROLL)
        def _(k, _):
            cols = pl.ds(pl.multiple_of(k * wide, wide), wide)
            pbuf[some, cols] = jnp.dot(gbuf[some, :], wt[:, cols], preferred_element_type=F32).astype(BF16)

    def deep(n):
        return lax.rem(n + BIG, DEEP)

    def room(n):
        return lax.rem(n + BIG, ROOM)

    def rs_copy(n, way, dist):
        to = behind[way] if isinstance(way, int) else choose(way, left, right)
        return remote(sbuf.at[way, dist - 1], rbuf.at[way, dist - 2, room(n)], rs_send.at[way, dist - 1],
                      rs_recv.at[way, dist - 2, room(n)], dev(to, c))

    def home_copy(n, way, cc, i):
        return remote(sbuf.at[way, 0, pl.ds(i * UT, UT)], hbuf.at[way, cc, room(n)], h_send.at[way, i],
                      h_recv.at[way, cc, room(n)], dev(behind[way], i))

    def pair_copy(n):
        return remote(sst.at[par(n)], sibp.at[deep(n)], sp_send.at[par(n)], sp_recv.at[deep(n)], sib)

    def rs_sent(n, dist):
        @guard(exists(n))
        def _():
            if dist == MAXD:
                rs_copy(n, par(n), dist).wait_send()
                return
            for way in WAYS:
                if dist == 1:
                    for i in WAYS:
                        home_copy(n, way, c, i).wait_send()
                else:
                    rs_copy(n, way, dist).wait_send()

    def rs_both(n, dist):
        rs_sent(n - (2 if dist == MAXD else 1), dist)

        def joined(way, mine):
            rs_copy(n, way, dist + 1).wait_recv()
            sbuf[way, dist - 1] = (mine.astype(F32) + rbuf[way, dist - 1, room(n)].astype(F32)).astype(BF16)

        @guard(exists(n))
        def _():
            if dist == MAXD:
                sbuf[par(n), dist - 1] = pbuf[block(MAXD), :]
                rs_copy(n, par(n), dist).start()
            elif dist == MAXD - 1:
                way = par(n)
                sbuf[1 - way, dist - 1] = part[choose(way, nz - dist, dist), deep(n)]
                rs_copy(n, 1 - way, dist).start()
                joined(way, part[choose(way, dist, nz - dist), deep(n)])
                rs_copy(n, way, dist).start()
            else:
                for way in WAYS:
                    joined(way, part[slot(way, dist), deep(n)])
                    if dist == 1:
                        for i in WAYS:
                            home_copy(n, way, c, i).start()
                    else:
                        rs_copy(n, way, dist).start()

    def rs_home(n):
        @guard(exists(n))
        def _():
            for cc in WAYS:
                for way in WAYS:
                    home_copy(n, way, cc, 0).wait_recv()
                at = unit_rows(n)
                acc_h[cc, n // per_row, at] = (acc_h[cc, n // per_row, at].astype(F32) + hbuf[0, cc, room(n)].astype(F32)
                                               + hbuf[1, cc, room(n)].astype(F32)).astype(BF16)

    def pair_send(n):
        @guard(exists(n - 2))
        def _():
            pair_copy(n - 2).wait_send()

        @guard(exists(n))
        def _():
            sst[par(n)] = pbuf[part_of_block(0, o), :]
            pair_copy(n).start()
            acc_h[c, n // per_row, unit_rows(n)] = pbuf[part_of_block(0, c), :]

    def pair_take(n):
        @guard(exists(n))
        def _():
            pair_copy(n).wait_recv()
            acc_h[o, n // per_row, unit_rows(n)] = sibp[deep(n)]

    last = n_unit + KB[MAXD]
    assert all(n_unit + KB[s] < last for s in near)

    def part_b(eighths):
        return v_chip // CB * eighths // SUB

    def bwd_step(j):
        b = par(j)
        page = pages(j, KB)
        late = None if steady else j >= 2

        def weights(k0, k1):
            @functools.partial(lax.fori_loop, k0, k1, init_val=None, unroll=UNROLL)
            def _(k, _):
                bwd_chunk(j, b, page, k)

        relay(KB, j - 2, 4)
        own_chip(KB, j - 1)
        rs_both(j - 3, 4)
        rs_both(j - 5, 1)
        xt[...] = xbuf[b].T
        weights(0, part_b(4))

        @guard(late)
        def _():
            relay(KB, j, 1, BWD)
        rs_both(j - 4, 2)
        weights(part_b(4), part_b(6))

        @guard(late)
        def _():
            relay(KB, j - 1, 3, BWD)
        weights(part_b(6), v_chip // CB)
        release(KB, j, ORDER)
        rs_both(j - 3, 3)
        bwd_hidden(0, 3)

        @guard(late)
        def _():
            injected(KB, j)
        inject(KB, j + 1, BWD)
        relay(KB, j, 2, BWD)
        rs_home(j - 5)
        bwd_hidden(3, 4)
        for s in range(1, nz):
            if s != MAXD:
                part[s, deep(j - KB[s])] = pbuf[block(s), :]
        pair_send(j - 1)
        pair_take(j - 2)

    @pl.loop(1, last - 1)
    def _(j):
        middle = (j >= 6) & (j < n_unit - 1)

        @pl.when(middle)
        def _():
            steady.append(BWD)
            bwd_step(j)
            steady.pop()

        @pl.when(jnp.logical_not(middle))
        def _():
            bwd_step(j)

    j = ZERO + last - 1
    b = par(j)
    page = pages(j, KB)
    some = slice(half, rows)
    relay(KB, j - 2, 4)
    rs_both(j - 3, 4)
    rs_both(j - 5, 1)

    @functools.partial(lax.fori_loop, 0, v_chip // CB, init_val=None, unroll=UNROLL)
    def _(k, _):
        bwd_chunk(j, b, page, k, far, False)
    rs_both(j - 4, 2)
    bwd_hidden(0, 4, some)
    for s in far:
        if s != MAXD:
            part[s, deep(j - KB[s])] = pbuf[block(s), :]
    rs_both(j + 1 - 3, 4)
    rs_both(j - 3, 3)
    release(KB, j, ORDER)
    pair_send(j - 1)
    pair_take(j - 2)
    rs_home(j - 5)
    xt[:, some] = xbuf[b, some].T

    @functools.partial(lax.fori_loop, 0, v_chip // CB, init_val=None, unroll=UNROLL)
    def _(k, _):
        cols = pl.ds(pl.multiple_of(k * CB, CB), CB)
        gw[:, cols] = gw[:, cols] + jnp.dot(xt[:, some], gbuf[some, cols], preferred_element_type=F32)

    n_part = gx_send.shape[0] - 1
    step = v_loc // n_part
    send_g = []
    for k in range(n_part):
        theirs = pl.ds(pl.multiple_of(o * v_loc + k * step, step), step)
        send_g.append(remote(gw.at[:, theirs], grecv.at[k % PAIR], gx_send.at[k], gx_recv.at[k], sib))
    send_gb = remote(gbacc.at[:, sib_cols], gbrecv, gx_send.at[n_part], gx_recv.at[n_part], sib)
    for cp in send_g[:PAIR]:
        cp.start()
    send_gb.start()

    w_outs = []

    def add_part():
        k = len(w_outs)
        send_g[k].wait_recv()
        at = pl.ds(pl.multiple_of(c * v_loc + k * step, step), step)

        @pl.loop(0, hid // BIG)
        def _(i):
            rr = pl.ds(pl.multiple_of(i * BIG, BIG), BIG)
            wbuf[rr, at] = (gw[rr, at] + grecv[k % PAIR, rr]).astype(BF16)
        w_outs.append(pltpu.make_async_copy(wbuf.at[:, at], gw_out.at[:, pl.ds(k * step, step)], out_sem.at[n_load + k]))
        w_outs[-1].start()
        if k + PAIR < n_part:
            pl.semaphore_signal(gx_cred, device_id=sib, device_id_type=MESH)
            pl.semaphore_wait(gx_cred)
            send_g[k + PAIR].start()

    n_load = len(loads)
    for j in range(last, n_unit + 5):
        n = ZERO + j
        if j > last:
            rs_both(n - 3, 4)
        rs_both(n - 5, 1)
        if j > last:
            add_part()
        rs_both(n - 4, 2)
        rs_both(n - 3, 3)
        pair_send(n - 1)
        if j == last:
            add_part()
        rs_home(n - 5)
    rs_sent(jnp.int32(n_unit - 1), 1)

    outs = []
    for cc in WAYS:
        outs.append(pltpu.make_async_copy(acc_h.at[cc, pl.ds(0, n_qpage)], dq_out.at[:, cc], out_sem.at[len(outs)]))
        for r in range(d_rows // PAIR):
            outs.append(pltpu.make_async_copy(acc_h.at[cc, pl.ds(n_qpage + r * pieces, pieces)], dd_out.at[r, cc],
                                              out_sem.at[len(outs)]))
    for cp in outs:
        cp.start()
    while len(w_outs) < n_part:
        add_part()
    send_gb.wait_recv()
    gb_ref[...] = jnp.sum(gbacc[:, my_cols] + gbrecv[...], axis=0, keepdims=True)

    @pl.when(z == 0)
    def _():
        for cp in send_loss:
            cp.wait_send()
        loss_ref[...] = lossf[0, 0:1, 0:1]

    @pl.when(z != 0)
    def _():
        send_loss[0].wait_recv()
        loss_ref[...] = lossf[1, 0:1, 0:1]
    for cp in send_g:
        cp.wait_send()
    send_gb.wait_send()
    for cp in outs + w_outs:
        cp.wait()


def solution(mesh):
    n_group = mesh.shape['tp']
    nz = n_group // PAIR
    row_spec = P(('dp', 'tp'))
    mask_spec = P(('dp', 'tp'), None)
    hid_spec = P(('dp', 'tp'), None, None)

    def local_step(q_hidden, d_hidden, q_mask, d_mask, positive, w_head, b_head):
        q_rows, q_len, hid = q_hidden.shape
        d_rows, d_len, _ = d_hidden.shape
        v_loc = w_head.shape[1]
        v_chip = PAIR * v_loc
        per_row = q_len // UT
        pieces = d_len // q_len
        n_page = q_rows // PAIR + d_rows // PAIR * pieces
        n_unit = n_page * per_row
        rows = nz * PAIR * UT
        nd, nq = d_rows // PAIR * n_group, q_rows // PAIR * n_group
        s_rows = -(-(PAIR * nd + 2) // SUB) * SUB
        n_part = 4 if v_loc >= 512 else 2
        n_load = PAIR * (1 + d_rows // PAIR)
        dma, reg = pltpu.SemaphoreType.DMA, pltpu.SemaphoreType.REGULAR
        anym = pl.BlockSpec(memory_space=pl.ANY)
        vm = pl.BlockSpec(memory_space=pltpu.VMEM)
        q_shape = (q_rows // PAIR, 2, q_len, hid)
        d_shape = (d_rows // PAIR, 2, pieces, q_len, hid)
        out_shape = (
            jax.ShapeDtypeStruct((1, 1), F32),
            jax.ShapeDtypeStruct((hid, v_loc), BF16),
            jax.ShapeDtypeStruct((1, v_loc), F32),
            jax.ShapeDtypeStruct(q_shape, BF16),
            jax.ShapeDtypeStruct(d_shape, BF16),
        )
        scratch = [
            pltpu.VMEM((hid, v_chip), BF16),
            pltpu.VMEM((v_chip, hid), BF16),
            pltpu.VMEM((hid, v_chip), F32),
            pltpu.VMEM((PAIR, hid, v_loc // n_part), F32),
            pltpu.VMEM(((n_unit + PAIR * PAD) // per_row, n_group, v_chip), F32),
            pltpu.VMEM((n_unit + PAIR * PAD, rows, LANE), F32),
            pltpu.VMEM((PAIR, n_page, q_len, hid), BF16),
            pltpu.VMEM((PAIR, n_page, q_len, hid), BF16),
            pltpu.VMEM((nz, DEEP, PAIR * UT, hid), BF16),
            pltpu.VMEM((PAIR, rows, hid), BF16),
            pltpu.VMEM((PAIR, MAXD - 1, ROOM, PAIR * UT, hid), BF16),
            pltpu.VMEM((PAIR, MAXD, PAIR * UT, hid), BF16),
            pltpu.VMEM((PAIR, 2, ROOM, UT, hid), BF16),
            pltpu.VMEM((DEEP, UT, hid), BF16),
            pltpu.VMEM((PAIR, UT, hid), BF16),
            pltpu.VMEM((rows, v_chip), BF16),
            pltpu.VMEM((rows, hid), BF16),
            pltpu.VMEM((hid, rows), BF16),
            pltpu.VMEM((PAIR, nd + SUB, v_chip), F32),
            pltpu.VMEM((PAIR, nd, v_chip), F32),
            pltpu.VMEM((nd, v_chip), F32),
            pltpu.VMEM((1, v_chip), F32),
            pltpu.VMEM((SUB, v_chip), F32),
            pltpu.VMEM((SUB, v_loc), F32),
            pltpu.VMEM((n_group, 2, 4, LANE), F32),
            pltpu.VMEM((nz, s_rows, LANE), F32),
            pltpu.VMEM((PAIR, SUB, LANE), F32),
            pltpu.VMEM((PAIR, SUB, LANE), F32),
            dma((PAIR, MAXD, 2)), dma((PAIR, nz, 2)), reg((PAIR, MAXD)), dma((PAIR, 2)), reg((PAIR, 2)), dma, reg,
            dma((PAIR, MAXD)), dma((PAIR, MAXD - 1, ROOM)), dma((PAIR, 2)), dma((PAIR, 2, ROOM)),
            dma((PAIR,)), dma((DEEP,)),
            dma((n_load + PAIR,)), dma((PAIR,)), dma((PAIR,)), dma((n_group - 1,)), dma((n_group - 1,)), dma((nz,)), dma((nz,)),
            dma((3, 2)), dma((n_part + 1,)), dma((n_part + 1,)), reg, dma((nz,)), dma, dma((n_load + n_part,)),
        ]
        loss, gw, gb, dq, dd = pl.pallas_call(
            functools.partial(kernel, n_group, q_rows, q_len, d_rows, d_len),
            out_shape=out_shape,
            in_specs=[anym] * 4 + [vm] * 3,
            out_specs=(vm, anym, vm, anym, anym),
            scratch_shapes=scratch,
            compiler_params=pltpu.CompilerParams(collective_id=0, has_side_effects=True, vmem_limit_bytes=67043328),
        )(q_hidden.reshape(q_shape), d_hidden.reshape(d_shape), w_head, b_head.reshape(1, v_loc),
          q_mask, d_mask, positive.reshape(1, q_rows))
        return (loss.reshape(1), gw, gb.reshape(v_loc), dq.reshape(q_hidden.shape), dd.reshape(d_hidden.shape))

    return jax.shard_map(local_step, mesh=mesh,
                         in_specs=(hid_spec, hid_spec, mask_spec, mask_spec, row_spec, P(None, 'tp'), P('tp')),
                         out_specs=(P('dp'), P('dp', 'tp'), row_spec, hid_spec, hid_spec),
                         check_vma=False)
```

```python
import functools
import math
import jax
import jax.numpy as jnp
from jax import lax
from jax.experimental import pallas as pl
from jax.experimental.pallas import tpu as pltpu
from jax.sharding import PartitionSpec as P

MESH = pl.DeviceIdType.MESH
HIGHEST = lax.Precision.HIGHEST
F32 = jnp.float32
BF16 = jnp.bfloat16
BWD = UNROLL = True

UT = 16
CH = 512
CB = 1024
MAXD = 4
KF = (1, 1, 2, 2, 3, 2, 1, 1)
KB = (1, 1, 1, 2, 2, 2, 1, 1)
LANE, SUB, PAIR, BIG = 128, 8, 2, 64
DEEP = 4
ROOM = 8
WAYS = (0, 1)
ORDER = (0, 1, 7, 2, 6, 3, 5, 4)
PAD = 4


def kernel(n_group, q_rows, q_len, d_rows, d_len,
           q_ref, d_ref, w_ref, b_ref, qm_ref, dm_ref, pos_ref,
           loss_ref, gw_out, gb_ref, dq_out, dd_out,
           wbuf, wt, gw, grecv, rep, maskx, own, acc_h, part, xbuf, rbuf, sbuf, hbuf, sibp, sst, gbuf, pbuf, xt,
           rdx, ddx, ddr, bias, gbacc, gbrecv, msgs, smsg, lossx, lossf,
           ag_send, ag_recv, ag_cred, inj_send, inj_cred, sib_send, sib_cred,
           rs_send, rs_recv, h_send, h_recv, sp_send, sp_recv,
           loc_sem, w_sem, bias_sem, msg_send, msg_recv, sm_send, sm_recv, pair_sem, gx_send, gx_recv, gx_cred,
           loss_send, loss_recv, out_sem):
    ZERO = jnp.int32(0)
    nz = n_group // PAIR
    hid = w_ref.shape[0]
    v_loc = w_ref.shape[1]
    v_chip = PAIR * v_loc
    per_row = q_len // UT
    pieces = d_len // q_len
    n_qpage = q_rows // PAIR
    n_dpage = d_rows // PAIR * pieces
    n_page = n_qpage + n_dpage
    n_unit = n_page * per_row
    br = PAIR * UT
    rows = nz * br
    half = rows // PAIR
    n_chunk = v_chip // CH
    pos = {s: i for i, s in enumerate(ORDER)}

    me = lax.axis_index('tp')
    z = me // PAIR
    c = lax.rem(me, 2)
    o = 1 - c
    right = lax.rem(z + 1, nz)
    left = lax.rem(z + nz - 1, nz)

    def dev(zz, cc):
        return {'tp': PAIR * zz + cc}

    sib = dev(z, o)
    ahead = (right, left)
    behind = (left, right)

    def slot(way, dist):
        return dist if way == 0 else nz - dist

    def dist_of(s):
        return min(s, nz - s)

    def chip_of(s):
        return lax.rem(z - s + nz, nz)

    def block(s):
        return pl.ds(pos[s] * br, br)

    def part_of_block(s, i):
        return pl.ds(pl.multiple_of(pos[s] * br + i * UT, UT), UT)

    def par(n):
        return lax.rem(n + BIG, 2)

    def unit_rows(n):
        return pl.ds(pl.multiple_of(lax.rem(n, per_row) * UT, UT), UT)

    peers = [dev(lax.rem(z + t, nz), c) for t in range(1, nz)]
    others = [dev(lax.rem(z + t, nz), lax.rem(c + u, 2)) for t in range(nz) for u in WAYS if t or u]

    loads = []
    for cc in WAYS:
        loads.append(pltpu.make_async_copy(q_ref.at[:, cc], own.at[cc, pl.ds(0, n_qpage)], loc_sem.at[len(loads)]))
        for r in range(d_rows // PAIR):
            loads.append(pltpu.make_async_copy(d_ref.at[r, cc], own.at[cc, pl.ds(n_qpage + r * pieces, pieces)],
                                               loc_sem.at[len(loads)]))
    my_cols = pl.ds(pl.multiple_of(c * v_loc, v_loc), v_loc)
    sib_cols = pl.ds(pl.multiple_of(o * v_loc, v_loc), v_loc)
    load_w = pltpu.make_async_copy(w_ref, wbuf.at[:, my_cols], loc_sem.at[len(loads)])
    load_b = pltpu.make_async_copy(b_ref, bias.at[:, my_cols], loc_sem.at[len(loads) + 1])
    for cp in loads + [load_w, load_b]:
        cp.start()
    xbuf[...] = jnp.zeros_like(xbuf)

    where = jnp.concatenate([pos_ref[...], jnp.zeros((1, LANE - q_rows), jnp.int32)], axis=1)
    for cc in WAYS:
        tokens = jnp.concatenate([qm_ref[r:r + 1, :] for r in range(cc, q_rows, PAIR)]
                                 + [dm_ref[r:r + 1, :] for r in range(cc, d_rows, PAIR)], axis=1)
        for r in range(tokens.shape[1] // LANE):
            msgs[me, cc, r:r + 1, :] = tokens[:, r * LANE:(r + 1) * LANE].astype(F32)
        msgs[me, cc, 3:4, :] = where.astype(F32)

    barrier = pltpu.get_barrier_semaphore()
    for d in others:
        pl.semaphore_signal(barrier, device_id=d, device_id_type=MESH)
    pl.semaphore_wait(barrier, n_group - 1)

    def remote(src, dst, ss, rs, to):
        return pltpu.make_async_remote_copy(src, dst, ss, rs, device_id=to, device_id_type=MESH)

    send_m = [remote(msgs.at[me], msgs.at[me], msg_send.at[k], msg_recv.at[k], d) for k, d in enumerate(others)]
    for cp in send_m:
        cp.start()
    send_w = remote(w_ref, wbuf.at[:, my_cols], w_sem.at[0], w_sem.at[1], sib)
    send_w.start()
    send_b = remote(b_ref, bias.at[:, my_cols], bias_sem.at[0], bias_sem.at[1], sib)
    send_b.start()
    for cp in loads:
        cp.wait()

    steady = []

    def guard(cond):
        return (lambda f: f()) if cond is None else pl.when(cond)

    def exists(n):
        return None if steady else (n >= 0) & (n < n_unit)

    def choose(way, a, b):
        return jnp.where(way == 0, a, b)

    def wait_credits(sems, k, s, n, bwd):
        if steady:
            for sem in sems:
                pl.semaphore_wait(sem)
            return
        counts = [(n >= 3 - k[s], 1)]
        if bwd:
            counts.append((n < 2, 1) if s == MAXD else (n == 0, 2))
        for cond, amount in counts:
            @pl.when(cond)
            def _():
                for sem in sems:
                    pl.semaphore_wait(sem, amount)

    def hop_copy(k, n, way, dist):
        s, s0 = slot(way, dist), slot(way, dist - 1)
        return remote(xbuf.at[par(n + k[s0]), block(s0)], xbuf.at[par(n + k[s]), block(s)],
                      ag_send.at[way, dist - 1, par(n)], ag_recv.at[par(n + k[s]), s, 0], dev(ahead[way], c))

    def last_hop(k, n):
        way, s0 = par(n), MAXD - 1
        here = pl.ds(pl.multiple_of(choose(way, pos[s0] * br, pos[nz - s0] * br), br), br)
        return remote(xbuf.at[par(n + k[s0]), here], xbuf.at[par(n + k[MAXD]), block(MAXD)],
                      ag_send.at[way, s0, par(n)], ag_recv.at[par(n + k[MAXD]), MAXD, 0], dev(choose(way, right, left), c))

    def inj_copy(k, n, way, cc, i):
        s = slot(way, 1)
        return remote(own.at[cc, n // per_row, unit_rows(n)], xbuf.at[par(n + k[s]), part_of_block(s, i)],
                      inj_send.at[way, cc], ag_recv.at[par(n + k[s]), s, i], dev(ahead[way], cc))

    def sib_copy(k, n):
        return remote(own.at[o, n // per_row, unit_rows(n)], xbuf.at[par(n + k[0]), part_of_block(0, c)],
                      sib_send, ag_recv.at[par(n + k[0]), 0, 0], sib)

    def inject(k, n, bwd=False):
        @guard(exists(n))
        def _():
            both = [(way, cc) for cc in WAYS for way in WAYS]
            wait_credits([inj_cred.at[way, cc] for way, cc in both] + [sib_cred], k, 0, n, bwd)
            for way, cc in both:
                inj_copy(k, n, way, cc, c).start()
            sib_copy(k, n).start()

    def injected(k, n):
        @guard(exists(n))
        def _():
            for cc in WAYS:
                for way in WAYS:
                    inj_copy(k, n, way, cc, c).wait_send()
            sib_copy(k, n).wait_send()

    def relay(k, n, dist, bwd=False):
        @guard(exists(n))
        def _():
            if dist == MAXD:
                last_hop(k, n).wait_recv()
                return
            for way in WAYS:
                if dist == 1:
                    for i in WAYS:
                        inj_copy(k, n, way, 0, i).wait_recv()
                else:
                    hop_copy(k, n, way, dist).wait_recv()
                if dist < MAXD - 1:
                    wait_credits([ag_cred.at[way, dist]], k, slot(way, dist + 1), n, bwd)
                    hop_copy(k, n, way, dist + 1).start()
            if dist == MAXD - 1:
                wait_credits([ag_cred.at[par(n), dist]], k, MAXD, n, bwd)
                last_hop(k, n).start()

    def own_chip(k, n):
        @guard(exists(n))
        def _():
            xbuf[par(n + k[0]), part_of_block(0, c)] = own[c, n // per_row, unit_rows(n)]
            sib_copy(k, n).wait_recv()

    def give_credit(s, way, amount=1):
        dist = dist_of(s)
        if dist == 0:
            pl.semaphore_signal(sib_cred, inc=amount, device_id=sib, device_id_type=MESH)
        elif dist == 1:
            for i in WAYS:
                pl.semaphore_signal(inj_cred.at[way, c], inc=amount, device_id=dev(behind[way], i), device_id_type=MESH)
        elif dist < MAXD:
            pl.semaphore_signal(ag_cred.at[way, dist - 1], inc=amount, device_id=dev(behind[way], c), device_id_type=MESH)
        else:
            pl.semaphore_signal(ag_cred.at[way, dist - 1], inc=amount, device_id=dev(choose(way, left, right), c),
                                device_id_type=MESH)

    def way_of(s):
        return 0 if s < MAXD else 1

    def release(k, j, slots):
        for s in slots:
            n, dist = j - k[s], dist_of(s)
            if 1 <= dist < MAXD - 1 or s == MAXD - 1:
                @guard(exists(n))
                def _():
                    (last_hop(k, n) if s == MAXD - 1 else hop_copy(k, n, way_of(s), dist + 1)).wait_send()
        for s in slots:
            n = j - k[s] + 2

            @guard(exists(n))
            def _():
                give_credit(s, par(n) if s == MAXD else way_of(s))

    near, far = ORDER[:nz // PAIR], ORDER[nz // PAIR:]
    for k in (KF, KB):
        assert k[0] == k[1] == k[nz - 1] and k[MAXD - 1] == k[MAXD + 1] and {MAXD - 1, MAXD, MAXD + 1} <= set(far)

    inject(KF, ZERO)

    @pl.loop(0, rep.shape[0])
    def _(i):
        rep[i] = jnp.zeros(rep.shape[1:], F32)

    @pl.loop(0, PAD)
    def _(i):
        maskx[i] = jnp.zeros(maskx.shape[1:], F32)
        maskx[PAD + n_unit + i] = jnp.zeros(maskx.shape[1:], F32)
    gbacc[...] = jnp.zeros_like(gbacc)

    @pl.loop(0, hid // BIG)
    def _(i):
        gw[pl.ds(pl.multiple_of(i * BIG, BIG), BIG), :] = jnp.zeros((BIG, v_chip), F32)

    for cp in send_m:
        cp.wait()

    in_row = LANE // UT
    for s in range(nz):
        for i in WAYS:
            for r in range(n_unit // in_row):
                tile = jnp.broadcast_to(msgs[PAIR * chip_of(s) + i, c, r:r + 1, :], (LANE, LANE)).T
                for t in range(in_row):
                    at = pos[s] * br + i * UT
                    maskx[PAD + r * in_row + t, at:at + UT, :] = tile[t * UT:(t + 1) * UT, :]

    relay(KF, ZERO, 1)
    injected(KF, ZERO)
    load_w.wait()
    load_b.wait()
    send_w.wait()
    send_b.wait()

    def pages(j, k):
        after = {d: (j - d + PAD) // per_row for d in set(k)}
        return [after[k[s]] for s in range(nz)]

    def mask_rows(j, k, slots):
        return jnp.concatenate([maskx[j - k[s] + PAD, block(s), :] for s in slots], axis=0)

    def fwd_group(j, b, g, k0, k1):
        slots = (near, far)[g]
        page = pages(j, KF)

        @functools.partial(lax.fori_loop, k0, k1, init_val=None, unroll=UNROLL)
        def _(k, _):
            at = pl.ds(pl.multiple_of(k * CH, CH), CH)
            logits = jnp.dot(xbuf[b, g * half:(g + 1) * half], wbuf[:, at], preferred_element_type=F32)
            for t in range(CH // LANE):
                at = pl.ds(pl.multiple_of(k * CH + t * LANE, LANE), LANE)
                zt = logits[:, t * LANE:(t + 1) * LANE] + bias[:, at]
                act = jnp.log(1.0 + jnp.maximum(zt, 0.0)) * mask_rows(j, KF, slots)
                for i, s in enumerate(slots):
                    for u in WAYS:
                        r0 = i * br + u * UT
                        row_sum = jnp.sum(act[r0:r0 + UT, :], axis=0, keepdims=True)
                        rep[page[s], PAIR * s + u:PAIR * s + u + 1, at] = rep[page[s], PAIR * s + u:PAIR * s + u + 1, at] + row_sum

    def cut(eighths):
        return n_chunk * eighths // SUB

    fwd_end = n_unit + KF[MAXD]

    def release_far(j):
        @pl.when(j >= 1)
        def _():
            release(KF, j, far)

    @pl.loop(1, fwd_end)
    def _(j):
        b = par(j)
        release_far(j - 1)
        inject(KF, j)
        own_chip(KF, j - KF[0])
        near_left = j < n_unit + max(KF[s] for s in near)

        @pl.when(near_left)
        def _():
            fwd_group(j, b, 0, 0, cut(6))
        relay(KF, j - 2, 3)

        @pl.when(near_left)
        def _():
            fwd_group(j, b, 0, cut(6), n_chunk)
        release(KF, j, near)
        relay(KF, j - 1, 2)
        relay(KF, j - 3, 4)
        fwd_group(j, b, 1, 0, cut(4))
        relay(KF, j, 1)
        fwd_group(j, b, 1, cut(4), n_chunk)
        injected(KF, j)

    release_far(jnp.int32(fwd_end - 1))

    for s in range(nz):
        if s == MAXD:
            for way in WAYS:
                give_credit(s, way)
        else:
            give_credit(s, way_of(s), 2)

    q_total = q_rows * n_group
    d_total = d_rows * n_group
    v_total = v_loc * n_group
    tau = q_len * math.sqrt(v_total * d_len) / 16.0
    lam_q = 4.0 / (v_total * q_len * q_len)
    lam_d = 4.0 / (v_total * d_len * d_len)
    nd = d_rows // PAIR * n_group
    nq = q_rows // PAIR * n_group
    q0 = PAD // per_row
    d0 = q0 + n_qpage

    @pl.loop(0, v_chip // CB)
    def _(k):
        at = pl.ds(pl.multiple_of(k * CB, CB), CB)
        for r in range(d_rows // PAIR):
            rdx[c, r * n_group:(r + 1) * n_group, at] = sum(rep[d0 + r * pieces + i, :, at] for i in range(pieces))
        q_sum = sum(rep[q0 + i, :, at] for i in range(n_qpage))
        rdx[c, nd:nd + SUB, at] = sum(q_sum[i * SUB:(i + 1) * SUB] for i in range(n_group // SUB))

    def to_sib(src, dst, i):
        return remote(src, dst, pair_sem.at[i, 0], pair_sem.at[i, 1], sib)

    send_rd = to_sib(rdx.at[c], rdx.at[c], 0)
    send_rd.start()
    inject(KB, ZERO, BWD)
    send_rd.wait()

    def d_reps(at):
        return jnp.concatenate([rdx[0, 0:nd, at], rdx[1, 0:nd, at]], axis=0)

    def q_mean_of(at):
        return jnp.sum(rdx[0, nd:nd + SUB, at] + rdx[1, nd:nd + SUB, at], axis=0, keepdims=True) * (1.0 / q_total)

    def d_mean_of(at):
        return jnp.sum(d_reps(at), axis=0, keepdims=True) * (1.0 / d_total)

    def lanes(v):
        return sum(v[:, t * LANE:(t + 1) * LANE] for t in range(CB // LANE))

    def score_chunk(k, carry):
        s_acc, rq, rd = carry
        at = pl.ds(pl.multiple_of(k * CB, CB), CB)
        q_rep = rep[q0:q0 + n_qpage, :, at].reshape(nq, CB)
        s_acc = s_acc + lax.dot_general(d_reps(at), q_rep, (((1,), (1,)), ((), ())), precision=HIGHEST,
                                        preferred_element_type=F32)
        qm, dm = q_mean_of(at), d_mean_of(at)
        return s_acc, rq + lanes(qm * qm), rd + lanes(dm * dm)

    score, reg_q, reg_d = lax.fori_loop(0, v_chip // CB, score_chunk,
                                        (jnp.zeros((PAIR * nd, nq), F32), jnp.zeros((1, LANE), F32), jnp.zeros((1, LANE), F32)))

    def turn(n):
        i = lax.broadcasted_iota(jnp.int32, (n, n), 0)
        k = lax.broadcasted_iota(jnp.int32, (n, n), 1)
        same = (i // n_group == k // n_group) & (i % 2 == k % 2)
        return (same & (((i // PAIR) % nz + (k // PAIR) % nz) % nz == z)).astype(F32)

    def exact(a, b):
        return jnp.dot(a, b, precision=HIGHEST, preferred_element_type=F32)

    turn_d, turn_q = turn(PAIR * nd), turn(nq)
    smsg[0, 0:PAIR * nd, 0:nq] = exact(exact(turn_d, score), turn_q)
    smsg[0, PAIR * nd:PAIR * nd + 1, :] = reg_q
    smsg[0, PAIR * nd + 1:PAIR * nd + 2, :] = reg_d
    send_s = [remote(smsg.at[0], smsg.at[t], sm_send.at[t], sm_recv.at[t], peers[t - 1]) for t in range(1, nz)]
    for cp in send_s:
        cp.start()

    @pl.loop(0, v_chip // LANE)
    def _(k):
        at = pl.ds(pl.multiple_of(k * LANE, LANE), LANE)
        wt[at, :] = wbuf[:, at].T

    pos_rows = jnp.concatenate([msgs[i, 0, 3:4, :] for i in range(n_group)], axis=0)
    spread = (lax.broadcasted_iota(jnp.int32, (LANE, nq), 0)
              == PAIR * (lax.broadcasted_iota(jnp.int32, (LANE, nq), 1) // n_group) + c).astype(F32)
    pos_all = exact(pos_rows, spread)
    pick = (lax.broadcasted_iota(jnp.int32, (n_group, nq), 1) % n_group
            == lax.broadcasted_iota(jnp.int32, (n_group, nq), 0))
    pos_row = jnp.sum(jnp.where(pick, pos_all, 0.0), axis=0, keepdims=True)
    ridx = lax.broadcasted_iota(jnp.int32, (PAIR * nd, nq), 0)
    doc = (ridx % n_group) * d_rows + PAIR * ((ridx % nd) // n_group) + ridx // nd
    target = (doc.astype(F32) == pos_row).astype(F32)

    relay(KB, ZERO, 1, BWD)
    injected(KB, ZERO)
    for cp in send_s:
        cp.wait()
    total = smsg[0]
    for t in range(1, nz):
        total = total + smsg[t]
    scores = total[0:PAIR * nd, 0:nq] * (1.0 / tau)
    top = jnp.max(scores, axis=0, keepdims=True)
    log_norm = top + jnp.log(jnp.sum(jnp.exp(scores - top), axis=0, keepdims=True))
    row_loss = log_norm - jnp.sum(scores * target, axis=0, keepdims=True)
    loss_part = jnp.sum(row_loss, axis=1, keepdims=True)
    gt = (jnp.exp(scores - log_norm) - target) * (1.0 / (q_total * tau))
    gt = exact(exact(turn_d, gt), turn_q)
    g = gt.T
    lossx[c] = jnp.broadcast_to(loss_part, (SUB, LANE))
    send_l = to_sib(lossx.at[c], lossx.at[c], 1)
    send_l.start()
    inject(KB, ZERO + 1, BWD)
    relay(KB, ZERO, 2, BWD)

    @pl.loop(0, v_chip // CB)
    def _(k):
        at = pl.ds(pl.multiple_of(k * CB, CB), CB)
        q_rep = rep[q0:q0 + n_qpage, :, at].reshape(nq, CB)
        dp = exact(gt, q_rep)
        ddx[0, :, at] = dp[0:nd]
        ddx[1, :, at] = dp[nd:PAIR * nd]

    send_dd = to_sib(ddx.at[o], ddr, 2)
    send_dd.start()

    @pl.loop(0, v_chip // CB)
    def _(k):
        at = pl.ds(pl.multiple_of(k * CB, CB), CB)
        gq = exact(g, d_reps(at)) + q_mean_of(at) * (2.0 * lam_q / q_total)
        rep[q0:q0 + n_qpage, :, at] = gq.reshape(n_qpage, n_group, CB)

    send_l.wait()
    reg = (jnp.sum(total[PAIR * nd:PAIR * nd + 1, :], axis=1, keepdims=True) * lam_q
           + jnp.sum(total[PAIR * nd + 1:PAIR * nd + 2, :], axis=1, keepdims=True) * lam_d)
    lossf[0] = (lossx[0] + lossx[1]) * (1.0 / q_total) + reg

    send_loss = [remote(lossf.at[0], lossf.at[1], loss_send.at[t], loss_recv, peers[t - 1]) for t in range(1, nz)]

    @pl.when(z == 0)
    def _():
        for cp in send_loss:
            cp.start()
    relay(KB, ZERO + 1, 1, BWD)
    injected(KB, ZERO + 1)
    relay(KB, ZERO, 3, BWD)
    send_dd.wait()

    @pl.loop(0, v_chip // CB)
    def _(k):
        at = pl.ds(pl.multiple_of(k * CB, CB), CB)
        gd = ddx[c, :, at] + ddr[:, at] + d_mean_of(at) * (2.0 * lam_d / d_total)
        for r in range(d_rows // PAIR):
            for i in range(pieces):
                rep[d0 + r * pieces + i, :, at] = gd[r * n_group:(r + 1) * n_group]

    def bwd_chunk(j, b, page, k, slots=ORDER, weights=BWD):
        at0 = pos[slots[0]] * br
        some = slice(at0, at0 + len(slots) * br)
        cols = pl.ds(pl.multiple_of(k * CB, CB), CB)
        logits = jnp.dot(xbuf[b, some], wbuf[:, cols], preferred_element_type=F32)
        low = []
        for t in range(CB // LANE):
            at = pl.ds(pl.multiple_of(k * CB + t * LANE, LANE), LANE)
            zt = logits[:, t * LANE:(t + 1) * LANE] + bias[:, at]
            grad = jnp.concatenate([jnp.broadcast_to(rep[page[s], PAIR * s + u:PAIR * s + u + 1, at], (UT, LANE))
                                    for s in slots for u in WAYS], axis=0)
            gz = jnp.where(zt > 0.0, grad * mask_rows(j, KB, slots) / (1.0 + jnp.maximum(zt, 0.0)), 0.0)
            gbacc[:, at] = gbacc[:, at] + jnp.sum(gz.reshape(-1, SUB, LANE), axis=0)
            low.append(gz.astype(BF16))
        low = jnp.concatenate(low, axis=1)
        gbuf[some, cols] = low
        if weights:
            gw[:, cols] = gw[:, cols] + jnp.dot(xt[...], low, preferred_element_type=F32)

    def bwd_hidden(k0, k1, some=slice(None)):
        wide = hid // 4

        @functools.partial(lax.fori_loop, k0, k1, init_val=None, unroll=UNROLL)
        def _(k, _):
            cols = pl.ds(pl.multiple_of(k * wide, wide), wide)
            pbuf[some, cols] = jnp.dot(gbuf[some, :], wt[:, cols], preferred_element_type=F32).astype(BF16)

    def deep(n):
        return lax.rem(n + BIG, DEEP)

    def room(n):
        return lax.rem(n + BIG, ROOM)

    def rs_copy(n, way, dist):
        to = behind[way] if isinstance(way, int) else choose(way, left, right)
        return remote(sbuf.at[way, dist - 1], rbuf.at[way, dist - 2, room(n)], rs_send.at[way, dist - 1],
                      rs_recv.at[way, dist - 2, room(n)], dev(to, c))

    def home_copy(n, way, cc, i):
        return remote(sbuf.at[way, 0, pl.ds(i * UT, UT)], hbuf.at[way, cc, room(n)], h_send.at[way, i],
                      h_recv.at[way, cc, room(n)], dev(behind[way], i))

    def pair_copy(n):
        return remote(sst.at[par(n)], sibp.at[deep(n)], sp_send.at[par(n)], sp_recv.at[deep(n)], sib)

    def rs_sent(n, dist):
        @guard(exists(n))
        def _():
            if dist == MAXD:
                rs_copy(n, par(n), dist).wait_send()
                return
            for way in WAYS:
                if dist == 1:
                    for i in WAYS:
                        home_copy(n, way, c, i).wait_send()
                else:
                    rs_copy(n, way, dist).wait_send()

    def rs_both(n, dist):
        rs_sent(n - (2 if dist == MAXD else 1), dist)

        def joined(way, mine):
            rs_copy(n, way, dist + 1).wait_recv()
            sbuf[way, dist - 1] = (mine.astype(F32) + rbuf[way, dist - 1, room(n)].astype(F32)).astype(BF16)

        @guard(exists(n))
        def _():
            if dist == MAXD:
                sbuf[par(n), dist - 1] = pbuf[block(MAXD), :]
                rs_copy(n, par(n), dist).start()
            elif dist == MAXD - 1:
                way = par(n)
                sbuf[1 - way, dist - 1] = part[choose(way, nz - dist, dist), deep(n)]
                rs_copy(n, 1 - way, dist).start()
                joined(way, part[choose(way, dist, nz - dist), deep(n)])
                rs_copy(n, way, dist).start()
            else:
                for way in WAYS:
                    joined(way, part[slot(way, dist), deep(n)])
                    if dist == 1:
                        for i in WAYS:
                            home_copy(n, way, c, i).start()
                    else:
                        rs_copy(n, way, dist).start()

    def rs_home(n):
        @guard(exists(n))
        def _():
            for cc in WAYS:
                for way in WAYS:
                    home_copy(n, way, cc, 0).wait_recv()
                at = unit_rows(n)
                acc_h[cc, n // per_row, at] = (acc_h[cc, n // per_row, at].astype(F32) + hbuf[0, cc, room(n)].astype(F32)
                                               + hbuf[1, cc, room(n)].astype(F32)).astype(BF16)

    def pair_send(n):
        @guard(exists(n - 2))
        def _():
            pair_copy(n - 2).wait_send()

        @guard(exists(n))
        def _():
            sst[par(n)] = pbuf[part_of_block(0, o), :]
            pair_copy(n).start()
            acc_h[c, n // per_row, unit_rows(n)] = pbuf[part_of_block(0, c), :]

    def pair_take(n):
        @guard(exists(n))
        def _():
            pair_copy(n).wait_recv()
            acc_h[o, n // per_row, unit_rows(n)] = sibp[deep(n)]

    last = n_unit + KB[MAXD]
    assert all(n_unit + KB[s] < last for s in near)

    def part_b(eighths):
        return v_chip // CB * eighths // SUB

    def bwd_step(j):
        b = par(j)
        page = pages(j, KB)
        late = None if steady else j >= 2

        def weights(k0, k1):
            @functools.partial(lax.fori_loop, k0, k1, init_val=None, unroll=UNROLL)
            def _(k, _):
                bwd_chunk(j, b, page, k)

        @guard(late)
        def _():
            relay(KB, j - 1, 2, BWD)
        relay(KB, j - 2, 4)
        own_chip(KB, j - 1)
        xt[...] = xbuf[b].T
        weights(0, part_b(2))
        rs_both(j - 3, 4)
        rs_both(j - 5, 1)
        weights(part_b(2), part_b(4))

        @guard(late)
        def _():
            relay(KB, j, 1, BWD)
        weights(part_b(4), part_b(6))

        @guard(late)
        def _():
            relay(KB, j - 1, 3, BWD)
        rs_both(j - 4, 2)
        weights(part_b(6), v_chip // CB)
        release(KB, j, ORDER)
        rs_both(j - 3, 3)
        bwd_hidden(0, 2)

        @guard(late)
        def _():
            injected(KB, j)
        inject(KB, j + 1, BWD)
        bwd_hidden(2, 3)
        rs_home(j - 5)
        bwd_hidden(3, 4)
        for s in range(1, nz):
            if s != MAXD:
                part[s, deep(j - KB[s])] = pbuf[block(s), :]
        pair_send(j - 1)
        pair_take(j - 2)

    @pl.loop(1, last - 1)
    def _(j):
        middle = (j >= 6) & (j < n_unit - 1)

        @pl.when(middle)
        def _():
            steady.append(BWD)
            bwd_step(j)
            steady.pop()

        @pl.when(jnp.logical_not(middle))
        def _():
            bwd_step(j)

    j = ZERO + last - 1
    b = par(j)
    page = pages(j, KB)
    some = slice(half, rows)
    relay(KB, j - 2, 4)
    rs_both(j - 3, 4)
    rs_both(j - 5, 1)

    @functools.partial(lax.fori_loop, 0, v_chip // CB, init_val=None, unroll=UNROLL)
    def _(k, _):
        bwd_chunk(j, b, page, k, far, False)
    rs_both(j - 4, 2)
    bwd_hidden(0, 4, some)
    for s in far:
        if s != MAXD:
            part[s, deep(j - KB[s])] = pbuf[block(s), :]
    rs_both(j + 1 - 3, 4)
    rs_both(j - 3, 3)
    release(KB, j, ORDER)
    pair_send(j - 1)
    pair_take(j - 2)
    rs_home(j - 5)
    xt[:, some] = xbuf[b, some].T

    @functools.partial(lax.fori_loop, 0, v_chip // CB, init_val=None, unroll=UNROLL)
    def _(k, _):
        cols = pl.ds(pl.multiple_of(k * CB, CB), CB)
        gw[:, cols] = gw[:, cols] + jnp.dot(xt[:, some], gbuf[some, cols], preferred_element_type=F32)

    n_part = gx_send.shape[0] - 1
    step = v_loc // n_part
    send_g = []
    for k in range(n_part):
        theirs = pl.ds(pl.multiple_of(o * v_loc + k * step, step), step)
        send_g.append(remote(gw.at[:, theirs], grecv.at[k % PAIR], gx_send.at[k], gx_recv.at[k], sib))
    send_gb = remote(gbacc.at[:, sib_cols], gbrecv, gx_send.at[n_part], gx_recv.at[n_part], sib)
    for cp in send_g[:PAIR]:
        cp.start()
    send_gb.start()

    w_outs = []

    def add_part():
        k = len(w_outs)
        send_g[k].wait_recv()
        at = pl.ds(pl.multiple_of(c * v_loc + k * step, step), step)

        @pl.loop(0, hid // BIG)
        def _(i):
            rr = pl.ds(pl.multiple_of(i * BIG, BIG), BIG)
            wbuf[rr, at] = (gw[rr, at] + grecv[k % PAIR, rr]).astype(BF16)
        w_outs.append(pltpu.make_async_copy(wbuf.at[:, at], gw_out.at[:, pl.ds(k * step, step)], out_sem.at[n_load + k]))
        w_outs[-1].start()
        if k + PAIR < n_part:
            pl.semaphore_signal(gx_cred, device_id=sib, device_id_type=MESH)
            pl.semaphore_wait(gx_cred)
            send_g[k + PAIR].start()

    n_load = len(loads)
    for j in range(last, n_unit + 5):
        n = ZERO + j
        if j > last:
            rs_both(n - 3, 4)
        rs_both(n - 5, 1)
        if j > last:
            add_part()
        rs_both(n - 4, 2)
        rs_both(n - 3, 3)
        pair_send(n - 1)
        if j == last:
            add_part()
        rs_home(n - 5)
    rs_sent(jnp.int32(n_unit - 1), 1)

    outs = []
    for cc in WAYS:
        outs.append(pltpu.make_async_copy(acc_h.at[cc, pl.ds(0, n_qpage)], dq_out.at[:, cc], out_sem.at[len(outs)]))
        for r in range(d_rows // PAIR):
            outs.append(pltpu.make_async_copy(acc_h.at[cc, pl.ds(n_qpage + r * pieces, pieces)], dd_out.at[r, cc],
                                              out_sem.at[len(outs)]))
    for cp in outs:
        cp.start()
    while len(w_outs) < n_part:
        add_part()
    send_gb.wait_recv()
    gb_ref[...] = jnp.sum(gbacc[:, my_cols] + gbrecv[...], axis=0, keepdims=True)

    @pl.when(z == 0)
    def _():
        for cp in send_loss:
            cp.wait_send()
        loss_ref[...] = lossf[0, 0:1, 0:1]

    @pl.when(z != 0)
    def _():
        send_loss[0].wait_recv()
        loss_ref[...] = lossf[1, 0:1, 0:1]
    for cp in send_g:
        cp.wait_send()
    send_gb.wait_send()
    for cp in outs + w_outs:
        cp.wait()


def settle(*refs):
    n = len(refs) // 4
    copies = []
    for a, z, buf, sem in zip(*(refs[k * n:(k + 1) * n] for k in range(4))):
        pieces = sem.shape[1]
        size = a.shape[0] // pieces
        for p in range(pieces):
            at = pl.ds(p * size, size)
            copies.append((pltpu.make_async_copy(a.at[at], buf.at[at], sem.at[0, p]),
                           pltpu.make_async_copy(buf.at[at], z.at[at], sem.at[1, p])))
    for cp, _ in copies:
        cp.start()
    for cp, back in copies:
        cp.wait()
        back.start()
    for _, back in copies:
        back.wait()


def solution(mesh):
    n_group = mesh.shape['tp']
    nz = n_group // PAIR
    row_spec = P(('dp', 'tp'))
    mask_spec = P(('dp', 'tp'), None)
    hid_spec = P(('dp', 'tp'), None, None)

    def local_step(q_hidden, d_hidden, q_mask, d_mask, positive, w_head, b_head):
        q_rows, q_len, hid = q_hidden.shape
        d_rows, d_len, _ = d_hidden.shape
        v_loc = w_head.shape[1]
        v_chip = PAIR * v_loc
        per_row = q_len // UT
        pieces = d_len // q_len
        n_page = q_rows // PAIR + d_rows // PAIR * pieces
        n_unit = n_page * per_row
        rows = nz * PAIR * UT
        nd, nq = d_rows // PAIR * n_group, q_rows // PAIR * n_group
        s_rows = -(-(PAIR * nd + 2) // SUB) * SUB
        n_part = 4 if v_loc >= 512 else 2
        n_load = PAIR * (1 + d_rows // PAIR)
        dma, reg = pltpu.SemaphoreType.DMA, pltpu.SemaphoreType.REGULAR
        anym = pl.BlockSpec(memory_space=pl.ANY)
        vm = pl.BlockSpec(memory_space=pltpu.VMEM)
        q_shape = (q_rows // PAIR, 2, q_len, hid)
        d_shape = (d_rows // PAIR, 2, pieces, q_len, hid)
        out_shape = (
            jax.ShapeDtypeStruct((1, 1), F32),
            jax.ShapeDtypeStruct((hid, v_loc), BF16),
            jax.ShapeDtypeStruct((1, v_loc), F32),
            jax.ShapeDtypeStruct(q_shape, BF16),
            jax.ShapeDtypeStruct(d_shape, BF16),
        )
        scratch = [
            pltpu.VMEM((hid, v_chip), BF16),
            pltpu.VMEM((v_chip, hid), BF16),
            pltpu.VMEM((hid, v_chip), F32),
            pltpu.VMEM((PAIR, hid, v_loc // n_part), F32),
            pltpu.VMEM(((n_unit + PAIR * PAD) // per_row, n_group, v_chip), F32),
            pltpu.VMEM((n_unit + PAIR * PAD, rows, LANE), F32),
            pltpu.VMEM((PAIR, n_page, q_len, hid), BF16),
            pltpu.VMEM((PAIR, n_page, q_len, hid), BF16),
            pltpu.VMEM((nz, DEEP, PAIR * UT, hid), BF16),
            pltpu.VMEM((PAIR, rows, hid), BF16),
            pltpu.VMEM((PAIR, MAXD - 1, ROOM, PAIR * UT, hid), BF16),
            pltpu.VMEM((PAIR, MAXD, PAIR * UT, hid), BF16),
            pltpu.VMEM((PAIR, 2, ROOM, UT, hid), BF16),
            pltpu.VMEM((DEEP, UT, hid), BF16),
            pltpu.VMEM((PAIR, UT, hid), BF16),
            pltpu.VMEM((rows, v_chip), BF16),
            pltpu.VMEM((rows, hid), BF16),
            pltpu.VMEM((hid, rows), BF16),
            pltpu.VMEM((PAIR, nd + SUB, v_chip), F32),
            pltpu.VMEM((PAIR, nd, v_chip), F32),
            pltpu.VMEM((nd, v_chip), F32),
            pltpu.VMEM((1, v_chip), F32),
            pltpu.VMEM((SUB, v_chip), F32),
            pltpu.VMEM((SUB, v_loc), F32),
            pltpu.VMEM((n_group, 2, 4, LANE), F32),
            pltpu.VMEM((nz, s_rows, LANE), F32),
            pltpu.VMEM((PAIR, SUB, LANE), F32),
            pltpu.VMEM((PAIR, SUB, LANE), F32),
            dma((PAIR, MAXD, 2)), dma((PAIR, nz, 2)), reg((PAIR, MAXD)), dma((PAIR, 2)), reg((PAIR, 2)), dma, reg,
            dma((PAIR, MAXD)), dma((PAIR, MAXD - 1, ROOM)), dma((PAIR, 2)), dma((PAIR, 2, ROOM)),
            dma((PAIR,)), dma((DEEP,)),
            dma((n_load + PAIR,)), dma((PAIR,)), dma((PAIR,)), dma((n_group - 1,)), dma((n_group - 1,)), dma((nz,)), dma((nz,)),
            dma((3, 2)), dma((n_part + 1,)), dma((n_part + 1,)), reg, dma((nz,)), dma, dma((n_load + n_part,)),
        ]
        loss, gw, gb, dq, dd = pl.pallas_call(
            functools.partial(kernel, n_group, q_rows, q_len, d_rows, d_len),
            out_shape=out_shape,
            in_specs=[anym] * 4 + [vm] * 3,
            out_specs=(vm, anym, vm, anym, anym),
            scratch_shapes=scratch,
            compiler_params=pltpu.CompilerParams(collective_id=0, has_side_effects=True, vmem_limit_bytes=67043328),
        )(q_hidden.reshape(q_shape), d_hidden.reshape(d_shape), w_head, b_head.reshape(1, v_loc),
          q_mask, d_mask, positive.reshape(1, q_rows))
        results = (gw, dq, dd, gb, loss)
        gw, dq, dd, gb, loss = pl.pallas_call(
            settle,
            out_shape=[jax.ShapeDtypeStruct(a.shape, a.dtype) for a in results],
            in_specs=[anym] * len(results),
            out_specs=[anym] * len(results),
            scratch_shapes=[pltpu.VMEM(a.shape, a.dtype) for a in results] + [dma((2, math.gcd(4, a.shape[0]))) for a in results],
            compiler_params=pltpu.CompilerParams(vmem_limit_bytes=67043328),
        )(*results)
        return (loss.reshape(1), gw, gb.reshape(v_loc), dq.reshape(q_hidden.shape), dd.reshape(d_hidden.shape))

    return jax.shard_map(local_step, mesh=mesh,
                         in_specs=(hid_spec, hid_spec, mask_spec, mask_spec, row_spec, P(None, 'tp'), P('tp')),
                         out_specs=(P('dp'), P('dp', 'tp'), row_spec, hid_spec, hid_spec),
                         check_vma=False)
```

```python
import functools
import math
import jax
import jax.numpy as jnp
from jax import lax
from jax.experimental import pallas as pl
from jax.experimental.pallas import tpu as pltpu
from jax.sharding import PartitionSpec as P

MESH = pl.DeviceIdType.MESH
HIGHEST = lax.Precision.HIGHEST
F32 = jnp.float32
BF16 = jnp.bfloat16
BWD = UNROLL = True

UT = 16
CH = 512
CB = 1024
MAXD = 4
KF = (1, 1, 2, 2, 3, 2, 1, 1)
KB = (1, 1, 1, 2, 2, 2, 1, 1)
LANE, SUB, PAIR, BIG = 128, 8, 2, 64
DEEP = 4
ROOM = 8
WAYS = (0, 1)
ORDER = (0, 1, 7, 2, 6, 3, 5, 4)
PAD = 4


def kernel(n_group, q_rows, q_len, d_rows, d_len,
           q_ref, d_ref, w_ref, b_ref, qm_ref, dm_ref, pos_ref,
           loss_ref, gw_out, gb_ref, dq_out, dd_out,
           wbuf, wt, gw, grecv, rep, maskx, own, acc_h, part, xbuf, rbuf, sbuf, hbuf, sibp, sst, gbuf, pbuf, xt,
           rdx, ddx, ddr, bias, gbacc, gbrecv, msgs, smsg, lossx, lossf,
           ag_send, ag_recv, ag_cred, inj_send, inj_cred, sib_send, sib_cred,
           rs_send, rs_recv, h_send, h_recv, sp_send, sp_recv,
           loc_sem, w_sem, bias_sem, msg_send, msg_recv, sm_send, sm_recv, pair_sem, gx_send, gx_recv, gx_cred,
           loss_send, loss_recv, out_sem):
    ZERO = jnp.int32(0)
    nz = n_group // PAIR
    hid = w_ref.shape[0]
    v_loc = w_ref.shape[1]
    v_chip = PAIR * v_loc
    per_row = q_len // UT
    pieces = d_len // q_len
    n_qpage = q_rows // PAIR
    n_dpage = d_rows // PAIR * pieces
    n_page = n_qpage + n_dpage
    n_unit = n_page * per_row
    br = PAIR * UT
    rows = nz * br
    half = rows // PAIR
    n_chunk = v_chip // CH
    pos = {s: i for i, s in enumerate(ORDER)}

    me = lax.axis_index('tp')
    z = me // PAIR
    c = lax.rem(me, 2)
    o = 1 - c
    right = lax.rem(z + 1, nz)
    left = lax.rem(z + nz - 1, nz)

    def dev(zz, cc):
        return {'tp': PAIR * zz + cc}

    sib = dev(z, o)
    ahead = (right, left)
    behind = (left, right)

    def slot(way, dist):
        return dist if way == 0 else nz - dist

    def dist_of(s):
        return min(s, nz - s)

    def chip_of(s):
        return lax.rem(z - s + nz, nz)

    def block(s):
        return pl.ds(pos[s] * br, br)

    def part_of_block(s, i):
        return pl.ds(pl.multiple_of(pos[s] * br + i * UT, UT), UT)

    def par(n):
        return lax.rem(n + BIG, 2)

    def unit_rows(n):
        return pl.ds(pl.multiple_of(lax.rem(n, per_row) * UT, UT), UT)

    peers = [dev(lax.rem(z + t, nz), c) for t in range(1, nz)]
    others = [dev(lax.rem(z + t, nz), lax.rem(c + u, 2)) for t in range(nz) for u in WAYS if t or u]

    loads = []
    for cc in WAYS:
        loads.append(pltpu.make_async_copy(q_ref.at[:, cc], own.at[cc, pl.ds(0, n_qpage)], loc_sem.at[len(loads)]))
        for r in range(d_rows // PAIR):
            loads.append(pltpu.make_async_copy(d_ref.at[r, cc], own.at[cc, pl.ds(n_qpage + r * pieces, pieces)],
                                               loc_sem.at[len(loads)]))
    my_cols = pl.ds(pl.multiple_of(c * v_loc, v_loc), v_loc)
    sib_cols = pl.ds(pl.multiple_of(o * v_loc, v_loc), v_loc)
    load_w = pltpu.make_async_copy(w_ref, wbuf.at[:, my_cols], loc_sem.at[len(loads)])
    load_b = pltpu.make_async_copy(b_ref, bias.at[:, my_cols], loc_sem.at[len(loads) + 1])
    for cp in loads + [load_w, load_b]:
        cp.start()
    xbuf[...] = jnp.zeros_like(xbuf)

    where = jnp.concatenate([pos_ref[...], jnp.zeros((1, LANE - q_rows), jnp.int32)], axis=1)
    for cc in WAYS:
        tokens = jnp.concatenate([qm_ref[r:r + 1, :] for r in range(cc, q_rows, PAIR)]
                                 + [dm_ref[r:r + 1, :] for r in range(cc, d_rows, PAIR)], axis=1)
        for r in range(tokens.shape[1] // LANE):
            msgs[me, cc, r:r + 1, :] = tokens[:, r * LANE:(r + 1) * LANE].astype(F32)
        msgs[me, cc, 3:4, :] = where.astype(F32)

    barrier = pltpu.get_barrier_semaphore()
    for d in others:
        pl.semaphore_signal(barrier, device_id=d, device_id_type=MESH)
    pl.semaphore_wait(barrier, n_group - 1)

    def remote(src, dst, ss, rs, to):
        return pltpu.make_async_remote_copy(src, dst, ss, rs, device_id=to, device_id_type=MESH)

    send_m = [remote(msgs.at[me], msgs.at[me], msg_send.at[k], msg_recv.at[k], d) for k, d in enumerate(others)]
    for cp in send_m:
        cp.start()
    send_w = remote(w_ref, wbuf.at[:, my_cols], w_sem.at[0], w_sem.at[1], sib)
    send_w.start()
    send_b = remote(b_ref, bias.at[:, my_cols], bias_sem.at[0], bias_sem.at[1], sib)
    send_b.start()
    for cp in loads:
        cp.wait()

    steady = []

    def guard(cond):
        return (lambda f: f()) if cond is None else pl.when(cond)

    def exists(n):
        return None if steady else (n >= 0) & (n < n_unit)

    def choose(way, a, b):
        return jnp.where(way == 0, a, b)

    def wait_credits(sems, k, s, n, bwd):
        if steady:
            for sem in sems:
                pl.semaphore_wait(sem)
            return
        counts = [(n >= 3 - k[s], 1)]
        if bwd:
            counts.append((n < 2, 1) if s == MAXD else (n == 0, 2))
        for cond, amount in counts:
            @pl.when(cond)
            def _():
                for sem in sems:
                    pl.semaphore_wait(sem, amount)

    def hop_copy(k, n, way, dist):
        s, s0 = slot(way, dist), slot(way, dist - 1)
        return remote(xbuf.at[par(n + k[s0]), block(s0)], xbuf.at[par(n + k[s]), block(s)],
                      ag_send.at[way, dist - 1, par(n)], ag_recv.at[par(n + k[s]), s, 0], dev(ahead[way], c))

    def last_hop(k, n):
        way, s0 = par(n), MAXD - 1
        here = pl.ds(pl.multiple_of(choose(way, pos[s0] * br, pos[nz - s0] * br), br), br)
        return remote(xbuf.at[par(n + k[s0]), here], xbuf.at[par(n + k[MAXD]), block(MAXD)],
                      ag_send.at[way, s0, par(n)], ag_recv.at[par(n + k[MAXD]), MAXD, 0], dev(choose(way, right, left), c))

    def inj_copy(k, n, way, cc, i):
        s = slot(way, 1)
        return remote(own.at[cc, n // per_row, unit_rows(n)], xbuf.at[par(n + k[s]), part_of_block(s, i)],
                      inj_send.at[way, cc], ag_recv.at[par(n + k[s]), s, i], dev(ahead[way], cc))

    def sib_copy(k, n):
        return remote(own.at[o, n // per_row, unit_rows(n)], xbuf.at[par(n + k[0]), part_of_block(0, c)],
                      sib_send, ag_recv.at[par(n + k[0]), 0, 0], sib)

    def inject(k, n, bwd=False):
        @guard(exists(n))
        def _():
            both = [(way, cc) for cc in WAYS for way in WAYS]
            wait_credits([inj_cred.at[way, cc] for way, cc in both] + [sib_cred], k, 0, n, bwd)
            for way, cc in both:
                inj_copy(k, n, way, cc, c).start()
            sib_copy(k, n).start()

    def injected(k, n):
        @guard(exists(n))
        def _():
            for cc in WAYS:
                for way in WAYS:
                    inj_copy(k, n, way, cc, c).wait_send()
            sib_copy(k, n).wait_send()

    def relay(k, n, dist, bwd=False):
        @guard(exists(n))
        def _():
            if dist == MAXD:
                last_hop(k, n).wait_recv()
                return
            for way in WAYS:
                if dist == 1:
                    for i in WAYS:
                        inj_copy(k, n, way, 0, i).wait_recv()
                else:
                    hop_copy(k, n, way, dist).wait_recv()
                if dist < MAXD - 1:
                    wait_credits([ag_cred.at[way, dist]], k, slot(way, dist + 1), n, bwd)
                    hop_copy(k, n, way, dist + 1).start()
            if dist == MAXD - 1:
                wait_credits([ag_cred.at[par(n), dist]], k, MAXD, n, bwd)
                last_hop(k, n).start()

    def own_chip(k, n):
        @guard(exists(n))
        def _():
            xbuf[par(n + k[0]), part_of_block(0, c)] = own[c, n // per_row, unit_rows(n)]
            sib_copy(k, n).wait_recv()

    def give_credit(s, way, amount=1):
        dist = dist_of(s)
        if dist == 0:
            pl.semaphore_signal(sib_cred, inc=amount, device_id=sib, device_id_type=MESH)
        elif dist == 1:
            for i in WAYS:
                pl.semaphore_signal(inj_cred.at[way, c], inc=amount, device_id=dev(behind[way], i), device_id_type=MESH)
        elif dist < MAXD:
            pl.semaphore_signal(ag_cred.at[way, dist - 1], inc=amount, device_id=dev(behind[way], c), device_id_type=MESH)
        else:
            pl.semaphore_signal(ag_cred.at[way, dist - 1], inc=amount, device_id=dev(choose(way, left, right), c),
                                device_id_type=MESH)

    def way_of(s):
        return 0 if s < MAXD else 1

    def release(k, j, slots):
        for s in slots:
            n, dist = j - k[s], dist_of(s)
            if 1 <= dist < MAXD - 1 or s == MAXD - 1:
                @guard(exists(n))
                def _():
                    (last_hop(k, n) if s == MAXD - 1 else hop_copy(k, n, way_of(s), dist + 1)).wait_send()
        for s in slots:
            n = j - k[s] + 2

            @guard(exists(n))
            def _():
                give_credit(s, par(n) if s == MAXD else way_of(s))

    near, far = ORDER[:nz // PAIR], ORDER[nz // PAIR:]
    for k in (KF, KB):
        assert k[0] == k[1] == k[nz - 1] and k[MAXD - 1] == k[MAXD + 1] and {MAXD - 1, MAXD, MAXD + 1} <= set(far)

    inject(KF, ZERO)

    @pl.loop(0, rep.shape[0])
    def _(i):
        rep[i] = jnp.zeros(rep.shape[1:], F32)

    @pl.loop(0, PAD)
    def _(i):
        maskx[i] = jnp.zeros(maskx.shape[1:], F32)
        maskx[PAD + n_unit + i] = jnp.zeros(maskx.shape[1:], F32)
    gbacc[...] = jnp.zeros_like(gbacc)

    @pl.loop(0, hid // BIG)
    def _(i):
        gw[pl.ds(pl.multiple_of(i * BIG, BIG), BIG), :] = jnp.zeros((BIG, v_chip), F32)

    for cp in send_m:
        cp.wait()

    in_row = LANE // UT
    for s in range(nz):
        for i in WAYS:
            for r in range(n_unit // in_row):
                tile = jnp.broadcast_to(msgs[PAIR * chip_of(s) + i, c, r:r + 1, :], (LANE, LANE)).T
                for t in range(in_row):
                    at = pos[s] * br + i * UT
                    maskx[PAD + r * in_row + t, at:at + UT, :] = tile[t * UT:(t + 1) * UT, :]

    relay(KF, ZERO, 1)
    injected(KF, ZERO)
    load_w.wait()
    load_b.wait()
    send_w.wait()
    send_b.wait()

    def pages(j, k):
        after = {d: (j - d + PAD) // per_row for d in set(k)}
        return [after[k[s]] for s in range(nz)]

    def mask_rows(j, k, slots):
        return jnp.concatenate([maskx[j - k[s] + PAD, block(s), :] for s in slots], axis=0)

    def fwd_group(j, b, g, k0, k1):
        slots = (near, far)[g]
        page = pages(j, KF)

        @functools.partial(lax.fori_loop, k0, k1, init_val=None, unroll=UNROLL)
        def _(k, _):
            at = pl.ds(pl.multiple_of(k * CH, CH), CH)
            logits = jnp.dot(xbuf[b, g * half:(g + 1) * half], wbuf[:, at], preferred_element_type=F32)
            for t in range(CH // LANE):
                at = pl.ds(pl.multiple_of(k * CH + t * LANE, LANE), LANE)
                zt = logits[:, t * LANE:(t + 1) * LANE] + bias[:, at]
                act = jnp.log(1.0 + jnp.maximum(zt, 0.0)) * mask_rows(j, KF, slots)
                for i, s in enumerate(slots):
                    for u in WAYS:
                        r0 = i * br + u * UT
                        row_sum = jnp.sum(act[r0:r0 + UT, :], axis=0, keepdims=True)
                        rep[page[s], PAIR * s + u:PAIR * s + u + 1, at] = rep[page[s], PAIR * s + u:PAIR * s + u + 1, at] + row_sum

    def cut(eighths):
        return n_chunk * eighths // SUB

    fwd_end = n_unit + KF[MAXD]

    def release_far(j):
        @pl.when(j >= 1)
        def _():
            release(KF, j, far)

    @pl.loop(1, fwd_end)
    def _(j):
        b = par(j)
        release_far(j - 1)
        inject(KF, j)
        own_chip(KF, j - KF[0])
        near_left = j < n_unit + max(KF[s] for s in near)

        @pl.when(near_left)
        def _():
            fwd_group(j, b, 0, 0, cut(6))
        relay(KF, j - 2, 3)

        @pl.when(near_left)
        def _():
            fwd_group(j, b, 0, cut(6), n_chunk)
        release(KF, j, near)
        relay(KF, j - 1, 2)
        relay(KF, j - 3, 4)
        fwd_group(j, b, 1, 0, cut(4))
        relay(KF, j, 1)
        fwd_group(j, b, 1, cut(4), n_chunk)
        injected(KF, j)

    release_far(jnp.int32(fwd_end - 1))

    for s in range(nz):
        if s == MAXD:
            for way in WAYS:
                give_credit(s, way)
        else:
            give_credit(s, way_of(s), 2)

    q_total = q_rows * n_group
    d_total = d_rows * n_group
    v_total = v_loc * n_group
    tau = q_len * math.sqrt(v_total * d_len) / 16.0
    lam_q = 4.0 / (v_total * q_len * q_len)
    lam_d = 4.0 / (v_total * d_len * d_len)
    nd = d_rows // PAIR * n_group
    nq = q_rows // PAIR * n_group
    q0 = PAD // per_row
    d0 = q0 + n_qpage

    @pl.loop(0, v_chip // CB)
    def _(k):
        at = pl.ds(pl.multiple_of(k * CB, CB), CB)
        for r in range(d_rows // PAIR):
            rdx[c, r * n_group:(r + 1) * n_group, at] = sum(rep[d0 + r * pieces + i, :, at] for i in range(pieces))
        q_sum = sum(rep[q0 + i, :, at] for i in range(n_qpage))
        rdx[c, nd:nd + SUB, at] = sum(q_sum[i * SUB:(i + 1) * SUB] for i in range(n_group // SUB))

    def to_sib(src, dst, i):
        return remote(src, dst, pair_sem.at[i, 0], pair_sem.at[i, 1], sib)

    send_rd = to_sib(rdx.at[c], rdx.at[c], 0)
    send_rd.start()
    inject(KB, ZERO, BWD)
    send_rd.wait()

    def d_reps(at):
        return jnp.concatenate([rdx[0, 0:nd, at], rdx[1, 0:nd, at]], axis=0)

    def q_mean_of(at):
        return jnp.sum(rdx[0, nd:nd + SUB, at] + rdx[1, nd:nd + SUB, at], axis=0, keepdims=True) * (1.0 / q_total)

    def d_mean_of(at):
        return jnp.sum(d_reps(at), axis=0, keepdims=True) * (1.0 / d_total)

    def lanes(v):
        return sum(v[:, t * LANE:(t + 1) * LANE] for t in range(CB // LANE))

    def score_chunk(k, carry):
        s_acc, rq, rd = carry
        at = pl.ds(pl.multiple_of(k * CB, CB), CB)
        q_rep = rep[q0:q0 + n_qpage, :, at].reshape(nq, CB)
        s_acc = s_acc + lax.dot_general(d_reps(at), q_rep, (((1,), (1,)), ((), ())), precision=HIGHEST,
                                        preferred_element_type=F32)
        qm, dm = q_mean_of(at), d_mean_of(at)
        return s_acc, rq + lanes(qm * qm), rd + lanes(dm * dm)

    score, reg_q, reg_d = lax.fori_loop(0, v_chip // CB, score_chunk,
                                        (jnp.zeros((PAIR * nd, nq), F32), jnp.zeros((1, LANE), F32), jnp.zeros((1, LANE), F32)))

    def turn(n):
        i = lax.broadcasted_iota(jnp.int32, (n, n), 0)
        k = lax.broadcasted_iota(jnp.int32, (n, n), 1)
        same = (i // n_group == k // n_group) & (i % 2 == k % 2)
        return (same & (((i // PAIR) % nz + (k // PAIR) % nz) % nz == z)).astype(F32)

    def exact(a, b):
        return jnp.dot(a, b, precision=HIGHEST, preferred_element_type=F32)

    turn_d, turn_q = turn(PAIR * nd), turn(nq)
    smsg[0, 0:PAIR * nd, 0:nq] = exact(exact(turn_d, score), turn_q)
    smsg[0, PAIR * nd:PAIR * nd + 1, :] = reg_q
    smsg[0, PAIR * nd + 1:PAIR * nd + 2, :] = reg_d
    send_s = [remote(smsg.at[0], smsg.at[t], sm_send.at[t], sm_recv.at[t], peers[t - 1]) for t in range(1, nz)]
    for cp in send_s:
        cp.start()

    def turn_head(first):
        @pl.loop(0, v_chip // LANE // PAIR)
        def _(k):
            at = pl.ds(pl.multiple_of((first * (v_chip // LANE // PAIR) + k) * LANE, LANE), LANE)
            wt[at, :] = wbuf[:, at].T

    pos_rows = jnp.concatenate([msgs[i, 0, 3:4, :] for i in range(n_group)], axis=0)
    spread = (lax.broadcasted_iota(jnp.int32, (LANE, nq), 0)
              == PAIR * (lax.broadcasted_iota(jnp.int32, (LANE, nq), 1) // n_group) + c).astype(F32)
    pos_all = exact(pos_rows, spread)
    pick = (lax.broadcasted_iota(jnp.int32, (n_group, nq), 1) % n_group
            == lax.broadcasted_iota(jnp.int32, (n_group, nq), 0))
    pos_row = jnp.sum(jnp.where(pick, pos_all, 0.0), axis=0, keepdims=True)
    ridx = lax.broadcasted_iota(jnp.int32, (PAIR * nd, nq), 0)
    doc = (ridx % n_group) * d_rows + PAIR * ((ridx % nd) // n_group) + ridx // nd
    target = (doc.astype(F32) == pos_row).astype(F32)

    turn_head(0)
    relay(KB, ZERO, 1, BWD)
    injected(KB, ZERO)
    turn_head(1)
    for cp in send_s:
        cp.wait()
    total = smsg[0]
    for t in range(1, nz):
        total = total + smsg[t]
    scores = total[0:PAIR * nd, 0:nq] * (1.0 / tau)
    top = jnp.max(scores, axis=0, keepdims=True)
    log_norm = top + jnp.log(jnp.sum(jnp.exp(scores - top), axis=0, keepdims=True))
    row_loss = log_norm - jnp.sum(scores * target, axis=0, keepdims=True)
    loss_part = jnp.sum(row_loss, axis=1, keepdims=True)
    gt = (jnp.exp(scores - log_norm) - target) * (1.0 / (q_total * tau))
    gt = exact(exact(turn_d, gt), turn_q)
    g = gt.T
    lossx[c] = jnp.broadcast_to(loss_part, (SUB, LANE))
    send_l = to_sib(lossx.at[c], lossx.at[c], 1)
    send_l.start()
    inject(KB, ZERO + 1, BWD)
    relay(KB, ZERO, 2, BWD)

    @pl.loop(0, v_chip // CB)
    def _(k):
        at = pl.ds(pl.multiple_of(k * CB, CB), CB)
        q_rep = rep[q0:q0 + n_qpage, :, at].reshape(nq, CB)
        dp = exact(gt, q_rep)
        ddx[0, :, at] = dp[0:nd]
        ddx[1, :, at] = dp[nd:PAIR * nd]

    send_dd = to_sib(ddx.at[o], ddr, 2)
    send_dd.start()

    @pl.loop(0, v_chip // CB)
    def _(k):
        at = pl.ds(pl.multiple_of(k * CB, CB), CB)
        gq = exact(g, d_reps(at)) + q_mean_of(at) * (2.0 * lam_q / q_total)
        rep[q0:q0 + n_qpage, :, at] = gq.reshape(n_qpage, n_group, CB)

    send_l.wait()
    reg = (jnp.sum(total[PAIR * nd:PAIR * nd + 1, :], axis=1, keepdims=True) * lam_q
           + jnp.sum(total[PAIR * nd + 1:PAIR * nd + 2, :], axis=1, keepdims=True) * lam_d)
    lossf[0] = (lossx[0] + lossx[1]) * (1.0 / q_total) + reg

    send_loss = [remote(lossf.at[0], lossf.at[1], loss_send.at[t], loss_recv, peers[t - 1]) for t in range(1, nz)]

    @pl.when(z == 0)
    def _():
        for cp in send_loss:
            cp.start()
    relay(KB, ZERO + 1, 1, BWD)
    injected(KB, ZERO + 1)
    relay(KB, ZERO, 3, BWD)
    send_dd.wait()

    @pl.loop(0, v_chip // CB)
    def _(k):
        at = pl.ds(pl.multiple_of(k * CB, CB), CB)
        gd = ddx[c, :, at] + ddr[:, at] + d_mean_of(at) * (2.0 * lam_d / d_total)
        for r in range(d_rows // PAIR):
            for i in range(pieces):
                rep[d0 + r * pieces + i, :, at] = gd[r * n_group:(r + 1) * n_group]

    def bwd_chunk(j, b, page, k, slots=ORDER, weights=BWD):
        at0 = pos[slots[0]] * br
        some = slice(at0, at0 + len(slots) * br)
        cols = pl.ds(pl.multiple_of(k * CB, CB), CB)
        logits = jnp.dot(xbuf[b, some], wbuf[:, cols], preferred_element_type=F32)
        low = []
        for t in range(CB // LANE):
            at = pl.ds(pl.multiple_of(k * CB + t * LANE, LANE), LANE)
            zt = logits[:, t * LANE:(t + 1) * LANE] + bias[:, at]
            grad = jnp.concatenate([jnp.broadcast_to(rep[page[s], PAIR * s + u:PAIR * s + u + 1, at], (UT, LANE))
                                    for s in slots for u in WAYS], axis=0)
            gz = jnp.where(zt > 0.0, grad * mask_rows(j, KB, slots) / (1.0 + jnp.maximum(zt, 0.0)), 0.0)
            gbacc[:, at] = gbacc[:, at] + jnp.sum(gz.reshape(-1, SUB, LANE), axis=0)
            low.append(gz.astype(BF16))
        low = jnp.concatenate(low, axis=1)
        gbuf[some, cols] = low
        if weights:
            gw[:, cols] = gw[:, cols] + jnp.dot(xt[...], low, preferred_element_type=F32)

    def bwd_hidden(k0, k1, some=slice(None)):
        wide = hid // 4

        @functools.partial(lax.fori_loop, k0, k1, init_val=None, unroll=UNROLL)
        def _(k, _):
            cols = pl.ds(pl.multiple_of(k * wide, wide), wide)
            pbuf[some, cols] = jnp.dot(gbuf[some, :], wt[:, cols], preferred_element_type=F32).astype(BF16)

    def deep(n):
        return lax.rem(n + BIG, DEEP)

    def room(n):
        return lax.rem(n + BIG, ROOM)

    def rs_copy(n, way, dist):
        to = behind[way] if isinstance(way, int) else choose(way, left, right)
        return remote(sbuf.at[way, dist - 1], rbuf.at[way, dist - 2, room(n)], rs_send.at[way, dist - 1],
                      rs_recv.at[way, dist - 2, room(n)], dev(to, c))

    def home_copy(n, way, cc, i):
        return remote(sbuf.at[way, 0, pl.ds(i * UT, UT)], hbuf.at[way, cc, room(n)], h_send.at[way, i],
                      h_recv.at[way, cc, room(n)], dev(behind[way], i))

    def pair_copy(n):
        return remote(sst.at[par(n)], sibp.at[deep(n)], sp_send.at[par(n)], sp_recv.at[deep(n)], sib)

    def rs_sent(n, dist):
        @guard(exists(n))
        def _():
            if dist == MAXD:
                rs_copy(n, par(n), dist).wait_send()
                return
            for way in WAYS:
                if dist == 1:
                    for i in WAYS:
                        home_copy(n, way, c, i).wait_send()
                else:
                    rs_copy(n, way, dist).wait_send()

    def rs_both(n, dist):
        rs_sent(n - (2 if dist == MAXD else 1), dist)

        def joined(way, mine):
            rs_copy(n, way, dist + 1).wait_recv()
            sbuf[way, dist - 1] = (mine.astype(F32) + rbuf[way, dist - 1, room(n)].astype(F32)).astype(BF16)

        @guard(exists(n))
        def _():
            if dist == MAXD:
                sbuf[par(n), dist - 1] = pbuf[block(MAXD), :]
                rs_copy(n, par(n), dist).start()
            elif dist == MAXD - 1:
                way = par(n)
                sbuf[1 - way, dist - 1] = part[choose(way, nz - dist, dist), deep(n)]
                rs_copy(n, 1 - way, dist).start()
                joined(way, part[choose(way, dist, nz - dist), deep(n)])
                rs_copy(n, way, dist).start()
            else:
                for way in WAYS:
                    joined(way, part[slot(way, dist), deep(n)])
                    if dist == 1:
                        for i in WAYS:
                            home_copy(n, way, c, i).start()
                    else:
                        rs_copy(n, way, dist).start()

    def rs_home(n):
        @guard(exists(n))
        def _():
            for cc in WAYS:
                for way in WAYS:
                    home_copy(n, way, cc, 0).wait_recv()
                at = unit_rows(n)
                acc_h[cc, n // per_row, at] = (acc_h[cc, n // per_row, at].astype(F32) + hbuf[0, cc, room(n)].astype(F32)
                                               + hbuf[1, cc, room(n)].astype(F32)).astype(BF16)

    def pair_send(n):
        @guard(exists(n - 2))
        def _():
            pair_copy(n - 2).wait_send()

        @guard(exists(n))
        def _():
            sst[par(n)] = pbuf[part_of_block(0, o), :]
            pair_copy(n).start()
            acc_h[c, n // per_row, unit_rows(n)] = pbuf[part_of_block(0, c), :]

    def pair_take(n):
        @guard(exists(n))
        def _():
            pair_copy(n).wait_recv()
            acc_h[o, n // per_row, unit_rows(n)] = sibp[deep(n)]

    last = n_unit + KB[MAXD]
    assert all(n_unit + KB[s] < last for s in near)

    def part_b(eighths):
        return v_chip // CB * eighths // SUB

    def bwd_step(j):
        b = par(j)
        page = pages(j, KB)
        late = None if steady else j >= 2

        def weights(k0, k1):
            @functools.partial(lax.fori_loop, k0, k1, init_val=None, unroll=UNROLL)
            def _(k, _):
                bwd_chunk(j, b, page, k)

        relay(KB, j - 2, 4)
        own_chip(KB, j - 1)
        rs_both(j - 3, 4)
        rs_both(j - 5, 1)
        xt[...] = xbuf[b].T
        weights(0, part_b(4))

        @guard(late)
        def _():
            relay(KB, j, 1, BWD)
        rs_both(j - 4, 2)
        weights(part_b(4), part_b(6))

        @guard(late)
        def _():
            relay(KB, j - 1, 3, BWD)
        weights(part_b(6), v_chip // CB)
        release(KB, j, ORDER)
        rs_both(j - 3, 3)
        bwd_hidden(0, 3)

        @guard(late)
        def _():
            injected(KB, j)
        inject(KB, j + 1, BWD)
        relay(KB, j, 2, BWD)
        rs_home(j - 5)
        bwd_hidden(3, 4)
        for s in range(1, nz):
            if s != MAXD:
                part[s, deep(j - KB[s])] = pbuf[block(s), :]
        pair_send(j - 1)
        pair_take(j - 2)

    @pl.loop(1, last - 1)
    def _(j):
        middle = (j >= 6) & (j < n_unit - 1)

        @pl.when(middle)
        def _():
            steady.append(BWD)
            bwd_step(j)
            steady.pop()

        @pl.when(jnp.logical_not(middle))
        def _():
            bwd_step(j)

    j = ZERO + last - 1
    b = par(j)
    page = pages(j, KB)
    some = slice(half, rows)
    relay(KB, j - 2, 4)
    rs_both(j - 3, 4)
    rs_both(j - 5, 1)

    @functools.partial(lax.fori_loop, 0, v_chip // CB, init_val=None, unroll=UNROLL)
    def _(k, _):
        bwd_chunk(j, b, page, k, far, False)
    rs_both(j - 4, 2)
    bwd_hidden(0, 4, some)
    for s in far:
        if s != MAXD:
            part[s, deep(j - KB[s])] = pbuf[block(s), :]
    rs_both(j + 1 - 3, 4)
    rs_both(j - 3, 3)
    release(KB, j, ORDER)
    pair_send(j - 1)
    pair_take(j - 2)
    rs_home(j - 5)
    xt[:, some] = xbuf[b, some].T

    @functools.partial(lax.fori_loop, 0, v_chip // CB, init_val=None, unroll=UNROLL)
    def _(k, _):
        cols = pl.ds(pl.multiple_of(k * CB, CB), CB)
        gw[:, cols] = gw[:, cols] + jnp.dot(xt[:, some], gbuf[some, cols], preferred_element_type=F32)

    n_part = gx_send.shape[0] - 1
    step = v_loc // n_part
    send_g = []
    for k in range(n_part):
        theirs = pl.ds(pl.multiple_of(o * v_loc + k * step, step), step)
        send_g.append(remote(gw.at[:, theirs], grecv.at[k % PAIR], gx_send.at[k], gx_recv.at[k], sib))
    send_gb = remote(gbacc.at[:, sib_cols], gbrecv, gx_send.at[n_part], gx_recv.at[n_part], sib)
    for cp in send_g[:PAIR]:
        cp.start()
    send_gb.start()

    w_outs = []

    def add_part():
        k = len(w_outs)
        send_g[k].wait_recv()
        at = pl.ds(pl.multiple_of(c * v_loc + k * step, step), step)

        @pl.loop(0, hid // BIG)
        def _(i):
            rr = pl.ds(pl.multiple_of(i * BIG, BIG), BIG)
            wbuf[rr, at] = (gw[rr, at] + grecv[k % PAIR, rr]).astype(BF16)
        w_outs.append(pltpu.make_async_copy(wbuf.at[:, at], gw_out.at[:, pl.ds(k * step, step)], out_sem.at[n_load + k]))
        w_outs[-1].start()
        if k + PAIR < n_part:
            pl.semaphore_signal(gx_cred, device_id=sib, device_id_type=MESH)
            pl.semaphore_wait(gx_cred)
            send_g[k + PAIR].start()

    n_load = len(loads)
    for j in range(last, n_unit + 5):
        n = ZERO + j
        if j > last:
            rs_both(n - 3, 4)
        if j == n_unit + 4:
            add_part()
        rs_both(n - 5, 1)
        rs_both(n - 4, 2)
        rs_both(n - 3, 3)
        pair_send(n - 1)
        add_part()
        rs_home(n - 5)
    rs_sent(jnp.int32(n_unit - 1), 1)

    outs = []
    for cc in WAYS:
        outs.append(pltpu.make_async_copy(acc_h.at[cc, pl.ds(0, n_qpage)], dq_out.at[:, cc], out_sem.at[len(outs)]))
        for r in range(d_rows // PAIR):
            outs.append(pltpu.make_async_copy(acc_h.at[cc, pl.ds(n_qpage + r * pieces, pieces)], dd_out.at[r, cc],
                                              out_sem.at[len(outs)]))
    for cp in outs:
        cp.start()
    while len(w_outs) < n_part:
        add_part()
    send_gb.wait_recv()
    gb_ref[...] = jnp.sum(gbacc[:, my_cols] + gbrecv[...], axis=0, keepdims=True)

    @pl.when(z == 0)
    def _():
        for cp in send_loss:
            cp.wait_send()
        loss_ref[...] = lossf[0, 0:1, 0:1]

    @pl.when(z != 0)
    def _():
        send_loss[0].wait_recv()
        loss_ref[...] = lossf[1, 0:1, 0:1]
    for cp in send_g:
        cp.wait_send()
    send_gb.wait_send()
    for cp in outs + w_outs:
        cp.wait()


def settle(*refs):
    n = len(refs) // 4
    copies = []
    for a, z, buf, sem in zip(*(refs[k * n:(k + 1) * n] for k in range(4))):
        pieces = sem.shape[1]
        size = a.shape[0] // pieces
        for p in range(pieces):
            at = pl.ds(p * size, size)
            copies.append((pltpu.make_async_copy(a.at[at], buf.at[at], sem.at[0, p]),
                           pltpu.make_async_copy(buf.at[at], z.at[at], sem.at[1, p])))
    for cp, _ in copies:
        cp.start()
    for cp, back in copies:
        cp.wait()
        back.start()
    for _, back in copies:
        back.wait()


def solution(mesh):
    n_group = mesh.shape['tp']
    nz = n_group // PAIR
    row_spec = P(('dp', 'tp'))
    mask_spec = P(('dp', 'tp'), None)
    hid_spec = P(('dp', 'tp'), None, None)

    def local_step(q_hidden, d_hidden, q_mask, d_mask, positive, w_head, b_head):
        q_rows, q_len, hid = q_hidden.shape
        d_rows, d_len, _ = d_hidden.shape
        v_loc = w_head.shape[1]
        v_chip = PAIR * v_loc
        per_row = q_len // UT
        pieces = d_len // q_len
        n_page = q_rows // PAIR + d_rows // PAIR * pieces
        n_unit = n_page * per_row
        rows = nz * PAIR * UT
        nd, nq = d_rows // PAIR * n_group, q_rows // PAIR * n_group
        s_rows = -(-(PAIR * nd + 2) // SUB) * SUB
        n_part = 4 if v_loc >= 512 else 2
        n_load = PAIR * (1 + d_rows // PAIR)
        dma, reg = pltpu.SemaphoreType.DMA, pltpu.SemaphoreType.REGULAR
        anym = pl.BlockSpec(memory_space=pl.ANY)
        vm = pl.BlockSpec(memory_space=pltpu.VMEM)
        q_shape = (q_rows // PAIR, 2, q_len, hid)
        d_shape = (d_rows // PAIR, 2, pieces, q_len, hid)
        out_shape = (
            jax.ShapeDtypeStruct((1, 1), F32),
            jax.ShapeDtypeStruct((hid, v_loc), BF16),
            jax.ShapeDtypeStruct((1, v_loc), F32),
            jax.ShapeDtypeStruct(q_shape, BF16),
            jax.ShapeDtypeStruct(d_shape, BF16),
        )
        scratch = [
            pltpu.VMEM((hid, v_chip), BF16),
            pltpu.VMEM((v_chip, hid), BF16),
            pltpu.VMEM((hid, v_chip), F32),
            pltpu.VMEM((PAIR, hid, v_loc // n_part), F32),
            pltpu.VMEM(((n_unit + PAIR * PAD) // per_row, n_group, v_chip), F32),
            pltpu.VMEM((n_unit + PAIR * PAD, rows, LANE), F32),
            pltpu.VMEM((PAIR, n_page, q_len, hid), BF16),
            pltpu.VMEM((PAIR, n_page, q_len, hid), BF16),
            pltpu.VMEM((nz, DEEP, PAIR * UT, hid), BF16),
            pltpu.VMEM((PAIR, rows, hid), BF16),
            pltpu.VMEM((PAIR, MAXD - 1, ROOM, PAIR * UT, hid), BF16),
            pltpu.VMEM((PAIR, MAXD, PAIR * UT, hid), BF16),
            pltpu.VMEM((PAIR, 2, ROOM, UT, hid), BF16),
            pltpu.VMEM((DEEP, UT, hid), BF16),
            pltpu.VMEM((PAIR, UT, hid), BF16),
            pltpu.VMEM((rows, v_chip), BF16),
            pltpu.VMEM((rows, hid), BF16),
            pltpu.VMEM((hid, rows), BF16),
            pltpu.VMEM((PAIR, nd + SUB, v_chip), F32),
            pltpu.VMEM((PAIR, nd, v_chip), F32),
            pltpu.VMEM((nd, v_chip), F32),
            pltpu.VMEM((1, v_chip), F32),
            pltpu.VMEM((SUB, v_chip), F32),
            pltpu.VMEM((SUB, v_loc), F32),
            pltpu.VMEM((n_group, 2, 4, LANE), F32),
            pltpu.VMEM((nz, s_rows, LANE), F32),
            pltpu.VMEM((PAIR, SUB, LANE), F32),
            pltpu.VMEM((PAIR, SUB, LANE), F32),
            dma((PAIR, MAXD, 2)), dma((PAIR, nz, 2)), reg((PAIR, MAXD)), dma((PAIR, 2)), reg((PAIR, 2)), dma, reg,
            dma((PAIR, MAXD)), dma((PAIR, MAXD - 1, ROOM)), dma((PAIR, 2)), dma((PAIR, 2, ROOM)),
            dma((PAIR,)), dma((DEEP,)),
            dma((n_load + PAIR,)), dma((PAIR,)), dma((PAIR,)), dma((n_group - 1,)), dma((n_group - 1,)), dma((nz,)), dma((nz,)),
            dma((3, 2)), dma((n_part + 1,)), dma((n_part + 1,)), reg, dma((nz,)), dma, dma((n_load + n_part,)),
        ]
        loss, gw, gb, dq, dd = pl.pallas_call(
            functools.partial(kernel, n_group, q_rows, q_len, d_rows, d_len),
            out_shape=out_shape,
            in_specs=[anym] * 4 + [vm] * 3,
            out_specs=(vm, anym, vm, anym, anym),
            scratch_shapes=scratch,
            compiler_params=pltpu.CompilerParams(collective_id=0, has_side_effects=True, vmem_limit_bytes=67043328),
        )(q_hidden.reshape(q_shape), d_hidden.reshape(d_shape), w_head, b_head.reshape(1, v_loc),
          q_mask, d_mask, positive.reshape(1, q_rows))
        results = (gw, dq, dd, gb, loss)
        gw, dq, dd, gb, loss = pl.pallas_call(
            settle,
            out_shape=[jax.ShapeDtypeStruct(a.shape, a.dtype) for a in results],
            in_specs=[anym] * len(results),
            out_specs=[anym] * len(results),
            scratch_shapes=[pltpu.VMEM(a.shape, a.dtype) for a in results] + [dma((2, math.gcd(4, a.shape[0]))) for a in results],
            compiler_params=pltpu.CompilerParams(vmem_limit_bytes=67043328),
        )(*results)
        return (loss.reshape(1), gw, gb.reshape(v_loc), dq.reshape(q_hidden.shape), dd.reshape(d_hidden.shape))

    return jax.shard_map(local_step, mesh=mesh,
                         in_specs=(hid_spec, hid_spec, mask_spec, mask_spec, row_spec, P(None, 'tp'), P('tp')),
                         out_specs=(P('dp'), P('dp', 'tp'), row_spec, hid_spec, hid_spec),
                         check_vma=False)
```

```python
import functools
import math
import jax
import jax.numpy as jnp
from jax import lax
from jax.experimental import pallas as pl
from jax.experimental.pallas import tpu as pltpu
from jax.sharding import PartitionSpec as P

MESH = pl.DeviceIdType.MESH
HIGHEST = lax.Precision.HIGHEST
F32 = jnp.float32
BF16 = jnp.bfloat16
BWD = UNROLL = True

UT = 16
CH = 512
CB = 1024
MAXD = 4
KF = (1, 1, 2, 2, 3, 2, 1, 1)
KB = (1, 1, 1, 2, 2, 2, 1, 1)
LANE, SUB, PAIR, BIG = 128, 8, 2, 64
DEEP = 4
ROOM = 8
WAYS = (0, 1)
ORDER = (0, 1, 7, 2, 6, 3, 5, 4)
PAD = 4


def kernel(n_group, q_rows, q_len, d_rows, d_len,
           q_ref, d_ref, w_ref, b_ref, qm_ref, dm_ref, pos_ref,
           loss_ref, gw_out, gb_ref, dq_out, dd_out,
           wbuf, wt, gw, grecv, rep, maskx, own, acc_h, part, xbuf, rbuf, sbuf, hbuf, sibp, sst, gbuf, pbuf, xt,
           rdx, ddx, ddr, bias, gbacc, gbrecv, msgs, smsg, lossx, lossf,
           ag_send, ag_recv, ag_cred, inj_send, inj_cred, sib_send, sib_cred,
           rs_send, rs_recv, h_send, h_recv, sp_send, sp_recv,
           loc_sem, w_sem, bias_sem, msg_send, msg_recv, sm_send, sm_recv, pair_sem, gx_send, gx_recv, gx_cred,
           loss_send, loss_recv, out_sem):
    ZERO = jnp.int32(0)
    nz = n_group // PAIR
    hid = w_ref.shape[0]
    v_loc = w_ref.shape[1]
    v_chip = PAIR * v_loc
    per_row = q_len // UT
    pieces = d_len // q_len
    n_qpage = q_rows // PAIR
    n_dpage = d_rows // PAIR * pieces
    n_page = n_qpage + n_dpage
    n_unit = n_page * per_row
    br = PAIR * UT
    rows = nz * br
    half = rows // PAIR
    n_chunk = v_chip // CH
    pos = {s: i for i, s in enumerate(ORDER)}

    me = lax.axis_index('tp')
    z = me // PAIR
    c = lax.rem(me, 2)
    o = 1 - c
    right = lax.rem(z + 1, nz)
    left = lax.rem(z + nz - 1, nz)

    def dev(zz, cc):
        return {'tp': PAIR * zz + cc}

    sib = dev(z, o)
    ahead = (right, left)
    behind = (left, right)

    def slot(way, dist):
        return dist if way == 0 else nz - dist

    def dist_of(s):
        return min(s, nz - s)

    def chip_of(s):
        return lax.rem(z - s + nz, nz)

    def block(s):
        return pl.ds(pos[s] * br, br)

    def part_of_block(s, i):
        return pl.ds(pl.multiple_of(pos[s] * br + i * UT, UT), UT)

    def par(n):
        return lax.rem(n + BIG, 2)

    def unit_rows(n):
        return pl.ds(pl.multiple_of(lax.rem(n, per_row) * UT, UT), UT)

    peers = [dev(lax.rem(z + t, nz), c) for t in range(1, nz)]
    others = [dev(lax.rem(z + t, nz), lax.rem(c + u, 2)) for t in range(nz) for u in WAYS if t or u]

    loads = []
    for cc in WAYS:
        loads.append(pltpu.make_async_copy(q_ref.at[:, cc], own.at[cc, pl.ds(0, n_qpage)], loc_sem.at[len(loads)]))
        for r in range(d_rows // PAIR):
            loads.append(pltpu.make_async_copy(d_ref.at[r, cc], own.at[cc, pl.ds(n_qpage + r * pieces, pieces)],
                                               loc_sem.at[len(loads)]))
    my_cols = pl.ds(pl.multiple_of(c * v_loc, v_loc), v_loc)
    sib_cols = pl.ds(pl.multiple_of(o * v_loc, v_loc), v_loc)
    load_w = pltpu.make_async_copy(w_ref, wbuf.at[:, my_cols], loc_sem.at[len(loads)])
    load_b = pltpu.make_async_copy(b_ref, bias.at[:, my_cols], loc_sem.at[len(loads) + 1])
    for cp in loads + [load_w, load_b]:
        cp.start()
    xbuf[...] = jnp.zeros_like(xbuf)

    where = jnp.concatenate([pos_ref[...], jnp.zeros((1, LANE - q_rows), jnp.int32)], axis=1)
    for cc in WAYS:
        tokens = jnp.concatenate([qm_ref[r:r + 1, :] for r in range(cc, q_rows, PAIR)]
                                 + [dm_ref[r:r + 1, :] for r in range(cc, d_rows, PAIR)], axis=1)
        for r in range(tokens.shape[1] // LANE):
            msgs[me, cc, r:r + 1, :] = tokens[:, r * LANE:(r + 1) * LANE].astype(F32)
        msgs[me, cc, 3:4, :] = where.astype(F32)

    barrier = pltpu.get_barrier_semaphore()
    for d in others:
        pl.semaphore_signal(barrier, device_id=d, device_id_type=MESH)
    pl.semaphore_wait(barrier, n_group - 1)

    def remote(src, dst, ss, rs, to):
        return pltpu.make_async_remote_copy(src, dst, ss, rs, device_id=to, device_id_type=MESH)

    send_m = [remote(msgs.at[me], msgs.at[me], msg_send.at[k], msg_recv.at[k], d) for k, d in enumerate(others)]
    for cp in send_m:
        cp.start()
    send_w = remote(w_ref, wbuf.at[:, my_cols], w_sem.at[0], w_sem.at[1], sib)
    send_w.start()
    send_b = remote(b_ref, bias.at[:, my_cols], bias_sem.at[0], bias_sem.at[1], sib)
    send_b.start()
    for cp in loads:
        cp.wait()

    steady = []

    def guard(cond):
        return (lambda f: f()) if cond is None else pl.when(cond)

    def exists(n):
        return None if steady else (n >= 0) & (n < n_unit)

    def choose(way, a, b):
        return jnp.where(way == 0, a, b)

    def wait_credits(sems, k, s, n, bwd):
        if steady:
            for sem in sems:
                pl.semaphore_wait(sem)
            return
        counts = [(n >= 3 - k[s], 1)]
        if bwd:
            counts.append((n < 2, 1) if s == MAXD else (n == 0, 2))
        for cond, amount in counts:
            @pl.when(cond)
            def _():
                for sem in sems:
                    pl.semaphore_wait(sem, amount)

    def hop_copy(k, n, way, dist):
        s, s0 = slot(way, dist), slot(way, dist - 1)
        return remote(xbuf.at[par(n + k[s0]), block(s0)], xbuf.at[par(n + k[s]), block(s)],
                      ag_send.at[way, dist - 1, par(n)], ag_recv.at[par(n + k[s]), s, 0], dev(ahead[way], c))

    def last_hop(k, n):
        way, s0 = par(n), MAXD - 1
        here = pl.ds(pl.multiple_of(choose(way, pos[s0] * br, pos[nz - s0] * br), br), br)
        return remote(xbuf.at[par(n + k[s0]), here], xbuf.at[par(n + k[MAXD]), block(MAXD)],
                      ag_send.at[way, s0, par(n)], ag_recv.at[par(n + k[MAXD]), MAXD, 0], dev(choose(way, right, left), c))

    def inj_copy(k, n, way, cc, i):
        s = slot(way, 1)
        return remote(own.at[cc, n // per_row, unit_rows(n)], xbuf.at[par(n + k[s]), part_of_block(s, i)],
                      inj_send.at[way, cc], ag_recv.at[par(n + k[s]), s, i], dev(ahead[way], cc))

    def sib_copy(k, n):
        return remote(own.at[o, n // per_row, unit_rows(n)], xbuf.at[par(n + k[0]), part_of_block(0, c)],
                      sib_send, ag_recv.at[par(n + k[0]), 0, 0], sib)

    def inject(k, n, bwd=False):
        @guard(exists(n))
        def _():
            both = [(way, cc) for cc in WAYS for way in WAYS]
            wait_credits([inj_cred.at[way, cc] for way, cc in both] + [sib_cred], k, 0, n, bwd)
            for way, cc in both:
                inj_copy(k, n, way, cc, c).start()
            sib_copy(k, n).start()

    def injected(k, n):
        @guard(exists(n))
        def _():
            for cc in WAYS:
                for way in WAYS:
                    inj_copy(k, n, way, cc, c).wait_send()
            sib_copy(k, n).wait_send()

    def relay(k, n, dist, bwd=False):
        @guard(exists(n))
        def _():
            if dist == MAXD:
                last_hop(k, n).wait_recv()
                return
            for way in WAYS:
                if dist == 1:
                    for i in WAYS:
                        inj_copy(k, n, way, 0, i).wait_recv()
                else:
                    hop_copy(k, n, way, dist).wait_recv()
                if dist < MAXD - 1:
                    wait_credits([ag_cred.at[way, dist]], k, slot(way, dist + 1), n, bwd)
                    hop_copy(k, n, way, dist + 1).start()
            if dist == MAXD - 1:
                wait_credits([ag_cred.at[par(n), dist]], k, MAXD, n, bwd)
                last_hop(k, n).start()

    def own_chip(k, n):
        @guard(exists(n))
        def _():
            xbuf[par(n + k[0]), part_of_block(0, c)] = own[c, n // per_row, unit_rows(n)]
            sib_copy(k, n).wait_recv()

    def give_credit(s, way, amount=1):
        dist = dist_of(s)
        if dist == 0:
            pl.semaphore_signal(sib_cred, inc=amount, device_id=sib, device_id_type=MESH)
        elif dist == 1:
            for i in WAYS:
                pl.semaphore_signal(inj_cred.at[way, c], inc=amount, device_id=dev(behind[way], i), device_id_type=MESH)
        elif dist < MAXD:
            pl.semaphore_signal(ag_cred.at[way, dist - 1], inc=amount, device_id=dev(behind[way], c), device_id_type=MESH)
        else:
            pl.semaphore_signal(ag_cred.at[way, dist - 1], inc=amount, device_id=dev(choose(way, left, right), c),
                                device_id_type=MESH)

    def way_of(s):
        return 0 if s < MAXD else 1

    def release(k, j, slots):
        for s in slots:
            n, dist = j - k[s], dist_of(s)
            if 1 <= dist < MAXD - 1 or s == MAXD - 1:
                @guard(exists(n))
                def _():
                    (last_hop(k, n) if s == MAXD - 1 else hop_copy(k, n, way_of(s), dist + 1)).wait_send()
        for s in slots:
            n = j - k[s] + 2

            @guard(exists(n))
            def _():
                give_credit(s, par(n) if s == MAXD else way_of(s))

    near, far = ORDER[:nz // PAIR], ORDER[nz // PAIR:]
    for k in (KF, KB):
        assert k[0] == k[1] == k[nz - 1] and k[MAXD - 1] == k[MAXD + 1] and {MAXD - 1, MAXD, MAXD + 1} <= set(far)

    inject(KF, ZERO)

    @pl.loop(0, rep.shape[0])
    def _(i):
        rep[i] = jnp.zeros(rep.shape[1:], F32)

    @pl.loop(0, PAD)
    def _(i):
        maskx[i] = jnp.zeros(maskx.shape[1:], F32)
        maskx[PAD + n_unit + i] = jnp.zeros(maskx.shape[1:], F32)
    gbacc[...] = jnp.zeros_like(gbacc)

    @pl.loop(0, hid // BIG)
    def _(i):
        gw[pl.ds(pl.multiple_of(i * BIG, BIG), BIG), :] = jnp.zeros((BIG, v_chip), F32)

    for cp in send_m:
        cp.wait()

    in_row = LANE // UT
    for s in range(nz):
        for i in WAYS:
            for r in range(n_unit // in_row):
                tile = jnp.broadcast_to(msgs[PAIR * chip_of(s) + i, c, r:r + 1, :], (LANE, LANE)).T
                for t in range(in_row):
                    at = pos[s] * br + i * UT
                    maskx[PAD + r * in_row + t, at:at + UT, :] = tile[t * UT:(t + 1) * UT, :]

    relay(KF, ZERO, 1)
    injected(KF, ZERO)
    load_w.wait()
    load_b.wait()
    send_w.wait()
    send_b.wait()

    def pages(j, k):
        after = {d: (j - d + PAD) // per_row for d in set(k)}
        return [after[k[s]] for s in range(nz)]

    def mask_rows(j, k, slots):
        return jnp.concatenate([maskx[j - k[s] + PAD, block(s), :] for s in slots], axis=0)

    def fwd_group(j, b, g, k0, k1):
        slots = (near, far)[g]
        page = pages(j, KF)

        @functools.partial(lax.fori_loop, k0, k1, init_val=None, unroll=UNROLL)
        def _(k, _):
            at = pl.ds(pl.multiple_of(k * CH, CH), CH)
            logits = jnp.dot(xbuf[b, g * half:(g + 1) * half], wbuf[:, at], preferred_element_type=F32)
            for t in range(CH // LANE):
                at = pl.ds(pl.multiple_of(k * CH + t * LANE, LANE), LANE)
                zt = logits[:, t * LANE:(t + 1) * LANE] + bias[:, at]
                act = jnp.log(1.0 + jnp.maximum(zt, 0.0)) * mask_rows(j, KF, slots)
                for i, s in enumerate(slots):
                    for u in WAYS:
                        r0 = i * br + u * UT
                        row_sum = jnp.sum(act[r0:r0 + UT, :], axis=0, keepdims=True)
                        rep[page[s], PAIR * s + u:PAIR * s + u + 1, at] = rep[page[s], PAIR * s + u:PAIR * s + u + 1, at] + row_sum

    def cut(eighths):
        return n_chunk * eighths // SUB

    fwd_end = n_unit + KF[MAXD]

    def release_far(j):
        @pl.when(j >= 1)
        def _():
            release(KF, j, far)

    @pl.loop(1, fwd_end)
    def _(j):
        b = par(j)
        release_far(j - 1)
        inject(KF, j)
        own_chip(KF, j - KF[0])
        near_left = j < n_unit + max(KF[s] for s in near)

        @pl.when(near_left)
        def _():
            fwd_group(j, b, 0, 0, cut(6))
        relay(KF, j - 2, 3)

        @pl.when(near_left)
        def _():
            fwd_group(j, b, 0, cut(6), n_chunk)
        release(KF, j, near)
        relay(KF, j - 1, 2)
        relay(KF, j - 3, 4)
        fwd_group(j, b, 1, 0, cut(4))
        relay(KF, j, 1)
        fwd_group(j, b, 1, cut(4), n_chunk)
        injected(KF, j)

    release_far(jnp.int32(fwd_end - 1))

    for s in range(nz):
        if s == MAXD:
            for way in WAYS:
                give_credit(s, way)
        else:
            give_credit(s, way_of(s), 2)

    q_total = q_rows * n_group
    d_total = d_rows * n_group
    v_total = v_loc * n_group
    tau = q_len * math.sqrt(v_total * d_len) / 16.0
    lam_q = 4.0 / (v_total * q_len * q_len)
    lam_d = 4.0 / (v_total * d_len * d_len)
    nd = d_rows // PAIR * n_group
    nq = q_rows // PAIR * n_group
    q0 = PAD // per_row
    d0 = q0 + n_qpage

    @pl.loop(0, v_chip // CB)
    def _(k):
        at = pl.ds(pl.multiple_of(k * CB, CB), CB)
        for r in range(d_rows // PAIR):
            rdx[c, r * n_group:(r + 1) * n_group, at] = sum(rep[d0 + r * pieces + i, :, at] for i in range(pieces))
        q_sum = sum(rep[q0 + i, :, at] for i in range(n_qpage))
        rdx[c, nd:nd + SUB, at] = sum(q_sum[i * SUB:(i + 1) * SUB] for i in range(n_group // SUB))

    def to_sib(src, dst, i):
        return remote(src, dst, pair_sem.at[i, 0], pair_sem.at[i, 1], sib)

    send_rd = to_sib(rdx.at[c], rdx.at[c], 0)
    send_rd.start()
    inject(KB, ZERO, BWD)
    send_rd.wait()

    def d_reps(at):
        return jnp.concatenate([rdx[0, 0:nd, at], rdx[1, 0:nd, at]], axis=0)

    def q_mean_of(at):
        return jnp.sum(rdx[0, nd:nd + SUB, at] + rdx[1, nd:nd + SUB, at], axis=0, keepdims=True) * (1.0 / q_total)

    def d_mean_of(at):
        return jnp.sum(d_reps(at), axis=0, keepdims=True) * (1.0 / d_total)

    def lanes(v):
        return sum(v[:, t * LANE:(t + 1) * LANE] for t in range(CB // LANE))

    def score_chunk(k, carry):
        s_acc, rq, rd = carry
        at = pl.ds(pl.multiple_of(k * CB, CB), CB)
        q_rep = rep[q0:q0 + n_qpage, :, at].reshape(nq, CB)
        s_acc = s_acc + lax.dot_general(d_reps(at), q_rep, (((1,), (1,)), ((), ())), precision=HIGHEST,
                                        preferred_element_type=F32)
        qm, dm = q_mean_of(at), d_mean_of(at)
        return s_acc, rq + lanes(qm * qm), rd + lanes(dm * dm)

    score, reg_q, reg_d = lax.fori_loop(0, v_chip // CB, score_chunk,
                                        (jnp.zeros((PAIR * nd, nq), F32), jnp.zeros((1, LANE), F32), jnp.zeros((1, LANE), F32)))

    def turn(n):
        i = lax.broadcasted_iota(jnp.int32, (n, n), 0)
        k = lax.broadcasted_iota(jnp.int32, (n, n), 1)
        same = (i // n_group == k // n_group) & (i % 2 == k % 2)
        return (same & (((i // PAIR) % nz + (k // PAIR) % nz) % nz == z)).astype(F32)

    def exact(a, b):
        return jnp.dot(a, b, precision=HIGHEST, preferred_element_type=F32)

    turn_d, turn_q = turn(PAIR * nd), turn(nq)
    smsg[0, 0:PAIR * nd, 0:nq] = exact(exact(turn_d, score), turn_q)
    smsg[0, PAIR * nd:PAIR * nd + 1, :] = reg_q
    smsg[0, PAIR * nd + 1:PAIR * nd + 2, :] = reg_d
    send_s = [remote(smsg.at[0], smsg.at[t], sm_send.at[t], sm_recv.at[t], peers[t - 1]) for t in range(1, nz)]
    for cp in send_s:
        cp.start()

    def turn_head(first):
        @pl.loop(0, v_chip // LANE // PAIR)
        def _(k):
            at = pl.ds(pl.multiple_of((first * (v_chip // LANE // PAIR) + k) * LANE, LANE), LANE)
            wt[at, :] = wbuf[:, at].T

    pos_rows = jnp.concatenate([msgs[i, 0, 3:4, :] for i in range(n_group)], axis=0)
    spread = (lax.broadcasted_iota(jnp.int32, (LANE, nq), 0)
              == PAIR * (lax.broadcasted_iota(jnp.int32, (LANE, nq), 1) // n_group) + c).astype(F32)
    pos_all = exact(pos_rows, spread)
    pick = (lax.broadcasted_iota(jnp.int32, (n_group, nq), 1) % n_group
            == lax.broadcasted_iota(jnp.int32, (n_group, nq), 0))
    pos_row = jnp.sum(jnp.where(pick, pos_all, 0.0), axis=0, keepdims=True)
    ridx = lax.broadcasted_iota(jnp.int32, (PAIR * nd, nq), 0)
    doc = (ridx % n_group) * d_rows + PAIR * ((ridx % nd) // n_group) + ridx // nd
    target = (doc.astype(F32) == pos_row).astype(F32)

    turn_head(0)
    relay(KB, ZERO, 1, BWD)
    injected(KB, ZERO)
    turn_head(1)
    for cp in send_s:
        cp.wait()
    total = smsg[0]
    for t in range(1, nz):
        total = total + smsg[t]
    scores = total[0:PAIR * nd, 0:nq] * (1.0 / tau)
    top = jnp.max(scores, axis=0, keepdims=True)
    log_norm = top + jnp.log(jnp.sum(jnp.exp(scores - top), axis=0, keepdims=True))
    row_loss = log_norm - jnp.sum(scores * target, axis=0, keepdims=True)
    loss_part = jnp.sum(row_loss, axis=1, keepdims=True)
    gt = (jnp.exp(scores - log_norm) - target) * (1.0 / (q_total * tau))
    gt = exact(exact(turn_d, gt), turn_q)
    g = gt.T
    lossx[c] = jnp.broadcast_to(loss_part, (SUB, LANE))
    send_l = to_sib(lossx.at[c], lossx.at[c], 1)
    send_l.start()
    inject(KB, ZERO + 1, BWD)
    relay(KB, ZERO, 2, BWD)

    @pl.loop(0, v_chip // CB)
    def _(k):
        at = pl.ds(pl.multiple_of(k * CB, CB), CB)
        q_rep = rep[q0:q0 + n_qpage, :, at].reshape(nq, CB)
        dp = exact(gt, q_rep)
        ddx[0, :, at] = dp[0:nd]
        ddx[1, :, at] = dp[nd:PAIR * nd]

    send_dd = to_sib(ddx.at[o], ddr, 2)
    send_dd.start()

    @pl.loop(0, v_chip // CB)
    def _(k):
        at = pl.ds(pl.multiple_of(k * CB, CB), CB)
        gq = exact(g, d_reps(at)) + q_mean_of(at) * (2.0 * lam_q / q_total)
        rep[q0:q0 + n_qpage, :, at] = gq.reshape(n_qpage, n_group, CB)

    send_l.wait()
    reg = (jnp.sum(total[PAIR * nd:PAIR * nd + 1, :], axis=1, keepdims=True) * lam_q
           + jnp.sum(total[PAIR * nd + 1:PAIR * nd + 2, :], axis=1, keepdims=True) * lam_d)
    lossf[0] = (lossx[0] + lossx[1]) * (1.0 / q_total) + reg

    send_loss = [remote(lossf.at[0], lossf.at[1], loss_send.at[t], loss_recv, peers[t - 1]) for t in range(1, nz)]

    @pl.when(z == 0)
    def _():
        for cp in send_loss:
            cp.start()
    relay(KB, ZERO + 1, 1, BWD)
    injected(KB, ZERO + 1)
    relay(KB, ZERO, 3, BWD)
    send_dd.wait()

    @pl.loop(0, v_chip // CB)
    def _(k):
        at = pl.ds(pl.multiple_of(k * CB, CB), CB)
        gd = ddx[c, :, at] + ddr[:, at] + d_mean_of(at) * (2.0 * lam_d / d_total)
        for r in range(d_rows // PAIR):
            for i in range(pieces):
                rep[d0 + r * pieces + i, :, at] = gd[r * n_group:(r + 1) * n_group]

    def bwd_chunk(j, b, page, k, slots=ORDER, weights=BWD):
        at0 = pos[slots[0]] * br
        some = slice(at0, at0 + len(slots) * br)
        cols = pl.ds(pl.multiple_of(k * CB, CB), CB)
        logits = jnp.dot(xbuf[b, some], wbuf[:, cols], preferred_element_type=F32)
        low = []
        for t in range(CB // LANE):
            at = pl.ds(pl.multiple_of(k * CB + t * LANE, LANE), LANE)
            zt = logits[:, t * LANE:(t + 1) * LANE] + bias[:, at]
            grad = jnp.concatenate([jnp.broadcast_to(rep[page[s], PAIR * s + u:PAIR * s + u + 1, at], (UT, LANE))
                                    for s in slots for u in WAYS], axis=0)
            gz = jnp.where(zt > 0.0, grad * mask_rows(j, KB, slots) / (1.0 + jnp.maximum(zt, 0.0)), 0.0)
            gbacc[:, at] = gbacc[:, at] + jnp.sum(gz.reshape(-1, SUB, LANE), axis=0)
            low.append(gz.astype(BF16))
        low = jnp.concatenate(low, axis=1)
        gbuf[some, cols] = low
        if weights:
            gw[:, cols] = gw[:, cols] + jnp.dot(xt[...], low, preferred_element_type=F32)

    def bwd_hidden(k0, k1, some=slice(None)):
        wide = hid // 4

        @functools.partial(lax.fori_loop, k0, k1, init_val=None, unroll=UNROLL)
        def _(k, _):
            cols = pl.ds(pl.multiple_of(k * wide, wide), wide)
            pbuf[some, cols] = jnp.dot(gbuf[some, :], wt[:, cols], preferred_element_type=F32).astype(BF16)

    def deep(n):
        return lax.rem(n + BIG, DEEP)

    def room(n):
        return lax.rem(n + BIG, ROOM)

    def rs_copy(n, way, dist):
        to = behind[way] if isinstance(way, int) else choose(way, left, right)
        return remote(sbuf.at[way, dist - 1], rbuf.at[way, dist - 2, room(n)], rs_send.at[way, dist - 1],
                      rs_recv.at[way, dist - 2, room(n)], dev(to, c))

    def home_copy(n, way, cc, i):
        return remote(sbuf.at[way, 0, pl.ds(i * UT, UT)], hbuf.at[way, cc, room(n)], h_send.at[way, i],
                      h_recv.at[way, cc, room(n)], dev(behind[way], i))

    def pair_copy(n):
        return remote(sst.at[par(n)], sibp.at[deep(n)], sp_send.at[par(n)], sp_recv.at[deep(n)], sib)

    def rs_sent(n, dist):
        @guard(exists(n))
        def _():
            if dist == MAXD:
                rs_copy(n, par(n), dist).wait_send()
                return
            for way in WAYS:
                if dist == 1:
                    for i in WAYS:
                        home_copy(n, way, c, i).wait_send()
                else:
                    rs_copy(n, way, dist).wait_send()

    def rs_both(n, dist):
        rs_sent(n - (2 if dist == MAXD else 1), dist)

        def joined(way, mine):
            rs_copy(n, way, dist + 1).wait_recv()
            sbuf[way, dist - 1] = (mine.astype(F32) + rbuf[way, dist - 1, room(n)].astype(F32)).astype(BF16)

        @guard(exists(n))
        def _():
            if dist == MAXD:
                sbuf[par(n), dist - 1] = pbuf[block(MAXD), :]
                rs_copy(n, par(n), dist).start()
            elif dist == MAXD - 1:
                way = par(n)
                sbuf[1 - way, dist - 1] = part[choose(way, nz - dist, dist), deep(n)]
                rs_copy(n, 1 - way, dist).start()
                joined(way, part[choose(way, dist, nz - dist), deep(n)])
                rs_copy(n, way, dist).start()
            else:
                for way in WAYS:
                    joined(way, part[slot(way, dist), deep(n)])
                    if dist == 1:
                        for i in WAYS:
                            home_copy(n, way, c, i).start()
                    else:
                        rs_copy(n, way, dist).start()

    def rs_home(n):
        @guard(exists(n))
        def _():
            for cc in WAYS:
                for way in WAYS:
                    home_copy(n, way, cc, 0).wait_recv()
                at = unit_rows(n)
                acc_h[cc, n // per_row, at] = (acc_h[cc, n // per_row, at].astype(F32) + hbuf[0, cc, room(n)].astype(F32)
                                               + hbuf[1, cc, room(n)].astype(F32)).astype(BF16)

    def pair_send(n):
        @guard(exists(n - 2))
        def _():
            pair_copy(n - 2).wait_send()

        @guard(exists(n))
        def _():
            sst[par(n)] = pbuf[part_of_block(0, o), :]
            pair_copy(n).start()
            acc_h[c, n // per_row, unit_rows(n)] = pbuf[part_of_block(0, c), :]

    def pair_take(n):
        @guard(exists(n))
        def _():
            pair_copy(n).wait_recv()
            acc_h[o, n // per_row, unit_rows(n)] = sibp[deep(n)]

    last = n_unit + KB[MAXD]
    assert all(n_unit + KB[s] < last for s in near)

    def part_b(eighths):
        return v_chip // CB * eighths // SUB

    def bwd_step(j):
        b = par(j)
        page = pages(j, KB)
        late = None if steady else j >= 2

        def weights(k0, k1):
            @functools.partial(lax.fori_loop, k0, k1, init_val=None, unroll=UNROLL)
            def _(k, _):
                bwd_chunk(j, b, page, k)

        relay(KB, j - 2, 4)
        own_chip(KB, j - 1)
        xt[...] = xbuf[b].T
        weights(0, part_b(4))

        @guard(late)
        def _():
            relay(KB, j, 1, BWD)
        rs_both(j - 3, 4)
        rs_both(j - 5, 1)
        weights(part_b(4), part_b(6))

        @guard(late)
        def _():
            relay(KB, j - 1, 3, BWD)
        weights(part_b(6), v_chip // CB)
        release(KB, j, ORDER)
        rs_both(j - 4, 2)
        bwd_hidden(0, 3)

        @guard(late)
        def _():
            injected(KB, j)
        inject(KB, j + 1, BWD)
        relay(KB, j, 2, BWD)
        rs_both(j - 3, 3)
        rs_home(j - 5)
        bwd_hidden(3, 4)
        for s in range(1, nz):
            if s != MAXD:
                part[s, deep(j - KB[s])] = pbuf[block(s), :]
        pair_send(j - 1)
        pair_take(j - 2)

    @pl.loop(1, last - 1)
    def _(j):
        middle = (j >= 6) & (j < n_unit - 1)

        @pl.when(middle)
        def _():
            steady.append(BWD)
            bwd_step(j)
            steady.pop()

        @pl.when(jnp.logical_not(middle))
        def _():
            bwd_step(j)

    j = ZERO + last - 1
    b = par(j)
    page = pages(j, KB)
    some = slice(half, rows)
    relay(KB, j - 2, 4)
    rs_both(j - 3, 4)
    rs_both(j - 5, 1)

    @functools.partial(lax.fori_loop, 0, v_chip // CB, init_val=None, unroll=UNROLL)
    def _(k, _):
        bwd_chunk(j, b, page, k, far, False)
    rs_both(j - 4, 2)
    bwd_hidden(0, 4, some)
    for s in far:
        if s != MAXD:
            part[s, deep(j - KB[s])] = pbuf[block(s), :]
    rs_both(j + 1 - 3, 4)
    rs_both(j - 3, 3)
    release(KB, j, ORDER)
    pair_send(j - 1)
    pair_take(j - 2)
    rs_home(j - 5)
    xt[:, some] = xbuf[b, some].T

    @functools.partial(lax.fori_loop, 0, v_chip // CB, init_val=None, unroll=UNROLL)
    def _(k, _):
        cols = pl.ds(pl.multiple_of(k * CB, CB), CB)
        gw[:, cols] = gw[:, cols] + jnp.dot(xt[:, some], gbuf[some, cols], preferred_element_type=F32)

    n_part = gx_send.shape[0] - 1
    step = v_loc // n_part
    send_g = []
    for k in range(n_part):
        theirs = pl.ds(pl.multiple_of(o * v_loc + k * step, step), step)
        send_g.append(remote(gw.at[:, theirs], grecv.at[k % PAIR], gx_send.at[k], gx_recv.at[k], sib))
    send_gb = remote(gbacc.at[:, sib_cols], gbrecv, gx_send.at[n_part], gx_recv.at[n_part], sib)
    for cp in send_g[:PAIR]:
        cp.start()
    send_gb.start()

    w_outs = []

    def add_part():
        k = len(w_outs)
        send_g[k].wait_recv()
        at = pl.ds(pl.multiple_of(c * v_loc + k * step, step), step)

        @pl.loop(0, hid // BIG)
        def _(i):
            rr = pl.ds(pl.multiple_of(i * BIG, BIG), BIG)
            wbuf[rr, at] = (gw[rr, at] + grecv[k % PAIR, rr]).astype(BF16)
        w_outs.append(pltpu.make_async_copy(wbuf.at[:, at], gw_out.at[:, pl.ds(k * step, step)], out_sem.at[n_load + k]))
        w_outs[-1].start()
        if k + PAIR < n_part:
            pl.semaphore_signal(gx_cred, device_id=sib, device_id_type=MESH)
            pl.semaphore_wait(gx_cred)
            send_g[k + PAIR].start()

    n_load = len(loads)
    for j in range(last, n_unit + 5):
        n = ZERO + j
        if j > last:
            rs_both(n - 3, 4)
        if j == n_unit + 4:
            add_part()
        rs_both(n - 5, 1)
        rs_both(n - 4, 2)
        rs_both(n - 3, 3)
        pair_send(n - 1)
        add_part()
        rs_home(n - 5)
    rs_sent(jnp.int32(n_unit - 1), 1)

    outs = []
    for cc in WAYS:
        outs.append(pltpu.make_async_copy(acc_h.at[cc, pl.ds(0, n_qpage)], dq_out.at[:, cc], out_sem.at[len(outs)]))
        for r in range(d_rows // PAIR):
            outs.append(pltpu.make_async_copy(acc_h.at[cc, pl.ds(n_qpage + r * pieces, pieces)], dd_out.at[r, cc],
                                              out_sem.at[len(outs)]))
    for cp in outs:
        cp.start()
    while len(w_outs) < n_part:
        add_part()
    send_gb.wait_recv()
    gb_ref[...] = jnp.sum(gbacc[:, my_cols] + gbrecv[...], axis=0, keepdims=True)

    @pl.when(z == 0)
    def _():
        for cp in send_loss:
            cp.wait_send()
        loss_ref[...] = lossf[0, 0:1, 0:1]

    @pl.when(z != 0)
    def _():
        send_loss[0].wait_recv()
        loss_ref[...] = lossf[1, 0:1, 0:1]
    for cp in send_g:
        cp.wait_send()
    send_gb.wait_send()
    for cp in outs + w_outs:
        cp.wait()


def settle(*refs):
    n = len(refs) // 4
    copies = []
    for a, z, buf, sem in zip(*(refs[k * n:(k + 1) * n] for k in range(4))):
        pieces = sem.shape[1]
        size = a.shape[0] // pieces
        for p in range(pieces):
            at = pl.ds(p * size, size)
            copies.append((pltpu.make_async_copy(a.at[at], buf.at[at], sem.at[0, p]),
                           pltpu.make_async_copy(buf.at[at], z.at[at], sem.at[1, p])))
    for cp, _ in copies:
        cp.start()
    for cp, back in copies:
        cp.wait()
        back.start()
    for _, back in copies:
        back.wait()


def solution(mesh):
    n_group = mesh.shape['tp']
    nz = n_group // PAIR
    row_spec = P(('dp', 'tp'))
    mask_spec = P(('dp', 'tp'), None)
    hid_spec = P(('dp', 'tp'), None, None)

    def local_step(q_hidden, d_hidden, q_mask, d_mask, positive, w_head, b_head):
        q_rows, q_len, hid = q_hidden.shape
        d_rows, d_len, _ = d_hidden.shape
        v_loc = w_head.shape[1]
        v_chip = PAIR * v_loc
        per_row = q_len // UT
        pieces = d_len // q_len
        n_page = q_rows // PAIR + d_rows // PAIR * pieces
        n_unit = n_page * per_row
        rows = nz * PAIR * UT
        nd, nq = d_rows // PAIR * n_group, q_rows // PAIR * n_group
        s_rows = -(-(PAIR * nd + 2) // SUB) * SUB
        n_part = 4 if v_loc >= 512 else 2
        n_load = PAIR * (1 + d_rows // PAIR)
        dma, reg = pltpu.SemaphoreType.DMA, pltpu.SemaphoreType.REGULAR
        anym = pl.BlockSpec(memory_space=pl.ANY)
        vm = pl.BlockSpec(memory_space=pltpu.VMEM)
        q_shape = (q_rows // PAIR, 2, q_len, hid)
        d_shape = (d_rows // PAIR, 2, pieces, q_len, hid)
        out_shape = (
            jax.ShapeDtypeStruct((1, 1), F32),
            jax.ShapeDtypeStruct((hid, v_loc), BF16),
            jax.ShapeDtypeStruct((1, v_loc), F32),
            jax.ShapeDtypeStruct(q_shape, BF16),
            jax.ShapeDtypeStruct(d_shape, BF16),
        )
        scratch = [
            pltpu.VMEM((hid, v_chip), BF16),
            pltpu.VMEM((v_chip, hid), BF16),
            pltpu.VMEM((hid, v_chip), F32),
            pltpu.VMEM((PAIR, hid, v_loc // n_part), F32),
            pltpu.VMEM(((n_unit + PAIR * PAD) // per_row, n_group, v_chip), F32),
            pltpu.VMEM((n_unit + PAIR * PAD, rows, LANE), F32),
            pltpu.VMEM((PAIR, n_page, q_len, hid), BF16),
            pltpu.VMEM((PAIR, n_page, q_len, hid), BF16),
            pltpu.VMEM((nz, DEEP, PAIR * UT, hid), BF16),
            pltpu.VMEM((PAIR, rows, hid), BF16),
            pltpu.VMEM((PAIR, MAXD - 1, ROOM, PAIR * UT, hid), BF16),
            pltpu.VMEM((PAIR, MAXD, PAIR * UT, hid), BF16),
            pltpu.VMEM((PAIR, 2, ROOM, UT, hid), BF16),
            pltpu.VMEM((DEEP, UT, hid), BF16),
            pltpu.VMEM((PAIR, UT, hid), BF16),
            pltpu.VMEM((rows, v_chip), BF16),
            pltpu.VMEM((rows, hid), BF16),
            pltpu.VMEM((hid, rows), BF16),
            pltpu.VMEM((PAIR, nd + SUB, v_chip), F32),
            pltpu.VMEM((PAIR, nd, v_chip), F32),
            pltpu.VMEM((nd, v_chip), F32),
            pltpu.VMEM((1, v_chip), F32),
            pltpu.VMEM((SUB, v_chip), F32),
            pltpu.VMEM((SUB, v_loc), F32),
            pltpu.VMEM((n_group, 2, 4, LANE), F32),
            pltpu.VMEM((nz, s_rows, LANE), F32),
            pltpu.VMEM((PAIR, SUB, LANE), F32),
            pltpu.VMEM((PAIR, SUB, LANE), F32),
            dma((PAIR, MAXD, 2)), dma((PAIR, nz, 2)), reg((PAIR, MAXD)), dma((PAIR, 2)), reg((PAIR, 2)), dma, reg,
            dma((PAIR, MAXD)), dma((PAIR, MAXD - 1, ROOM)), dma((PAIR, 2)), dma((PAIR, 2, ROOM)),
            dma((PAIR,)), dma((DEEP,)),
            dma((n_load + PAIR,)), dma((PAIR,)), dma((PAIR,)), dma((n_group - 1,)), dma((n_group - 1,)), dma((nz,)), dma((nz,)),
            dma((3, 2)), dma((n_part + 1,)), dma((n_part + 1,)), reg, dma((nz,)), dma, dma((n_load + n_part,)),
        ]
        loss, gw, gb, dq, dd = pl.pallas_call(
            functools.partial(kernel, n_group, q_rows, q_len, d_rows, d_len),
            out_shape=out_shape,
            in_specs=[anym] * 4 + [vm] * 3,
            out_specs=(vm, anym, vm, anym, anym),
            scratch_shapes=scratch,
            compiler_params=pltpu.CompilerParams(collective_id=0, has_side_effects=True, vmem_limit_bytes=67043328),
        )(q_hidden.reshape(q_shape), d_hidden.reshape(d_shape), w_head, b_head.reshape(1, v_loc),
          q_mask, d_mask, positive.reshape(1, q_rows))
        results = (gw, dq, dd, gb, loss)
        gw, dq, dd, gb, loss = pl.pallas_call(
            settle,
            out_shape=[jax.ShapeDtypeStruct(a.shape, a.dtype) for a in results],
            in_specs=[anym] * len(results),
            out_specs=[anym] * len(results),
            scratch_shapes=[pltpu.VMEM(a.shape, a.dtype) for a in results] + [dma((2, math.gcd(4, a.shape[0]))) for a in results],
            compiler_params=pltpu.CompilerParams(vmem_limit_bytes=67043328),
        )(*results)
        return (loss.reshape(1), gw, gb.reshape(v_loc), dq.reshape(q_hidden.shape), dd.reshape(d_hidden.shape))

    return jax.shard_map(local_step, mesh=mesh,
                         in_specs=(hid_spec, hid_spec, mask_spec, mask_spec, row_spec, P(None, 'tp'), P('tp')),
                         out_specs=(P('dp'), P('dp', 'tp'), row_spec, hid_spec, hid_spec),
                         check_vma=False)
```
